8 devices in a mesh: dp: 1 (over z), ctx: 8 (over y, x, core).
Axes of the slice: x: 2, y: 2, z: 1, core: 2. Of those that a mesh axis runs over, the one named last changes fastest.
Arguments:
- x_seq: bfloat16 [512, 2560], P(('dp', 'ctx'))
- pos_ids: int32 [512], P(('dp', 'ctx'))
- seg_ids: int32 [512], P(('dp', 'ctx'))
- w_dq: bfloat16 [2560, 768], replicated
- w_uq: bfloat16 [768, 2560], replicated
- w_qr: bfloat16 [768, 1280], replicated
- w_dkv: bfloat16 [2560, 256], replicated
- w_kr: bfloat16 [2560, 32], replicated
- w_uk: bfloat16 [256, 2560], replicated
- w_uv: bfloat16 [256, 2560], replicated
- w_out: bfloat16 [2560, 2560], replicated
- gain_q: bfloat16 [768], replicated
- gain_kv: bfloat16 [256], replicated
Outputs:
- output: bfloat16 [512, 2560], P(('dp', 'ctx'))
All inputs are finite; a program needn't handle non-finite values.
Results may differ from the reference program's by a relative error of at most 0.0079002.
Values are sent between devices in bfloat16 or wider.
A program may use at most 1 GiB of HBM per device.

```python
import jax
import jax.numpy as jnp
from jax import lax

D_MODEL = 2560
NUM_HEADS = 40
Q_RANK = 768
KV_RANK = 256
NOPE_DIM = 64
ROPE_DIM = 32
V_DIM = 64
SEQ_DEV = 64
GROUP_SIZE = 8
NUM_DOCS = 4
NORM_EPS = 1e-6
SEQ_LEN = SEQ_DEV * GROUP_SIZE
HALF_DEV = SEQ_DEV // 2
NUM_BLOCKS = SEQ_LEN // SEQ_DEV


def draw_documents(doc_key):
    doc_cuts = jnp.sort(jax.random.permutation(doc_key, SEQ_LEN - 1)[:NUM_DOCS - 1] + 1).astype(jnp.int32)
    doc_starts = jnp.concatenate([jnp.zeros((1,), jnp.int32), doc_cuts])
    row_ids = jnp.arange(SEQ_LEN, dtype=jnp.int32)
    device_ids = row_ids // SEQ_DEV
    in_device = row_ids % SEQ_DEV
    piece_ids = jnp.where(in_device < HALF_DEV, device_ids, 2 * GROUP_SIZE - 1 - device_ids)
    token_ids = piece_ids * HALF_DEV + in_device % HALF_DEV
    seg_ids = jnp.sum((token_ids[:, None] >= doc_cuts[None, :]).astype(jnp.int32), axis=1)
    pos_ids = token_ids - doc_starts[seg_ids]
    return pos_ids.astype(jnp.int32), seg_ids.astype(jnp.int32)


def init_weight(rng_key, fan_in, fan_out):
    return (jax.random.normal(rng_key, (fan_in, fan_out), jnp.float32) * fan_in ** -0.5).astype(jnp.bfloat16)


def setup_inputs(seed: int = 0, part: int = 0) -> dict:
    root_key = jax.random.key(seed)
    part_key = jax.random.fold_in(root_key, part)
    data_keys = jax.random.split(part_key, 2)
    weight_keys = jax.random.split(root_key, 10)
    pos_ids, seg_ids = draw_documents(data_keys[1])
    x_seq = jax.random.normal(data_keys[0], (SEQ_LEN, D_MODEL), jnp.float32).astype(jnp.bfloat16)
    return {
        'x_seq': x_seq,
        'pos_ids': pos_ids,
        'seg_ids': seg_ids,
        'w_dq': init_weight(weight_keys[0], D_MODEL, Q_RANK),
        'w_uq': init_weight(weight_keys[1], Q_RANK, NUM_HEADS * NOPE_DIM),
        'w_qr': init_weight(weight_keys[2], Q_RANK, NUM_HEADS * ROPE_DIM),
        'w_dkv': init_weight(weight_keys[3], D_MODEL, KV_RANK),
        'w_kr': init_weight(weight_keys[4], D_MODEL, ROPE_DIM),
        'w_uk': init_weight(weight_keys[5], KV_RANK, NUM_HEADS * NOPE_DIM),
        'w_uv': init_weight(weight_keys[6], KV_RANK, NUM_HEADS * V_DIM),
        'w_out': init_weight(weight_keys[7], NUM_HEADS * V_DIM, D_MODEL),
        'gain_q': jax.random.uniform(weight_keys[8], (Q_RANK,), jnp.float32, 0.5, 1.5).astype(jnp.bfloat16),
        'gain_kv': jax.random.uniform(weight_keys[9], (KV_RANK,), jnp.float32, 0.5, 1.5).astype(jnp.bfloat16),
    }


def rms_norm(vals, gain):
    mean_sq = jnp.mean(vals * vals, axis=-1, keepdims=True)
    return (vals * lax.rsqrt(mean_sq + NORM_EPS) * gain.astype(jnp.float32)).astype(jnp.bfloat16)


def rope_tables(pos_ids):
    half_dim = ROPE_DIM // 2
    inv_freq = 10000.0 ** (-2.0 * jnp.arange(half_dim, dtype=jnp.float32) / ROPE_DIM)
    angles = pos_ids.astype(jnp.float32)[:, None] * inv_freq[None, :]
    return jnp.cos(angles), jnp.sin(angles)


def apply_rope(vals, cos_tab, sin_tab):
    half_dim = vals.shape[-1] // 2
    lead_half = vals[..., :half_dim]
    tail_half = vals[..., half_dim:]
    return jnp.concatenate([lead_half * cos_tab - tail_half * sin_tab, tail_half * cos_tab + lead_half * sin_tab], axis=-1)


def reference(x_seq, pos_ids, seg_ids, w_dq, w_uq, w_qr, w_dkv, w_kr, w_uk, w_uv, w_out, gain_q, gain_kv):
    cos_tab, sin_tab = rope_tables(pos_ids)
    c_q = rms_norm(jnp.dot(x_seq, w_dq, preferred_element_type=jnp.float32), gain_q)
    q_nope = jnp.dot(c_q, w_uq, preferred_element_type=jnp.float32).astype(jnp.bfloat16)
    q_rope = jnp.dot(c_q, w_qr, preferred_element_type=jnp.float32).reshape(SEQ_LEN, NUM_HEADS, ROPE_DIM)
    q_rope = apply_rope(q_rope, cos_tab[:, None, :], sin_tab[:, None, :]).astype(jnp.bfloat16)
    c_kv = rms_norm(jnp.dot(x_seq, w_dkv, preferred_element_type=jnp.float32), gain_kv)
    k_rope = apply_rope(jnp.dot(x_seq, w_kr, preferred_element_type=jnp.float32), cos_tab, sin_tab)
    k_rope = k_rope.astype(jnp.bfloat16).astype(jnp.float32)
    score_scale = (NOPE_DIM + ROPE_DIM) ** -0.5
    head_inputs = (
        q_nope.reshape(SEQ_LEN, NUM_HEADS, NOPE_DIM).transpose(1, 0, 2).reshape(NUM_HEADS, NUM_BLOCKS, SEQ_DEV, NOPE_DIM),
        q_rope.transpose(1, 0, 2).reshape(NUM_HEADS, NUM_BLOCKS, SEQ_DEV, ROPE_DIM),
        w_uk.reshape(KV_RANK, NUM_HEADS, NOPE_DIM).transpose(1, 0, 2),
        w_uv.reshape(KV_RANK, NUM_HEADS, V_DIM).transpose(1, 0, 2),
    )
    block_pos = pos_ids.reshape(NUM_BLOCKS, SEQ_DEV)
    block_seg = seg_ids.reshape(NUM_BLOCKS, SEQ_DEV)

    def one_head(head_args):
        q_nope_h, q_rope_h, w_uk_h, w_uv_h = head_args
        k_nope = jnp.dot(c_kv, w_uk_h, preferred_element_type=jnp.float32).astype(jnp.bfloat16).astype(jnp.float32)
        v_head = jnp.dot(c_kv, w_uv_h, preferred_element_type=jnp.float32).astype(jnp.bfloat16).astype(jnp.float32)

        def one_block(block_args):
            qn_blk, qr_blk, pos_blk, seg_blk = block_args
            scores = jnp.dot(qn_blk.astype(jnp.float32), k_nope.T) + jnp.dot(qr_blk.astype(jnp.float32), k_rope.T)
            allowed = (pos_ids[None, :] <= pos_blk[:, None]) & (seg_ids[None, :] == seg_blk[:, None])
            scores = jnp.where(allowed, scores * score_scale, -jnp.inf)
            weights = jnp.exp(scores - jnp.max(scores, axis=1, keepdims=True))
            return (jnp.dot(weights, v_head) / jnp.sum(weights, axis=1, keepdims=True)).astype(jnp.bfloat16)

        return lax.map(one_block, (q_nope_h, q_rope_h, block_pos, block_seg))

    head_out = lax.map(one_head, head_inputs)
    attn_out = head_out.reshape(NUM_HEADS, SEQ_LEN, V_DIM).transpose(1, 0, 2).reshape(SEQ_LEN, NUM_HEADS * V_DIM)
    return jnp.dot(attn_out, w_out, preferred_element_type=jnp.float32).astype(jnp.bfloat16)
```

```python
import functools
import math

import numpy as np
import jax
import jax.numpy as jnp
from jax import lax
from jax.experimental import pallas as pl
from jax.experimental.pallas import tpu as pltpu
from jax.sharding import PartitionSpec as P

NORM_EPS = 1e-6
MESH = pl.DeviceIdType.MESH
F32 = jnp.float32
BF16 = jnp.bfloat16
GROUP_HEADS = 4


def rms_rows(vals, gain):
    mean_sq = jnp.mean(vals * vals, axis=-1, keepdims=True)
    return (vals * lax.rsqrt(mean_sq + NORM_EPS) * gain.astype(F32)).astype(BF16)


def dot_nn(a, b):
    return lax.dot_general(a, b, (((1,), (0,)), ((), ())), preferred_element_type=F32)


def dot_nt(a, b):
    return lax.dot_general(a, b, (((1,), (1,)), ((), ())), preferred_element_type=F32)


def dot_tn(a, b):
    return lax.dot_general(a, b, (((0,), (0,)), ((), ())), preferred_element_type=F32)


def kernel(n, x_hbm, pos_hbm, wdq_hbm, wuq_hbm, wqr_hbm, wdkv_hbm, wkr_hbm, wuk_hbm, wuv_hbm, wout_hbm, gq_hbm, gkv_hbm,
           y_ref, x, pos, wdq, wuq, wqr, wdkv, wkr, wuk, wuv, wout, gq, gkv,
           lat, gath, bias, qn_s, qr_s, kn_s, v_s, krep_s, o_s, load_sem, send_sem, recv_sem):
    me = lax.axis_index('ctx')
    rows = x.shape[0]
    half = rows // 2
    rank = wdkv.shape[1]
    rope = wkr.shape[0]
    num_heads = wqr.shape[1] // rope
    nope = wuq.shape[1] // num_heads
    keys = n * rows
    gw = GROUP_HEADS * nope
    rw = GROUP_HEADS * rope
    lanes = GROUP_HEADS * rows
    groups = num_heads // GROUP_HEADS

    barrier = pltpu.get_barrier_semaphore()
    for j in range(1, n):
        pl.semaphore_signal(barrier, inc=1, device_id={'ctx': lax.rem(me + j, n)}, device_id_type=MESH)

    loads = []

    def load(src, dst):
        copy = pltpu.make_async_copy(src, dst, load_sem.at[len(loads)])
        copy.start()
        loads.append(copy)
        return copy

    def load_cols(src, dst, width):
        return [load(src.at[:, pl.ds(c, width)], dst.at[:, pl.ds(c, width)]) for c in range(0, src.shape[1], width)]

    def load_rows(src, dst, height):
        return [load(src.at[pl.ds(c, height), :], dst.at[pl.ds(c, height), :]) for c in range(0, src.shape[0], height)]

    ld_pos = load(pos_hbm, pos)
    ld_x = load(x_hbm, x)
    ld_dkv = load_rows(wdkv_hbm, wdkv, 1280)
    ld_kr = load(wkr_hbm, wkr)
    ld_gkv = load(gkv_hbm, gkv)
    ld_dq = load_rows(wdq_hbm, wdq, 640)
    ld_gq = load(gq_hbm, gq)
    ld_uq = load_rows(wuq_hbm, wuq, 256)
    ld_qr = load_rows(wqr_hbm, wqr, 384)
    ld_uk = load(wuk_hbm, wuk)
    ld_uv = load(wuv_hbm, wuv)
    ld_out = load_rows(wout_hbm, wout, 256)

    ld_pos.wait()
    pos_row = pos[...]
    freq_iota = lax.broadcasted_iota(jnp.int32, (rope // 2, rows), 0)
    inv_freq = jnp.zeros((rope // 2, rows), F32)
    for i in range(rope // 2):
        inv_freq = jnp.where(freq_iota == i, np.float32(10000.0 ** (-2.0 * i / rope)), inv_freq)
    angles = pos_row.astype(F32) * inv_freq
    reps = 128 // (rope // 2)

    def table(vals):
        tall = jnp.concatenate([vals] * reps, axis=0)
        wide = jnp.concatenate([tall, tall], axis=1)
        return jnp.transpose(wide)[:rows, :]

    cos_t = table(jnp.cos(angles))
    sin_t = table(jnp.sin(angles))
    lane = lax.broadcasted_iota(jnp.int32, (rows, 128), 1)
    lead = lax.rem(lane, rope) < rope // 2
    sin_t = jnp.where(lead, -sin_t, sin_t)

    def rope128(a):
        other = jnp.where(lead, pltpu.roll(a, 128 - rope // 2, 1), pltpu.roll(a, rope // 2, 1))
        return a * cos_t + other * sin_t

    pos_l = jnp.concatenate([pos_row] * GROUP_HEADS, axis=1)
    q_in = lax.rem(lax.broadcasted_iota(jnp.int32, (1, lanes), 1), rows)
    q_tok = jnp.where(q_in < half, half * me + q_in, half * (2 * n - 1 - me) + q_in - half)
    q_first = q_tok - pos_l
    for j in range(n):
        r = lax.broadcasted_iota(jnp.int32, (rows, lanes), 0)
        k_tok = jnp.where(r < half, half * j + r, half * (2 * n - 1 - j) + r - half)
        ok = (k_tok <= q_tok) & (k_tok >= q_first)
        bias[pl.ds(j * rows, rows), :] = jnp.where(ok, jnp.inf, -jnp.inf)

    ld_x.wait()
    for c in ld_dkv:
        c.wait()
    ld_kr.wait()
    ld_gkv.wait()
    xv = x[...]
    c_kv = rms_rows(dot_nn(xv, wdkv[...]), gkv[...])
    kr = dot_nt(xv, wkr[...])
    kr = rope128(jnp.concatenate([kr] * (128 // rope), axis=1))
    pack = kr[0:16, :]
    lane16 = lax.broadcasted_iota(jnp.int32, (16, 128), 1) // rope
    for b in range(1, rows // 16):
        pack = jnp.where(lane16 == b, kr[16 * b:16 * b + 16, :], pack)
    pack = pack.astype(BF16)
    lat[0:rows, :] = c_kv[:, :128]
    lat[rows:2 * rows, :] = c_kv[:, 128:]
    lat[2 * rows:2 * rows + 16, :] = pack
    gath[me, 0:rows, :] = c_kv[:, :128]
    gath[me, rows:2 * rows, :] = c_kv[:, 128:]
    gath[me, 2 * rows:2 * rows + 16, :] = pack

    pl.semaphore_wait(barrier, n - 1)
    sends = []
    for j in range(1, n):
        peer = lax.rem(me + j, n)
        copy = pltpu.make_async_remote_copy(
            src_ref=lat, dst_ref=gath.at[me], send_sem=send_sem.at[j - 1], recv_sem=recv_sem.at[j - 1],
            device_id={'ctx': peer}, device_id_type=MESH)
        copy.start()
        sends.append(copy)

    for c in ld_dq:
        c.wait()
    ld_gq.wait()
    c_q = rms_rows(dot_nn(xv, wdq[...]), gq[...])
    for c in ld_uq:
        c.wait()
    for c in range(0, wuq.shape[1], 512):
        qn_s[:, c:c + 512] = dot_nn(c_q, wuq[:, c:c + 512]).astype(BF16)
    for c in ld_qr:
        c.wait()
    for c in range(0, wqr.shape[1], 256):
        a = dot_nn(c_q, wqr[:, c:c + 256])
        qr_s[:, c:c + 128] = rope128(a[:, :128]).astype(BF16)
        qr_s[:, c + 128:c + 256] = rope128(a[:, 128:]).astype(BF16)

    for copy in sends:
        copy.wait()
    ld_uk.wait()
    ld_uv.wait()
    c_all = jnp.concatenate([gath[:, 0:rows, :].reshape(keys, 128), gath[:, rows:2 * rows, :].reshape(keys, 128)], axis=1)
    spread_r = lax.broadcasted_iota(jnp.int32, (128, 512), 0)
    spread_c = lax.broadcasted_iota(jnp.int32, (128, 512), 1)
    spread = (spread_r == rope * (spread_c // 128) + lax.rem(spread_c, rope)).astype(F32).astype(BF16)
    wide = dot_nn(gath[:, 2 * rows:2 * rows + 16, :].reshape(n * 16, 128), spread).astype(BF16)
    for b in range(rows // 16):
        for j in range(n):
            krep_s[j * rows + 16 * b:j * rows + 16 * b + 16, :] = wide[16 * j:16 * j + 16, 128 * b:128 * b + 128]
    for c in range(0, wuk.shape[1], gw):
        kn_s[:, c:c + gw] = dot_nn(c_all, wuk[:, c:c + gw]).astype(BF16)
    for c in range(0, wuv.shape[1], gw):
        v_s[:, c:c + gw] = dot_nn(c_all, wuv[:, c:c + gw]).astype(BF16)

    scale2 = (nope + rope) ** -0.5 * math.log2(math.e)
    lane_n = lax.broadcasted_iota(jnp.int32, (1, gw), 1) // nope
    lane_r = lax.broadcasted_iota(jnp.int32, (1, rw), 1) // rope
    mask_n = [(lane_n == h).astype(F32).astype(BF16) for h in range(GROUP_HEADS)]
    mask_r = [(lane_r == h).astype(F32).astype(BF16) for h in range(GROUP_HEADS)]
    low = lax.broadcasted_iota(jnp.int32, (rows, 128), 1) < nope

    def group(g):
        qn = qn_s[:, g * gw:(g + 1) * gw]
        qr = qr_s[:, g * rw:(g + 1) * rw]
        qn_bd = jnp.concatenate([qn * mask_n[h] for h in range(GROUP_HEADS)], axis=0)
        qr_bd = jnp.concatenate([qr * mask_r[h] for h in range(GROUP_HEADS)], axis=0)
        s = dot_nt(kn_s[:, g * gw:(g + 1) * gw], qn_bd) + dot_nt(krep_s[...], qr_bd)
        s = jnp.minimum(s, bias[...])
        m = jnp.max(s, axis=0, keepdims=True)
        p = jnp.exp2((s - m) * scale2)
        inv = 1.0 / jnp.sum(p, axis=0, keepdims=True)
        o = dot_tn(p.astype(BF16), v_s[:, g * gw:(g + 1) * gw])
        inv_t = jnp.transpose(jnp.broadcast_to(inv, (128, lanes)))
        for t in range(gw // 128):
            first, second = 2 * t * rows, (2 * t + 1) * rows
            part = jnp.where(low,
                             o[first:first + rows, 128 * t:128 * t + 128] * inv_t[first:first + rows, :],
                             o[second:second + rows, 128 * t:128 * t + 128] * inv_t[second:second + rows, :])
            o_s[:, g * gw + 128 * t:g * gw + 128 * t + 128] = part.astype(BF16)

    for g in range(groups):
        group(g)

    for c in ld_out:
        c.wait()
    ov = o_s[...]
    for c in range(0, wout.shape[1], 512):
        y_ref[:, c:c + 512] = dot_nn(ov, wout[:, c:c + 512]).astype(BF16)


def solution(mesh):
    n = mesh.shape['ctx']
    row_spec = P(('dp', 'ctx'), None)
    id_spec = P(('dp', 'ctx'))

    def per_device(x_rows, pos_rows, seg_rows, w_dq, w_uq, w_qr, w_dkv, w_kr, w_uk, w_uv, w_out, gain_q, gain_kv):
        rows, d_model = x_rows.shape
        keys = n * rows
        operands = (x_rows, pos_rows.reshape(1, rows), w_dq, w_uq, w_qr, w_dkv, w_kr.T, w_uk, w_uv, w_out,
                    gain_q.reshape(1, -1), gain_kv.reshape(1, -1))
        vm = lambda a: pltpu.VMEM(a.shape, a.dtype)
        return pl.pallas_call(
            functools.partial(kernel, n),
            out_shape=jax.ShapeDtypeStruct((rows, w_out.shape[1]), BF16),
            in_specs=[pl.BlockSpec(memory_space=pl.ANY)] * len(operands),
            out_specs=pl.BlockSpec(memory_space=pltpu.VMEM),
            scratch_shapes=[vm(a) for a in operands] + [
                pltpu.VMEM((2 * rows + 16, 128), BF16),
                pltpu.VMEM((n, 2 * rows + 16, 128), BF16),
                pltpu.VMEM((keys, GROUP_HEADS * rows), F32),
                pltpu.VMEM((rows, w_uq.shape[1]), BF16),
                pltpu.VMEM((rows, w_qr.shape[1]), BF16),
                pltpu.VMEM((keys, w_uk.shape[1]), BF16),
                pltpu.VMEM((keys, w_uv.shape[1]), BF16),
                pltpu.VMEM((keys, 128), BF16),
                pltpu.VMEM((rows, w_out.shape[0]), BF16),
                pltpu.SemaphoreType.DMA((40,)),
                pltpu.SemaphoreType.DMA((n - 1,)),
                pltpu.SemaphoreType.DMA((n - 1,)),
            ],
            compiler_params=pltpu.CompilerParams(collective_id=0, has_side_effects=True, vmem_limit_bytes=62 * 1024 * 1024),
        )(*operands)

    return jax.shard_map(per_device, mesh=mesh, in_specs=(row_spec, id_spec, id_spec) + (P(),) * 10, out_specs=row_spec, check_vma=False)
```

```python
import functools
import math

import numpy as np
import jax
import jax.numpy as jnp
from jax import lax
from jax.experimental import pallas as pl
from jax.experimental.pallas import tpu as pltpu
from jax.sharding import PartitionSpec as P

NORM_EPS = 1e-6
MESH = pl.DeviceIdType.MESH
F32 = jnp.float32
BF16 = jnp.bfloat16
GROUP_HEADS = 4


def rms_rows(vals, gain):
    mean_sq = jnp.mean(vals * vals, axis=-1, keepdims=True)
    return (vals * lax.rsqrt(mean_sq + NORM_EPS) * gain.astype(F32)).astype(BF16)


def dot_nn(a, b):
    return lax.dot_general(a, b, (((1,), (0,)), ((), ())), preferred_element_type=F32)


def dot_nt(a, b):
    return lax.dot_general(a, b, (((1,), (1,)), ((), ())), preferred_element_type=F32)


def dot_tn(a, b):
    return lax.dot_general(a, b, (((0,), (0,)), ((), ())), preferred_element_type=F32)


def kernel(n, x_hbm, pos_hbm, wdq_hbm, wuq_hbm, wqr_hbm, wdkv_hbm, wkr_hbm, wuk_hbm, wuv_hbm, wout_hbm, gq_hbm, gkv_hbm,
           y_ref, x, pos, wdq, wuq, wqr, wdkv, wkr, wuk, wuv, wout, gq, gkv,
           lat, gath, bias, qn_s, qr_s, kn_s, v_s, krep_s, o_s, load_sem, send_sem, recv_sem):
    me = lax.axis_index('ctx')
    rows = x.shape[0]
    half = rows // 2
    rank = wdkv.shape[1]
    rope = wkr.shape[0]
    num_heads = wqr.shape[1] // rope
    nope = wuq.shape[1] // num_heads
    keys = n * rows
    gw = GROUP_HEADS * nope
    rw = GROUP_HEADS * rope
    lanes = GROUP_HEADS * rows
    groups = num_heads // GROUP_HEADS

    barrier = pltpu.get_barrier_semaphore()
    for j in range(1, n):
        pl.semaphore_signal(barrier, inc=1, device_id={'ctx': lax.rem(me + j, n)}, device_id_type=MESH)

    loads = []

    def load(src, dst):
        copy = pltpu.make_async_copy(src, dst, load_sem.at[len(loads)])
        copy.start()
        loads.append(copy)
        return copy

    def load_cols(src, dst, width):
        return [load(src.at[:, pl.ds(c, width)], dst.at[:, pl.ds(c, width)]) for c in range(0, src.shape[1], width)]

    def load_rows(src, dst, height):
        return [load(src.at[pl.ds(c, height), :], dst.at[pl.ds(c, height), :]) for c in range(0, src.shape[0], height)]

    ld_pos = load(pos_hbm, pos)
    ld_x = load(x_hbm, x)
    ld_dkv = load_rows(wdkv_hbm, wdkv, 1280)
    ld_kr = load(wkr_hbm, wkr)
    ld_gkv = load(gkv_hbm, gkv)
    ld_dq = load_rows(wdq_hbm, wdq, 640)
    ld_gq = load(gq_hbm, gq)
    ld_uq = load_rows(wuq_hbm, wuq, 256)
    ld_qr = load_rows(wqr_hbm, wqr, 384)
    ld_uk = load(wuk_hbm, wuk)
    ld_uv = load(wuv_hbm, wuv)
    ld_out = load_rows(wout_hbm, wout, 256)

    ld_pos.wait()
    pos_row = pos[...]
    freq_iota = lax.broadcasted_iota(jnp.int32, (rope // 2, rows), 0)
    inv_freq = jnp.zeros((rope // 2, rows), F32)
    for i in range(rope // 2):
        inv_freq = jnp.where(freq_iota == i, np.float32(10000.0 ** (-2.0 * i / rope)), inv_freq)
    angles = pos_row.astype(F32) * inv_freq
    reps = 128 // (rope // 2)

    def table(vals):
        tall = jnp.concatenate([vals] * reps, axis=0)
        wide = jnp.concatenate([tall, tall], axis=1)
        return jnp.transpose(wide)[:rows, :]

    cos_t = table(jnp.cos(angles))
    sin_t = table(jnp.sin(angles))
    lane = lax.broadcasted_iota(jnp.int32, (rows, 128), 1)
    lead = lax.rem(lane, rope) < rope // 2
    sin_t = jnp.where(lead, -sin_t, sin_t)

    def rope128(a):
        other = jnp.where(lead, pltpu.roll(a, 128 - rope // 2, 1), pltpu.roll(a, rope // 2, 1))
        return a * cos_t + other * sin_t

    pos_l = jnp.concatenate([pos_row] * GROUP_HEADS, axis=1)
    q_in = lax.rem(lax.broadcasted_iota(jnp.int32, (1, lanes), 1), rows)
    q_tok = jnp.where(q_in < half, half * me + q_in, half * (2 * n - 1 - me) + q_in - half)
    q_first = q_tok - pos_l
    for j in range(n):
        r = lax.broadcasted_iota(jnp.int32, (rows, lanes), 0)
        k_tok = jnp.where(r < half, half * j + r, half * (2 * n - 1 - j) + r - half)
        ok = (k_tok <= q_tok) & (k_tok >= q_first)
        bias[pl.ds(j * rows, rows), :] = jnp.where(ok, jnp.inf, -jnp.inf)

    ld_x.wait()
    for c in ld_dkv:
        c.wait()
    ld_kr.wait()
    ld_gkv.wait()
    xv = x[...]
    c_kv = rms_rows(dot_nn(xv, wdkv[...]), gkv[...].reshape(1, rank))
    kr = dot_nt(xv, wkr[...])
    kr = rope128(jnp.concatenate([kr] * (128 // rope), axis=1))
    pack = kr[0:16, :]
    lane16 = lax.broadcasted_iota(jnp.int32, (16, 128), 1) // rope
    for b in range(1, rows // 16):
        pack = jnp.where(lane16 == b, kr[16 * b:16 * b + 16, :], pack)
    pack = pack.astype(BF16)
    lat[0:rows, :] = c_kv[:, :128]
    lat[rows:2 * rows, :] = c_kv[:, 128:]
    lat[2 * rows:2 * rows + 16, :] = pack
    gath[me, 0:rows, :] = c_kv[:, :128]
    gath[me, rows:2 * rows, :] = c_kv[:, 128:]
    gath[me, 2 * rows:2 * rows + 16, :] = pack

    pl.semaphore_wait(barrier, n - 1)
    sends = []
    for j in range(1, n):
        peer = lax.rem(me + j, n)
        copy = pltpu.make_async_remote_copy(
            src_ref=lat, dst_ref=gath.at[me], send_sem=send_sem.at[j - 1], recv_sem=recv_sem.at[j - 1],
            device_id={'ctx': peer}, device_id_type=MESH)
        copy.start()
        sends.append(copy)

    for c in ld_dq:
        c.wait()
    ld_gq.wait()
    c_q = rms_rows(dot_nn(xv, wdq[...]), gq[...].reshape(1, wdq.shape[1]))
    for c in ld_uq:
        c.wait()
    for c in range(0, wuq.shape[1], 512):
        qn_s[:, c:c + 512] = dot_nn(c_q, wuq[:, c:c + 512]).astype(BF16)
    for c in ld_qr:
        c.wait()
    for c in range(0, wqr.shape[1], 256):
        a = dot_nn(c_q, wqr[:, c:c + 256])
        qr_s[:, c:c + 128] = rope128(a[:, :128]).astype(BF16)
        qr_s[:, c + 128:c + 256] = rope128(a[:, 128:]).astype(BF16)

    for copy in sends:
        copy.wait()
    ld_uk.wait()
    ld_uv.wait()
    c_all = jnp.concatenate([gath[:, 0:rows, :].reshape(keys, 128), gath[:, rows:2 * rows, :].reshape(keys, 128)], axis=1)
    spread_r = lax.broadcasted_iota(jnp.int32, (128, 512), 0)
    spread_c = lax.broadcasted_iota(jnp.int32, (128, 512), 1)
    spread = (spread_r == rope * (spread_c // 128) + lax.rem(spread_c, rope)).astype(F32).astype(BF16)
    wide = dot_nn(gath[:, 2 * rows:2 * rows + 16, :].reshape(n * 16, 128), spread).astype(BF16)
    for b in range(rows // 16):
        for j in range(n):
            krep_s[j * rows + 16 * b:j * rows + 16 * b + 16, :] = wide[16 * j:16 * j + 16, 128 * b:128 * b + 128]
    for c in range(0, wuk.shape[1], gw):
        kn_s[:, c:c + gw] = dot_nn(c_all, wuk[:, c:c + gw]).astype(BF16)
    for c in range(0, wuv.shape[1], gw):
        v_s[:, c:c + gw] = dot_nn(c_all, wuv[:, c:c + gw]).astype(BF16)

    scale2 = (nope + rope) ** -0.5 * math.log2(math.e)
    lane_n = lax.broadcasted_iota(jnp.int32, (1, gw), 1) // nope
    lane_r = lax.broadcasted_iota(jnp.int32, (1, rw), 1) // rope
    mask_n = [(lane_n == h).astype(F32).astype(BF16) for h in range(GROUP_HEADS)]
    mask_r = [(lane_r == h).astype(F32).astype(BF16) for h in range(GROUP_HEADS)]
    low = lax.broadcasted_iota(jnp.int32, (rows, 128), 1) < nope

    def group(g):
        qn = qn_s[:, g * gw:(g + 1) * gw]
        qr = qr_s[:, g * rw:(g + 1) * rw]
        qn_bd = jnp.concatenate([qn * mask_n[h] for h in range(GROUP_HEADS)], axis=0)
        qr_bd = jnp.concatenate([qr * mask_r[h] for h in range(GROUP_HEADS)], axis=0)
        s = dot_nt(kn_s[:, g * gw:(g + 1) * gw], qn_bd) + dot_nt(krep_s[...], qr_bd)
        s = jnp.minimum(s, bias[...])
        m = jnp.max(s, axis=0, keepdims=True)
        p = jnp.exp2((s - m) * scale2)
        inv = 1.0 / jnp.sum(p, axis=0, keepdims=True)
        o = dot_tn(p.astype(BF16), v_s[:, g * gw:(g + 1) * gw])
        inv_t = jnp.transpose(jnp.broadcast_to(inv, (128, lanes)))
        for t in range(gw // 128):
            first, second = 2 * t * rows, (2 * t + 1) * rows
            part = jnp.where(low,
                             o[first:first + rows, 128 * t:128 * t + 128] * inv_t[first:first + rows, :],
                             o[second:second + rows, 128 * t:128 * t + 128] * inv_t[second:second + rows, :])
            o_s[:, g * gw + 128 * t:g * gw + 128 * t + 128] = part.astype(BF16)

    for g in range(groups):
        group(g)

    for c in ld_out:
        c.wait()
    ov = o_s[...]
    for c in range(0, wout.shape[1], 512):
        y_ref[:, c:c + 512] = dot_nn(ov, wout[:, c:c + 512]).astype(BF16)


def solution(mesh):
    n = mesh.shape['ctx']
    row_spec = P(('dp', 'ctx'), None)
    id_spec = P(('dp', 'ctx'))

    def per_device(x_rows, pos_rows, seg_rows, w_dq, w_uq, w_qr, w_dkv, w_kr, w_uk, w_uv, w_out, gain_q, gain_kv):
        rows, d_model = x_rows.shape
        keys = n * rows
        operands = (x_rows, pos_rows.reshape(1, rows), w_dq, w_uq, w_qr, w_dkv, w_kr.T, w_uk, w_uv, w_out,
                    gain_q, gain_kv)
        operands = tuple(pltpu.with_memory_space_constraint(a, pltpu.HBM) for a in operands)
        vm = lambda a: pltpu.VMEM(a.shape, a.dtype)
        return pl.pallas_call(
            functools.partial(kernel, n),
            out_shape=jax.ShapeDtypeStruct((rows, w_out.shape[1]), BF16),
            in_specs=[pl.BlockSpec(memory_space=pl.ANY)] * len(operands),
            out_specs=pl.BlockSpec(memory_space=pltpu.VMEM),
            scratch_shapes=[vm(a) for a in operands] + [
                pltpu.VMEM((2 * rows + 16, 128), BF16),
                pltpu.VMEM((n, 2 * rows + 16, 128), BF16),
                pltpu.VMEM((keys, GROUP_HEADS * rows), F32),
                pltpu.VMEM((rows, w_uq.shape[1]), BF16),
                pltpu.VMEM((rows, w_qr.shape[1]), BF16),
                pltpu.VMEM((keys, w_uk.shape[1]), BF16),
                pltpu.VMEM((keys, w_uv.shape[1]), BF16),
                pltpu.VMEM((keys, 128), BF16),
                pltpu.VMEM((rows, w_out.shape[0]), BF16),
                pltpu.SemaphoreType.DMA((40,)),
                pltpu.SemaphoreType.DMA((n - 1,)),
                pltpu.SemaphoreType.DMA((n - 1,)),
            ],
            compiler_params=pltpu.CompilerParams(collective_id=0, has_side_effects=True, vmem_limit_bytes=42 * 1024 * 1024),
        )(*operands)

    return jax.shard_map(per_device, mesh=mesh, in_specs=(row_spec, id_spec, id_spec) + (P(),) * 10, out_specs=row_spec, check_vma=False)
```

```python
import functools
import math

import numpy as np
import jax
import jax.numpy as jnp
from jax import lax
from jax.experimental import pallas as pl
from jax.experimental.pallas import tpu as pltpu
from jax.sharding import PartitionSpec as P

NORM_EPS = 1e-6
MESH = pl.DeviceIdType.MESH
F32 = jnp.float32
BF16 = jnp.bfloat16
LANES = 128


def rms_rows(vals, gain):
    mean_sq = jnp.mean(vals * vals, axis=-1, keepdims=True)
    return (vals * lax.rsqrt(mean_sq + NORM_EPS) * gain.astype(F32)).astype(BF16)


def dot_nn(a, b):
    return lax.dot_general(a, b, (((1,), (0,)), ((), ())), preferred_element_type=F32)


def dot_nt(a, b):
    return lax.dot_general(a, b, (((1,), (1,)), ((), ())), preferred_element_type=F32)


def dot_tt(a, b):
    return lax.dot_general(a, b, (((0,), (1,)), ((), ())), preferred_element_type=F32)


def iota(shape, axis):
    return lax.broadcasted_iota(jnp.int32, shape, axis)


def kernel(n, rows, rope, nope, x_hbm, pos_hbm, wdq_hbm, wuq_hbm, wqr_hbm, wdkv_hbm, wkr_hbm, wuk_hbm, wuv_hbm, wout_hbm,
           gq_hbm, gkv_hbm, y_ref, x, pos, wdq, wuq, wqr, wdkv, wkr, wuk, wuv, wout, gq, gkv,
           lat, gath, bias, qbd, kn_s, vt_s, m_s, l_s, acc_s, o_own, o_out, o_in, y_acc,
           load_sem, send_sem, recv_sem, pair_send, pair_recv):
    me = lax.axis_index('ctx')
    core = lax.rem(me, 2)
    chip = me // 2
    partner = me + 1 - 2 * core
    half = rows // 2
    rank = wdkv.shape[1]
    pair = 2 * rows
    cols = wuq.shape[1]
    groups = cols // LANES
    part = n // 2
    keys = part * rows
    tables = rope // 2

    barrier = pltpu.get_barrier_semaphore()
    for j in range(1, n):
        pl.semaphore_signal(barrier, inc=1, device_id={'ctx': lax.rem(me + j, n)}, device_id_type=MESH)

    loads = []

    def load(src, dst):
        copy = pltpu.make_async_copy(src, dst, load_sem.at[len(loads)])
        copy.start()
        loads.append(copy)
        return copy

    def load_rows(src, dst, height, first=0):
        return [load(src.at[pl.ds(first + c, height), :], dst.at[pl.ds(c, height), :]) for c in range(0, dst.shape[0], height)]

    mine = pl.ds(pl.multiple_of(core * rows, rows), rows)
    head_cols = pl.ds(pl.multiple_of(core * cols, LANES), cols)
    rope_cols = pl.ds(pl.multiple_of(core * wqr.shape[1], LANES), wqr.shape[1])
    ld_pos = load(pos_hbm, pos.at[core])
    ld_x = load(x_hbm, x.at[mine, :])
    ld_dkv = load_rows(wdkv_hbm, wdkv, 1280)
    ld_kr = load(wkr_hbm, wkr)
    ld_gkv = load(gkv_hbm, gkv)
    ld_dq = load_rows(wdq_hbm, wdq, 640)
    ld_gq = load(gq_hbm, gq)
    ld_uq = load(wuq_hbm.at[:, head_cols], wuq)
    ld_qr = load(wqr_hbm.at[:, rope_cols], wqr)
    ld_uk = load(wuk_hbm.at[:, head_cols], wuk)
    ld_uv = load(wuv_hbm.at[:, head_cols], wuv)
    row_a = pl.multiple_of(core * cols, LANES)
    row_b = pl.multiple_of((1 - core) * cols, LANES)
    ld_out = [load(wout_hbm.at[pl.ds(row_a + c, 256), :], wout.at[pl.ds(c, 256), :]) for c in range(0, cols, 256)]
    ld_out += [load(wout_hbm.at[pl.ds(row_b + c, 256), :], wout.at[pl.ds(cols + c, 256), :]) for c in range(0, cols, 256)]

    def rope_tables(pos_row):
        width = pos_row.shape[1]
        freq = iota((tables, width), 0)
        inv_freq = jnp.zeros((tables, width), F32)
        for i in range(tables):
            inv_freq = jnp.where(freq == i, np.float32(10000.0 ** (-2.0 * i / rope)), inv_freq)
        angles = pos_row.astype(F32) * inv_freq

        def table(vals):
            tall = jnp.concatenate([vals] * (LANES // tables), axis=0)
            if width < LANES:
                tall = jnp.concatenate([tall] * (LANES // width), axis=1)
            return jnp.transpose(tall)[:width, :]

        lead = lax.rem(iota((width, LANES), 1), rope) < tables
        cos_t, sin_t = table(jnp.cos(angles)), table(jnp.sin(angles))
        return cos_t, jnp.where(lead, -sin_t, sin_t), lead

    def rotate(a, tabs):
        cos_t, sin_t, lead = tabs
        other = jnp.where(lead, pltpu.roll(a, LANES - tables, 1), pltpu.roll(a, tables, 1))
        return a * cos_t + other * sin_t

    ld_pos.wait()
    tabs = rope_tables(pos[core])
    ld_x.wait()
    for c in ld_dkv:
        c.wait()
    ld_kr.wait()
    ld_gkv.wait()
    xv = x[mine, :]
    c_kv = rms_rows(dot_nn(xv, wdkv[...]), gkv[...].reshape(1, rank))
    kr = dot_nt(xv, wkr[...])
    kr = rotate(jnp.concatenate([kr] * (LANES // rope), axis=1), tabs)
    pack = kr[0:16, :]
    lane16 = iota((16, LANES), 1) // rope
    for b in range(1, rows // 16):
        pack = jnp.where(lane16 == b, kr[16 * b:16 * b + 16, :], pack)
    pack = pack.astype(BF16)
    lat[0:rows, :] = c_kv[:, :LANES]
    lat[rows:2 * rows, :] = c_kv[:, LANES:]
    lat[2 * rows:2 * rows + 16, :] = pack
    gath[me, 0:rows, :] = c_kv[:, :LANES]
    gath[me, rows:2 * rows, :] = c_kv[:, LANES:]
    gath[me, 2 * rows:2 * rows + 16, :] = pack

    pl.semaphore_wait(barrier, n - 1)
    sends = []
    for j in range(1, n):
        flip_chip, flip_core = j // 2, j % 2
        bit0 = lax.rem(chip, 2)
        bit1 = chip // 2
        peer_chip = (bit0 + (flip_chip % 2) * (1 - 2 * bit0)) + 2 * (bit1 + (flip_chip // 2) * (1 - 2 * bit1))
        peer = 2 * peer_chip + core + flip_core * (1 - 2 * core)
        copy = pltpu.make_async_remote_copy(
            src_ref=lat, dst_ref=gath.at[me], send_sem=send_sem.at[j - 1], recv_sem=recv_sem.at[j - 1],
            device_id={'ctx': peer}, device_id_type=MESH)
        copy.start()
        sends.append(copy)

    def to_partner(src, dst, index):
        copy = pltpu.make_async_remote_copy(
            src_ref=src, dst_ref=dst, send_sem=pair_send.at[index], recv_sem=pair_recv.at[index],
            device_id={'ctx': partner}, device_id_type=MESH)
        copy.start()
        return copy

    pair_x = to_partner(x.at[mine, :], x.at[mine, :], 0)
    pair_pos = to_partner(pos.at[core], pos.at[core], 1)
    qbd[...] = jnp.zeros_like(qbd)

    pair_pos.wait()
    pos_row = jnp.concatenate([pos[0], pos[1]], axis=1)
    tabs = rope_tables(pos_row)
    pair_x.wait()
    for c in ld_dq:
        c.wait()
    ld_gq.wait()
    c_q = rms_rows(dot_nn(x[...], wdq[...]), gq[...].reshape(1, wdq.shape[1]))
    ld_uq.wait()
    for c in range(0, cols, 256):
        q = dot_nn(c_q, wuq[:, c:c + 256]).astype(BF16)
        for t in range(2):
            qt = jnp.transpose(q[:, LANES * t:LANES * t + LANES])
            g = c // LANES + t
            qbd[g, 0:nope, 0:pair] = qt[0:nope, :]
            qbd[g, nope:2 * nope, pair:2 * pair] = qt[nope:2 * nope, :]
    ld_qr.wait()
    qr_all = dot_nn(c_q, wqr[...])
    for t in range(groups // 2):
        qt = jnp.transpose(rotate(qr_all[:, LANES * t:LANES * t + LANES], tabs).astype(BF16))
        for k in range(4):
            lo = (k % 2) * pair
            qbd[2 * t + k // 2, LANES + rope * k:LANES + rope * k + rope, lo:lo + pair] = qt[rope * k:rope * k + rope, :]

    near = me // part
    q_in = lax.rem(iota((1, pair), 1), rows)
    q_dev = 2 * chip + iota((1, pair), 1) // rows
    q_tok = jnp.where(q_in < half, half * q_dev + q_in, half * (2 * n - 1 - q_dev) + q_in - half)
    q_first = q_tok - pos_row
    sides = (near, 1 - near)
    for side in range(2):
        r = iota((keys, pair), 0)
        k_in = lax.rem(r, rows)
        k_dev = part * sides[side] + r // rows
        k_tok = jnp.where(k_in < half, half * k_dev + k_in, half * (2 * n - 1 - k_dev) + k_in - half)
        ok = (k_tok <= q_tok) & (k_tok >= q_first)
        bias[side] = jnp.where(ok, jnp.inf, -jnp.inf)

    spread_r = iota((LANES, 4 * LANES), 0)
    spread_c = iota((LANES, 4 * LANES), 1)
    spread = (spread_r == rope * (spread_c // LANES) + lax.rem(spread_c, rope)).astype(F32).astype(BF16)
    scale2 = (nope + rope) ** -0.5 * math.log2(math.e)
    ld_uk.wait()
    ld_uv.wait()

    def attend(side):
        slots = pl.ds(part * sides[side], part)
        c_all = jnp.concatenate([gath[slots, 0:rows, :].reshape(keys, LANES), gath[slots, rows:2 * rows, :].reshape(keys, LANES)], axis=1)
        wide = dot_nn(gath[slots, 2 * rows:2 * rows + 16, :].reshape(part * 16, LANES), spread).astype(BF16)
        krep = jnp.concatenate([wide[16 * j:16 * j + 16, LANES * b:LANES * b + LANES] for j in range(part) for b in range(rows // 16)], axis=0)
        for c in range(0, cols, 256):
            kn_s[side, :, c:c + 256] = dot_nn(c_all, wuk[:, c:c + 256]).astype(BF16)
            vt_s[side, c:c + 256, :] = dot_tt(wuv[:, c:c + 256], c_all).astype(BF16)
        for g in range(groups):
            lanes = slice(g * LANES, (g + 1) * LANES)
            s = dot_nn(jnp.concatenate([kn_s[side, :, lanes], krep], axis=1), qbd[g])
            limit = bias[side]
            s = jnp.minimum(s, jnp.concatenate([limit, limit], axis=1))
            m = jnp.max(s, axis=0, keepdims=True)
            if side == 1:
                m_old = m_s[g]
                m = jnp.maximum(m, m_old)
            p = jnp.exp2((s - m) * scale2)
            l = jnp.sum(p, axis=0, keepdims=True)
            o = dot_nn(vt_s[side, lanes, :], p.astype(BF16))
            o = [o[:nope, :pair], o[nope:, pair:]]
            if side == 0:
                m_s[g] = m
                l_s[g] = l
                acc_s[g, :nope, :] = o[0]
                acc_s[g, nope:, :] = o[1]
            else:
                alpha = jnp.exp2((m_old - m) * scale2)
                inv = 1.0 / (l_s[g] * alpha + l)
                o = [(acc_s[g, h * nope:(h + 1) * nope, :] * alpha[:, h * pair:(h + 1) * pair] + o[h])
                     * inv[:, h * pair:(h + 1) * pair] for h in range(2)]
                ot = jnp.transpose(jnp.concatenate(o, axis=0).astype(BF16))
                both = [ot[:rows, :], ot[rows:, :]]
                o_own[:, lanes] = jnp.where(core == 0, both[0], both[1])
                o_out[:, lanes] = jnp.where(core == 0, both[1], both[0])

    for c in range(3):
        sends[c].wait()
    attend(0)
    for c in range(3, n - 1):
        sends[c].wait()
    attend(1)

    pair_o = to_partner(o_out, o_in, 2)
    for c in ld_out:
        c.wait()
    ov = o_own[...]
    for c in range(0, y_ref.shape[1], 512):
        y_acc[:, c:c + 512] = dot_nn(ov, wout[:cols, c:c + 512])
    pair_o.wait()
    ov = o_in[...]
    for c in range(0, y_ref.shape[1], 512):
        y_ref[:, c:c + 512] = (y_acc[:, c:c + 512] + dot_nn(ov, wout[cols:, c:c + 512])).astype(BF16)


def solution(mesh):
    n = mesh.shape['ctx']
    row_spec = P(('dp', 'ctx'), None)
    id_spec = P(('dp', 'ctx'))

    def per_device(x_rows, pos_rows, seg_rows, w_dq, w_uq, w_qr, w_dkv, w_kr, w_uk, w_uv, w_out, gain_q, gain_kv):
        rows, d_model = x_rows.shape
        rope = w_kr.shape[1]
        nope = w_uq.shape[1] * rope // w_qr.shape[1]
        cols = w_uq.shape[1] // 2
        groups = cols // LANES
        keys = n // 2 * rows
        operands = (x_rows, pos_rows.reshape(1, rows), w_dq, w_uq, w_qr, w_dkv, w_kr.T, w_uk, w_uv, w_out, gain_q, gain_kv)
        operands = tuple(pltpu.with_memory_space_constraint(a, pltpu.HBM) for a in operands)
        vm = lambda a: pltpu.VMEM(a.shape, a.dtype)
        cut = lambda a: pltpu.VMEM((a.shape[0], a.shape[1] // 2), a.dtype)
        return pl.pallas_call(
            functools.partial(kernel, n, rows, rope, nope),
            out_shape=jax.ShapeDtypeStruct((rows, w_out.shape[1]), BF16),
            in_specs=[pl.BlockSpec(memory_space=pl.ANY)] * len(operands),
            out_specs=pl.BlockSpec(memory_space=pltpu.VMEM),
            scratch_shapes=[
                pltpu.VMEM((2 * rows, d_model), BF16),
                pltpu.VMEM((2, 1, rows), jnp.int32),
                vm(w_dq), cut(w_uq), cut(w_qr), vm(w_dkv), vm(w_kr.T), cut(w_uk), cut(w_uv), vm(w_out), vm(gain_q), vm(gain_kv),
                pltpu.VMEM((2 * rows + 16, LANES), BF16),
                pltpu.VMEM((n, 2 * rows + 16, LANES), BF16),
                pltpu.VMEM((2, keys, 2 * rows), F32),
                pltpu.VMEM((groups, 2 * LANES, 4 * rows), BF16),
                pltpu.VMEM((2, keys, cols), BF16),
                pltpu.VMEM((2, cols, keys), BF16),
                pltpu.VMEM((groups, 1, 4 * rows), F32),
                pltpu.VMEM((groups, 1, 4 * rows), F32),
                pltpu.VMEM((groups, 2 * nope, 2 * rows), F32),
                pltpu.VMEM((rows, cols), BF16),
                pltpu.VMEM((rows, cols), BF16),
                pltpu.VMEM((rows, cols), BF16),
                pltpu.VMEM((rows, w_out.shape[1]), F32),
                pltpu.SemaphoreType.DMA((40,)),
                pltpu.SemaphoreType.DMA((n - 1,)),
                pltpu.SemaphoreType.DMA((n - 1,)),
                pltpu.SemaphoreType.DMA((3,)),
                pltpu.SemaphoreType.DMA((3,)),
            ],
            compiler_params=pltpu.CompilerParams(collective_id=0, has_side_effects=True, vmem_limit_bytes=42 * 1024 * 1024),
        )(*operands)

    return jax.shard_map(per_device, mesh=mesh, in_specs=(row_spec, id_spec, id_spec) + (P(),) * 10, out_specs=row_spec, check_vma=False)
```

```python
import functools
import math

import numpy as np
import jax
import jax.numpy as jnp
from jax import lax
from jax.experimental import pallas as pl
from jax.experimental.pallas import tpu as pltpu
from jax.sharding import PartitionSpec as P

NORM_EPS = 1e-6
MESH = pl.DeviceIdType.MESH
F32 = jnp.float32
BF16 = jnp.bfloat16
LANES = 128
AHEAD = 2
SLOTS = AHEAD + 1


def rms_rows(vals, gain):
    mean_sq = jnp.mean(vals * vals, axis=-1, keepdims=True)
    return (vals * lax.rsqrt(mean_sq + NORM_EPS) * gain.astype(F32)).astype(BF16)


def dot_nn(a, b):
    return lax.dot_general(a, b, (((1,), (0,)), ((), ())), preferred_element_type=F32)


def dot_nt(a, b):
    return lax.dot_general(a, b, (((1,), (1,)), ((), ())), preferred_element_type=F32)


def dot_tt(a, b):
    return lax.dot_general(a, b, (((0,), (1,)), ((), ())), preferred_element_type=F32)


def iota(shape, axis):
    return lax.broadcasted_iota(jnp.int32, shape, axis)


def kernel(n, rows, rope, nope, x_hbm, pos_hbm, wdq_hbm, wuq_hbm, wqr_hbm, wdkv_hbm, wkr_hbm, wuk_hbm, wuv_hbm, wout_hbm,
           gq_hbm, gkv_hbm, y_ref, x, pos, wdq, wuq, wqr, wdkv, wkr, wuk, wuv, wout, gq, gkv,
           lat, gath, bias, qbd, kn_s, vt_s, m_s, l_s, acc_s, o_own, o_out, o_in, y_acc, s_s,
           load_sem, send_sem, recv_sem, pair_send, pair_recv):
    me = lax.axis_index('ctx')
    core = lax.rem(me, 2)
    chip = me // 2
    partner = me + 1 - 2 * core
    half = rows // 2
    rank = wdkv.shape[1]
    pair = 2 * rows
    cols = wuq.shape[1]
    groups = cols // LANES
    part = n // 2
    keys = part * rows
    tables = rope // 2

    barrier = pltpu.get_barrier_semaphore()
    for j in range(1, n):
        pl.semaphore_signal(barrier, inc=1, device_id={'ctx': lax.rem(me + j, n)}, device_id_type=MESH)

    loads = []

    def load(src, dst):
        copy = pltpu.make_async_copy(src, dst, load_sem.at[len(loads)])
        copy.start()
        loads.append(copy)
        return copy

    def load_rows(src, dst, height, first=0):
        return [load(src.at[pl.ds(first + c, height), :], dst.at[pl.ds(c, height), :]) for c in range(0, dst.shape[0], height)]

    mine = pl.ds(pl.multiple_of(core * rows, rows), rows)
    head_cols = pl.ds(pl.multiple_of(core * cols, LANES), cols)
    rope_cols = pl.ds(pl.multiple_of(core * wqr.shape[1], LANES), wqr.shape[1])
    ld_pos = load(pos_hbm, pos.at[core])
    ld_x = load(x_hbm, x.at[mine, :])
    ld_dkv = load_rows(wdkv_hbm, wdkv, 1280)
    ld_kr = load(wkr_hbm, wkr)
    ld_gkv = load(gkv_hbm, gkv)
    ld_dq = load_rows(wdq_hbm, wdq, 640)
    ld_gq = load(gq_hbm, gq)
    ld_uq = load(wuq_hbm.at[:, head_cols], wuq)
    ld_qr = load(wqr_hbm.at[:, rope_cols], wqr)
    ld_uk = load(wuk_hbm.at[:, head_cols], wuk)
    ld_uv = load(wuv_hbm.at[:, head_cols], wuv)
    row_a = pl.multiple_of(core * cols, LANES)
    row_b = pl.multiple_of((1 - core) * cols, LANES)
    ld_out = [load(wout_hbm.at[pl.ds(row_a + c, 256), :], wout.at[pl.ds(c, 256), :]) for c in range(0, cols, 256)]
    ld_out += [load(wout_hbm.at[pl.ds(row_b + c, 256), :], wout.at[pl.ds(cols + c, 256), :]) for c in range(0, cols, 256)]

    def rope_tables(pos_row):
        width = pos_row.shape[1]
        freq = iota((tables, width), 0)
        inv_freq = jnp.zeros((tables, width), F32)
        for i in range(tables):
            inv_freq = jnp.where(freq == i, np.float32(10000.0 ** (-2.0 * i / rope)), inv_freq)
        angles = pos_row.astype(F32) * inv_freq

        def table(vals):
            tall = jnp.concatenate([vals] * (LANES // tables), axis=0)
            if width < LANES:
                tall = jnp.concatenate([tall] * (LANES // width), axis=1)
            return jnp.transpose(tall)[:width, :]

        lead = lax.rem(iota((width, LANES), 1), rope) < tables
        cos_t, sin_t = table(jnp.cos(angles)), table(jnp.sin(angles))
        return cos_t, jnp.where(lead, -sin_t, sin_t), lead

    def rotate(a, tabs):
        cos_t, sin_t, lead = tabs
        other = jnp.where(lead, pltpu.roll(a, LANES - tables, 1), pltpu.roll(a, tables, 1))
        return a * cos_t + other * sin_t

    ld_pos.wait()
    tabs = rope_tables(pos[core])
    ld_x.wait()
    for c in ld_dkv:
        c.wait()
    ld_kr.wait()
    ld_gkv.wait()
    xv = x[mine, :]
    c_kv = rms_rows(dot_nn(xv, wdkv[...]), gkv[...].reshape(1, rank))
    kr = dot_nt(xv, wkr[...])
    kr = rotate(jnp.concatenate([kr] * (LANES // rope), axis=1), tabs)
    pack = kr[0:16, :]
    lane16 = iota((16, LANES), 1) // rope
    for b in range(1, rows // 16):
        pack = jnp.where(lane16 == b, kr[16 * b:16 * b + 16, :], pack)
    pack = pack.astype(BF16)
    lat[0:rows, :] = c_kv[:, :LANES]
    lat[rows:2 * rows, :] = c_kv[:, LANES:]
    lat[2 * rows:2 * rows + 16, :] = pack
    gath[me, 0:rows, :] = c_kv[:, :LANES]
    gath[me, rows:2 * rows, :] = c_kv[:, LANES:]
    gath[me, 2 * rows:2 * rows + 16, :] = pack

    pl.semaphore_wait(barrier, n - 1)
    sends = []
    for j in range(1, n):
        flip_chip, flip_core = j // 2, j % 2
        bit0 = lax.rem(chip, 2)
        bit1 = chip // 2
        peer_chip = (bit0 + (flip_chip % 2) * (1 - 2 * bit0)) + 2 * (bit1 + (flip_chip // 2) * (1 - 2 * bit1))
        peer = 2 * peer_chip + core + flip_core * (1 - 2 * core)
        copy = pltpu.make_async_remote_copy(
            src_ref=lat, dst_ref=gath.at[me], send_sem=send_sem.at[j - 1], recv_sem=recv_sem.at[j - 1],
            device_id={'ctx': peer}, device_id_type=MESH)
        copy.start()
        sends.append(copy)

    def to_partner(src, dst, index):
        copy = pltpu.make_async_remote_copy(
            src_ref=src, dst_ref=dst, send_sem=pair_send.at[index], recv_sem=pair_recv.at[index],
            device_id={'ctx': partner}, device_id_type=MESH)
        copy.start()
        return copy

    pair_x = to_partner(x.at[mine, :], x.at[mine, :], 0)
    pair_pos = to_partner(pos.at[core], pos.at[core], 1)
    qbd[...] = jnp.zeros_like(qbd)

    pair_pos.wait()
    pos_row = jnp.concatenate([pos[0], pos[1]], axis=1)
    tabs = rope_tables(pos_row)
    pair_x.wait()
    for c in ld_dq:
        c.wait()
    ld_gq.wait()
    c_q = rms_rows(dot_nn(x[...], wdq[...]), gq[...].reshape(1, wdq.shape[1]))
    ld_uq.wait()
    for c in range(0, cols, 256):
        q = dot_nn(c_q, wuq[:, c:c + 256]).astype(BF16)
        for t in range(2):
            qt = jnp.transpose(q[:, LANES * t:LANES * t + LANES])
            g = c // LANES + t
            qbd[g, 0:nope, 0:pair] = qt[0:nope, :]
            qbd[g, nope:2 * nope, pair:2 * pair] = qt[nope:2 * nope, :]
    ld_qr.wait()
    qr_all = dot_nn(c_q, wqr[...])
    for t in range(groups // 2):
        qt = jnp.transpose(rotate(qr_all[:, LANES * t:LANES * t + LANES], tabs).astype(BF16))
        for k in range(4):
            lo = (k % 2) * pair
            qbd[2 * t + k // 2, LANES + rope * k:LANES + rope * k + rope, lo:lo + pair] = qt[rope * k:rope * k + rope, :]

    near = me // part
    q_in = lax.rem(iota((1, pair), 1), rows)
    q_dev = 2 * chip + iota((1, pair), 1) // rows
    q_tok = jnp.where(q_in < half, half * q_dev + q_in, half * (2 * n - 1 - q_dev) + q_in - half)
    q_first = q_tok - pos_row
    sides = (near, 1 - near)
    for side in range(2):
        r = iota((keys, pair), 0)
        k_in = lax.rem(r, rows)
        k_dev = part * sides[side] + r // rows
        k_tok = jnp.where(k_in < half, half * k_dev + k_in, half * (2 * n - 1 - k_dev) + k_in - half)
        ok = (k_tok <= q_tok) & (k_tok >= q_first)
        bias[side] = jnp.where(ok, jnp.inf, -jnp.inf)

    spread_r = iota((LANES, 4 * LANES), 0)
    spread_c = iota((LANES, 4 * LANES), 1)
    spread = (spread_r == rope * (spread_c // LANES) + lax.rem(spread_c, rope)).astype(F32).astype(BF16)
    scale2 = (nope + rope) ** -0.5 * math.log2(math.e)
    ld_uk.wait()
    ld_uv.wait()

    def attend(side):
        slots = pl.ds(part * sides[side], part)
        c_all = jnp.concatenate([gath[slots, 0:rows, :].reshape(keys, LANES), gath[slots, rows:2 * rows, :].reshape(keys, LANES)], axis=1)
        wide = dot_nn(gath[slots, 2 * rows:2 * rows + 16, :].reshape(part * 16, LANES), spread).astype(BF16)
        krep = jnp.concatenate([wide[16 * j:16 * j + 16, LANES * b:LANES * b + LANES] for j in range(part) for b in range(rows // 16)], axis=0)
        def project(c):
            kn_s[side, :, c:c + 256] = dot_nn(c_all, wuk[:, c:c + 256]).astype(BF16)
            vt_s[side, c:c + 256, :] = dot_tt(wuv[:, c:c + 256], c_all).astype(BF16)

        def score(g):
            s = dot_nn(jnp.concatenate([kn_s[side, :, g * LANES:(g + 1) * LANES], krep], axis=1), qbd[g])
            limit = bias[side]
            s = jnp.minimum(s, jnp.concatenate([limit, limit], axis=1))
            s_s[g % SLOTS] = s
            m = jnp.max(s, axis=0, keepdims=True)
            return m if side == 0 else jnp.maximum(m, m_s[g])

        def finish(g, m):
            lanes = slice(g * LANES, (g + 1) * LANES)
            p = jnp.exp2((s_s[g % SLOTS] - m) * scale2)
            l = jnp.sum(p, axis=0, keepdims=True)
            o = dot_nn(vt_s[side, lanes, :], p.astype(BF16))
            o = [o[:nope, :pair], o[nope:, pair:]]
            if side == 0:
                m_s[g] = m
                l_s[g] = l
                acc_s[g, :nope, :] = o[0]
                acc_s[g, nope:, :] = o[1]
            else:
                alpha = jnp.exp2((m_s[g] - m) * scale2)
                inv = 1.0 / (l_s[g] * alpha + l)
                o = [(acc_s[g, h * nope:(h + 1) * nope, :] * alpha[:, h * pair:(h + 1) * pair] + o[h])
                     * inv[:, h * pair:(h + 1) * pair] for h in range(2)]
                ot = jnp.transpose(jnp.concatenate(o, axis=0).astype(BF16))
                both = [ot[:rows, :], ot[rows:, :]]
                o_own[:, lanes] = jnp.where(core == 0, both[0], both[1])
                o_out[:, lanes] = jnp.where(core == 0, both[1], both[0])

        tops = {}
        project(0)
        for g in range(AHEAD):
            tops[g] = score(g)
        for g in range(groups):
            if g % 2 == 0 and (g + 2) * LANES < cols:
                project((g + 2) * LANES)
            if g + AHEAD < groups:
                tops[g + AHEAD] = score(g + AHEAD)
            finish(g, tops[g])

    for c in range(3):
        sends[c].wait()
    attend(0)
    for c in range(3, n - 1):
        sends[c].wait()
    attend(1)

    pair_o = to_partner(o_out, o_in, 2)
    for c in ld_out:
        c.wait()
    ov = o_own[...]
    for c in range(0, y_ref.shape[1], 512):
        y_acc[:, c:c + 512] = dot_nn(ov, wout[:cols, c:c + 512])
    pair_o.wait()
    ov = o_in[...]
    for c in range(0, y_ref.shape[1], 512):
        y_ref[:, c:c + 512] = (y_acc[:, c:c + 512] + dot_nn(ov, wout[cols:, c:c + 512])).astype(BF16)


def solution(mesh):
    n = mesh.shape['ctx']
    row_spec = P(('dp', 'ctx'), None)
    id_spec = P(('dp', 'ctx'))

    def per_device(x_rows, pos_rows, seg_rows, w_dq, w_uq, w_qr, w_dkv, w_kr, w_uk, w_uv, w_out, gain_q, gain_kv):
        rows, d_model = x_rows.shape
        rope = w_kr.shape[1]
        nope = w_uq.shape[1] * rope // w_qr.shape[1]
        cols = w_uq.shape[1] // 2
        groups = cols // LANES
        keys = n // 2 * rows
        operands = (x_rows, pos_rows.reshape(1, rows), w_dq, w_uq, w_qr, w_dkv, w_kr.T, w_uk, w_uv, w_out, gain_q, gain_kv)
        operands = tuple(pltpu.with_memory_space_constraint(a, pltpu.HBM) for a in operands)
        vm = lambda a: pltpu.VMEM(a.shape, a.dtype)
        cut = lambda a: pltpu.VMEM((a.shape[0], a.shape[1] // 2), a.dtype)
        return pl.pallas_call(
            functools.partial(kernel, n, rows, rope, nope),
            out_shape=jax.ShapeDtypeStruct((rows, w_out.shape[1]), BF16),
            in_specs=[pl.BlockSpec(memory_space=pl.ANY)] * len(operands),
            out_specs=pl.BlockSpec(memory_space=pltpu.VMEM),
            scratch_shapes=[
                pltpu.VMEM((2 * rows, d_model), BF16),
                pltpu.VMEM((2, 1, rows), jnp.int32),
                vm(w_dq), cut(w_uq), cut(w_qr), vm(w_dkv), vm(w_kr.T), cut(w_uk), cut(w_uv), vm(w_out), vm(gain_q), vm(gain_kv),
                pltpu.VMEM((2 * rows + 16, LANES), BF16),
                pltpu.VMEM((n, 2 * rows + 16, LANES), BF16),
                pltpu.VMEM((2, keys, 2 * rows), F32),
                pltpu.VMEM((groups, 2 * LANES, 4 * rows), BF16),
                pltpu.VMEM((2, keys, cols), BF16),
                pltpu.VMEM((2, cols, keys), BF16),
                pltpu.VMEM((groups, 1, 4 * rows), F32),
                pltpu.VMEM((groups, 1, 4 * rows), F32),
                pltpu.VMEM((groups, 2 * nope, 2 * rows), F32),
                pltpu.VMEM((rows, cols), BF16),
                pltpu.VMEM((rows, cols), BF16),
                pltpu.VMEM((rows, cols), BF16),
                pltpu.VMEM((rows, w_out.shape[1]), F32),
                pltpu.VMEM((SLOTS, keys, 4 * rows), F32),
                pltpu.SemaphoreType.DMA((40,)),
                pltpu.SemaphoreType.DMA((n - 1,)),
                pltpu.SemaphoreType.DMA((n - 1,)),
                pltpu.SemaphoreType.DMA((3,)),
                pltpu.SemaphoreType.DMA((3,)),
            ],
            compiler_params=pltpu.CompilerParams(collective_id=0, has_side_effects=True, vmem_limit_bytes=42 * 1024 * 1024),
        )(*operands)

    return jax.shard_map(per_device, mesh=mesh, in_specs=(row_spec, id_spec, id_spec) + (P(),) * 10, out_specs=row_spec, check_vma=False)
```

```python
import functools
import math

import numpy as np
import jax
import jax.numpy as jnp
from jax import lax
from jax.experimental import pallas as pl
from jax.experimental.pallas import tpu as pltpu
from jax.sharding import PartitionSpec as P

NORM_EPS = 1e-6
MESH = pl.DeviceIdType.MESH
F32 = jnp.float32
BF16 = jnp.bfloat16
LANES = 128
STAGES = (2, 3, 4)
LEAD = 2
SLOTS = 5
OUT_COLS = 512
STRIP = 32


def rms_rows(vals, gain):
    mean_sq = jnp.mean(vals * vals, axis=-1, keepdims=True)
    return (vals * lax.rsqrt(mean_sq + NORM_EPS) * gain.astype(F32)).astype(BF16)


def dot_nn(a, b):
    return lax.dot_general(a, b, (((1,), (0,)), ((), ())), preferred_element_type=F32)


def dot_nt(a, b):
    return lax.dot_general(a, b, (((1,), (1,)), ((), ())), preferred_element_type=F32)


def dot_tt(a, b):
    return lax.dot_general(a, b, (((0,), (1,)), ((), ())), preferred_element_type=F32)


def iota(shape, axis):
    return lax.broadcasted_iota(jnp.int32, shape, axis)


def kernel(n, rows, rope, nope, x_hbm, pos_hbm, wdq_hbm, wuq_hbm, wqr_hbm, wdkv_hbm, wkr_hbm, wuk_hbm, wuv_hbm, wout_hbm,
           gq_hbm, gkv_hbm, y_ref, x, pos, wdq, wuq, wqr, wdkv, wkr, wukv, wout, gq, gkv,
           cq, lat, gath, bias, qbd, kn_s, vt_s, m_s, l_s, acc_s, o_own, o_out, o_in, y_acc, s_s, p_s,
           load_sem, send_sem, recv_sem, pair_send, pair_recv):
    me = lax.axis_index('ctx')
    core = lax.rem(me, 2)
    chip = me // 2
    partner = me + 1 - 2 * core
    half = rows // 2
    rank = wdkv.shape[1]
    pair = 2 * rows
    cols = wuq.shape[1]
    groups = cols // LANES
    tables = rope // 2

    barrier = pltpu.get_barrier_semaphore()
    for j in range(1, n):
        pl.semaphore_signal(barrier, inc=1, device_id={'ctx': lax.rem(me + j, n)}, device_id_type=MESH)

    loads = []

    def load(src, dst, sem=None):
        sem = len(loads) if sem is None else sem
        copy = pltpu.make_async_copy(src, dst, load_sem.at[sem])
        copy.start()
        loads.append(copy)
        return copy

    def wait_all(ref, sem):
        pltpu.make_async_copy(ref, ref, sem).wait()

    mine = pl.ds(pl.multiple_of(core * rows, rows), rows)
    head_cols = pl.ds(pl.multiple_of(core * cols, LANES), cols)
    rope_cols = pl.ds(pl.multiple_of(core * wqr.shape[1], LANES), wqr.shape[1])
    d_model = x.shape[1]
    cuts = [(0, 1024), (1024, 1024), (2048, d_model - 2048)]
    ld_x = load(x_hbm, x.at[pl.ds(0, rows), :])
    x[rows:, :] = jnp.zeros((rows, d_model), BF16)
    o_own[rows:, :] = jnp.zeros((rows, cols), BF16)
    o_in[rows:, :] = jnp.zeros((rows, cols), BF16)
    ld_kr = load(wkr_hbm, wkr)
    ld_pos = load(pos_hbm, pos.at[core])
    ld_dkv = [load(wdkv_hbm.at[pl.ds(c, h), :], wdkv.at[pl.ds(c, h), :]) for c, h in cuts]
    ld_gkv = load(gkv_hbm, gkv)
    ld_dq = load(wdq_hbm, wdq)
    ld_gq = load(gq_hbm, gq)
    ld_uq = load(wuq_hbm.at[:, head_cols], wuq)
    ld_qr = load(wqr_hbm.at[:, rope_cols], wqr)
    ukv = len(loads)
    load(wuk_hbm.at[:, head_cols], wukv.at[0], ukv)
    load(wuv_hbm.at[:, head_cols], wukv.at[1], ukv)
    row_a = pl.multiple_of(core * cols, LANES)
    row_b = pl.multiple_of((1 - core) * cols, LANES)
    ld_out = [load(wout_hbm.at[pl.ds(row, cols), :], wout.at[pl.ds(at, cols), :], ukv + 1 + i) for i, (row, at) in enumerate(((row_a, 0), (row_b, cols)))]

    def rope_tables(pos_row):
        width = pos_row.shape[1]
        freq = iota((tables, width), 0)
        inv_freq = jnp.zeros((tables, width), F32)
        for i in range(tables):
            inv_freq = jnp.where(freq == i, np.float32(10000.0 ** (-2.0 * i / rope)), inv_freq)
        angles = pos_row.astype(F32) * inv_freq

        def table(vals):
            tall = jnp.concatenate([vals] * (LANES // tables), axis=0)
            if width < LANES:
                tall = jnp.concatenate([tall] * (LANES // width), axis=1)
            return jnp.transpose(tall)[:width, :]

        lead = lax.rem(iota((width, LANES), 1), rope) < tables
        cos_t, sin_t = table(jnp.cos(angles)), table(jnp.sin(angles))
        return cos_t, jnp.where(lead, -sin_t, sin_t), lead

    def rotate(a, tabs):
        cos_t, sin_t, lead = tabs
        other = jnp.where(lead, pltpu.roll(a, LANES - tables, 1), pltpu.roll(a, tables, 1))
        return a * cos_t + other * sin_t

    ld_pos.wait()
    tabs = rope_tables(pos[core])
    ld_x.wait()
    ld_kr.wait()
    kr = dot_nt(x[0:rows, :], wkr[...])
    c_kv = None
    for c, (first, height) in zip(ld_dkv, cuts):
        c.wait()
        term = dot_nn(x[0:rows, first:first + height], wdkv[first:first + height, :])
        c_kv = term if c_kv is None else c_kv + term
    ld_gkv.wait()
    c_kv = rms_rows(c_kv, gkv[...].reshape(1, rank))
    kr = rotate(jnp.concatenate([kr] * (LANES // rope), axis=1), tabs)
    pack = kr[0:16, :]
    lane16 = iota((16, LANES), 1) // rope
    for b in range(1, rows // 16):
        pack = jnp.where(lane16 == b, kr[16 * b:16 * b + 16, :], pack)
    pack = pack.astype(BF16)
    lat[0:rows, :] = c_kv[:, :LANES]
    lat[rows:2 * rows, :] = c_kv[:, LANES:]
    lat[2 * rows:2 * rows + 16, :] = pack
    gath[me, 0:rows, :] = c_kv[:, :LANES]
    gath[me, rows:2 * rows, :] = c_kv[:, LANES:]
    gath[me, 2 * rows:2 * rows + 16, :] = pack

    def query_latents():
        ld_dq.wait()
        ld_gq.wait()
        both = dot_nn(x[...], wdq[...])
        cq[mine, :] = rms_rows(both[:rows, :] + both[rows:, :], gq[...].reshape(1, wdq.shape[1]))

    pl.when(chip == 0)(query_latents)
    pl.semaphore_wait(barrier, n - 1)
    bit0, bit1 = lax.rem(chip, 2), chip // 2
    for j in range(1, n):
        flip_chip, flip_core = j // 2, j % 2
        peer_chip = (bit0 + (flip_chip % 2) * (1 - 2 * bit0)) + 2 * (bit1 + (flip_chip // 2) * (1 - 2 * bit1))
        peer = 2 * peer_chip + core + flip_core * (1 - 2 * core)
        pltpu.make_async_remote_copy(
            src_ref=lat, dst_ref=gath.at[me], send_sem=send_sem.at[0], recv_sem=recv_sem.at[(flip_chip + 1) // 2],
            device_id={'ctx': peer}, device_id_type=MESH).start()

    def to_partner(src, dst, index):
        copy = pltpu.make_async_remote_copy(
            src_ref=src, dst_ref=dst, send_sem=pair_send.at[index], recv_sem=pair_recv.at[index],
            device_id={'ctx': partner}, device_id_type=MESH)
        copy.start()
        return copy

    pair_pos = to_partner(pos.at[core], pos.at[core], 0)

    pl.when(chip > 0)(query_latents)
    pair_cq = to_partner(cq.at[mine, :], cq.at[mine, :], 1)
    qbd[...] = jnp.zeros_like(qbd)
    pair_pos.wait()
    pos_row = jnp.concatenate([pos[0], pos[1]], axis=1)
    tabs = rope_tables(pos_row)

    q_in = lax.rem(iota((1, pair), 1), rows)
    q_dev = 2 * chip + iota((1, pair), 1) // rows
    q_tok = jnp.where(q_in < half, half * q_dev + q_in, half * (2 * n - 1 - q_dev) + q_in - half)
    q_first = q_tok - pos_row
    side0, side1 = 1 - 2 * bit0, 2 - 4 * bit1
    chips = (chip, chip + side0, chip + side1, chip + side0 + side1)
    chunks = (chips[:1], chips[1:3], chips[3:])
    for i, owner in enumerate(chips):
        r = iota((pair, pair), 0)
        k_in = lax.rem(r, rows)
        k_dev = 2 * owner + r // rows
        k_tok = jnp.where(k_in < half, half * k_dev + k_in, half * (2 * n - 1 - k_dev) + k_in - half)
        ok = (k_tok <= q_tok) & (k_tok >= q_first)
        bias[i * pair:(i + 1) * pair, :] = jnp.where(ok, jnp.inf, -jnp.inf)

    pair_cq.wait()
    c_q = cq[...]
    ld_uq.wait()
    ld_qr.wait()
    qr_all = dot_nn(c_q, wqr[...])
    q_cols = {c: dot_nn(c_q, wuq[:, c:c + 256]).astype(BF16) for c in range(0, cols, 256)}
    for t in range(groups // 2):
        qt = jnp.transpose(rotate(qr_all[:, LANES * t:LANES * t + LANES], tabs).astype(BF16))
        for k in range(4):
            lo = (k % 2) * pair
            qbd[2 * t + k // 2, LANES + rope * k:LANES + rope * k + rope, lo:lo + pair] = qt[rope * k:rope * k + rope, :]
    for g in range(groups):
        qt = jnp.transpose(q_cols[g // 2 * 256][:, g % 2 * LANES:g % 2 * LANES + LANES])
        qbd[g, 0:nope, 0:pair] = qt[0:nope, :]
        qbd[g, nope:2 * nope, pair:2 * pair] = qt[nope:2 * nope, :]

    spread_r = iota((LANES, 4 * LANES), 0)
    spread_c = iota((LANES, 4 * LANES), 1)
    spread = (spread_r == rope * (spread_c // LANES) + lax.rem(spread_c, rope)).astype(F32).astype(BF16)
    scale2 = (nope + rope) ** -0.5 * math.log2(math.e)
    wait_all(wukv, load_sem.at[ukv])

    def attend(index):
        owners = chunks[index]
        count = 2 * len(owners)
        keys = count * rows
        base = 2 * sum(len(c) for c in chunks[:index])

        def rows_of(first, size):
            parts = [gath[pl.ds(2 * owner, 2), first:first + size, :].reshape(2 * size, LANES) for owner in owners]
            return jnp.concatenate(parts, axis=0)

        c_all = jnp.concatenate([rows_of(0, rows), rows_of(rows, rows)], axis=1)
        wide = dot_nn(rows_of(2 * rows, 16), spread).astype(BF16)
        krep = jnp.concatenate([wide[16 * j:16 * j + 16, LANES * b:LANES * b + LANES] for j in range(count) for b in range(rows // 16)], axis=0)

        def project(c):
            kn_s[0:keys, c:c + 256] = dot_nn(c_all, wukv[0, :, c:c + 256]).astype(BF16)
            vt_s[c:c + 256, 0:keys] = dot_tt(wukv[1, :, c:c + 256], c_all).astype(BF16)

        def score(g):
            s = dot_nn(jnp.concatenate([kn_s[0:keys, g * LANES:(g + 1) * LANES], krep], axis=1), qbd[g])
            tall = None
            for r in range(0, keys, STRIP):
                limit = bias[base * rows + r:base * rows + r + STRIP, :]
                strip = jnp.minimum(s[r:r + STRIP, :], jnp.concatenate([limit, limit], axis=1))
                s_s[g % SLOTS, r:r + STRIP, :] = strip
                for k in range(0, STRIP, 8):
                    tall = strip[k:k + 8, :] if tall is None else jnp.maximum(tall, strip[k:k + 8, :])
            m = jnp.max(tall, axis=0, keepdims=True)
            tops[g] = m if index == 0 else jnp.maximum(m, m_s[g])

        def weigh(g):
            total = None
            for r in range(0, keys, STRIP):
                p = jnp.exp2((s_s[g % SLOTS, r:r + STRIP, :] - tops[g]) * scale2)
                p_s[g % SLOTS, r:r + STRIP, :] = p.astype(BF16)
                for k in range(0, STRIP, 8):
                    total = p[k:k + 8, :] if total is None else total + p[k:k + 8, :]
            sums[g] = jnp.sum(total, axis=0, keepdims=True)

        def mix(g):
            o = dot_nn(vt_s[g * LANES:(g + 1) * LANES, 0:keys], p_s[g % SLOTS, 0:keys, :])
            outs[g] = [o[:nope, :pair], o[nope:, pair:]]

        def finish(g):
            lanes = slice(g * LANES, (g + 1) * LANES)
            m, l, o = tops[g], sums[g], outs[g]
            if index > 0:
                alpha = jnp.exp2((m_s[g] - m) * scale2)
                l = l_s[g] * alpha + l
                o = [acc_s[g, h * nope:(h + 1) * nope, :] * alpha[:, h * pair:(h + 1) * pair] + o[h] for h in range(2)]
            if index < len(chunks) - 1:
                m_s[g] = m
                l_s[g] = l
                acc_s[g, :nope, :] = o[0]
                acc_s[g, nope:, :] = o[1]
            else:
                inv = 1.0 / l
                o = [o[h] * inv[:, h * pair:(h + 1) * pair] for h in range(2)]
                ot = jnp.transpose(jnp.concatenate(o, axis=0).astype(BF16))
                both = [ot[:rows, :], ot[rows:, :]]
                o_own[0:rows, lanes] = jnp.where(core == 0, both[0], both[1])
                o_out[:, lanes] = jnp.where(core == 0, both[1], both[0])

        tops, sums, outs = {}, {}, {}
        project(0)
        for t in range(groups + STAGES[2]):
            if t % 2 == 0 and 0 < t + LEAD < groups:
                project((t + LEAD) * LANES)
            for stage, lag in ((score, 0), (weigh, STAGES[0]), (mix, STAGES[1]), (finish, STAGES[2])):
                if 0 <= t - lag < groups:
                    stage(t - lag)

    wait_all(gath.at[pl.ds(0, 1)], recv_sem.at[0])
    attend(0)
    wait_all(gath.at[pl.ds(0, 4)], recv_sem.at[1])
    attend(1)
    wait_all(gath.at[pl.ds(0, 2)], recv_sem.at[2])
    attend(2)

    pair_o = to_partner(o_out, o_in.at[pl.ds(0, rows), :], 2)
    wait_all(gath.at[pl.ds(0, n - 1)], send_sem.at[0])
    for c in ld_out:
        c.wait()
    ov = o_own[...]
    for c in range(0, d_model, OUT_COLS):
        y_acc[:, c:c + OUT_COLS] = dot_nn(ov, wout[:cols, c:c + OUT_COLS])
    pair_o.wait()
    ov = o_in[...]
    for c in range(0, d_model, OUT_COLS):
        out = y_acc[:, c:c + OUT_COLS] + dot_nn(ov, wout[cols:, c:c + OUT_COLS])
        y_ref[:, c:c + OUT_COLS] = (out[:rows, :] + out[rows:, :]).astype(BF16)


def solution(mesh):
    n = mesh.shape['ctx']
    row_spec = P(('dp', 'ctx'), None)
    id_spec = P(('dp', 'ctx'))

    def per_device(x_rows, pos_rows, seg_rows, w_dq, w_uq, w_qr, w_dkv, w_kr, w_uk, w_uv, w_out, gain_q, gain_kv):
        rows, d_model = x_rows.shape
        rope = w_kr.shape[1]
        nope = w_uq.shape[1] * rope // w_qr.shape[1]
        cols = w_uq.shape[1] // 2
        groups = cols // LANES
        keys = n // 2 * rows
        operands = (x_rows, pos_rows.reshape(1, rows), w_dq, w_uq, w_qr, w_dkv, w_kr.T, w_uk, w_uv, w_out, gain_q, gain_kv)
        operands = tuple(pltpu.with_memory_space_constraint(a, pltpu.HBM) for a in operands)
        vm = lambda a: pltpu.VMEM(a.shape, a.dtype)
        cut = lambda a: pltpu.VMEM((a.shape[0], a.shape[1] // 2), a.dtype)
        return pl.pallas_call(
            functools.partial(kernel, n, rows, rope, nope),
            out_shape=jax.ShapeDtypeStruct((rows, w_out.shape[1]), BF16),
            in_specs=[pl.BlockSpec(memory_space=pl.ANY)] * len(operands),
            out_specs=pl.BlockSpec(memory_space=pltpu.VMEM),
            scratch_shapes=[
                pltpu.VMEM((2 * rows, d_model), BF16),
                pltpu.VMEM((2, 1, rows), jnp.int32),
                vm(w_dq), cut(w_uq), cut(w_qr), vm(w_dkv), vm(w_kr.T),
                pltpu.VMEM((2, w_uk.shape[0], cols), BF16),
                vm(w_out), vm(gain_q), vm(gain_kv),
                pltpu.VMEM((2 * rows, w_dq.shape[1]), BF16),
                pltpu.VMEM((2 * rows + 16, LANES), BF16),
                pltpu.VMEM((n, 2 * rows + 16, LANES), BF16),
                pltpu.VMEM((n * rows, 2 * rows), F32),
                pltpu.VMEM((groups, 2 * LANES, 4 * rows), BF16),
                pltpu.VMEM((keys, cols), BF16),
                pltpu.VMEM((cols, keys), BF16),
                pltpu.VMEM((groups, 1, 4 * rows), F32),
                pltpu.VMEM((groups, 1, 4 * rows), F32),
                pltpu.VMEM((groups, 2 * nope, 2 * rows), F32),
                pltpu.VMEM((2 * rows, cols), BF16),
                pltpu.VMEM((rows, cols), BF16),
                pltpu.VMEM((2 * rows, cols), BF16),
                pltpu.VMEM((2 * rows, w_out.shape[1]), F32),
                pltpu.VMEM((SLOTS, keys, 4 * rows), F32),
                pltpu.VMEM((SLOTS, keys, 4 * rows), BF16),
                pltpu.SemaphoreType.DMA((14,)),
                pltpu.SemaphoreType.DMA((1,)),
                pltpu.SemaphoreType.DMA((3,)),
                pltpu.SemaphoreType.DMA((3,)),
                pltpu.SemaphoreType.DMA((3,)),
            ],
            compiler_params=pltpu.CompilerParams(collective_id=0, has_side_effects=True, vmem_limit_bytes=42 * 1024 * 1024),
        )(*operands)

    return jax.shard_map(per_device, mesh=mesh, in_specs=(row_spec, id_spec, id_spec) + (P(),) * 10, out_specs=row_spec, check_vma=False)
```

```python
import functools
import math

import numpy as np
import jax
import jax.numpy as jnp
from jax import lax
from jax.experimental import pallas as pl
from jax.experimental.pallas import tpu as pltpu
from jax.sharding import PartitionSpec as P

NORM_EPS = 1e-6
MESH = pl.DeviceIdType.MESH
F32 = jnp.float32
BF16 = jnp.bfloat16
LANES = 128
STAGES = ((4, 6, 8), (2, 4, 6))
LEAD = 2
SLOTS = 10
OUT_COLS = 512
STRIP = 32


def rms_rows(vals, gain):
    mean_sq = jnp.mean(vals * vals, axis=-1, keepdims=True)
    return (vals * lax.rsqrt(mean_sq + NORM_EPS) * gain.astype(F32)).astype(BF16)


def dot_nn(a, b):
    return lax.dot_general(a, b, (((1,), (0,)), ((), ())), preferred_element_type=F32)


def dot_nt(a, b):
    return lax.dot_general(a, b, (((1,), (1,)), ((), ())), preferred_element_type=F32)


def dot_tt(a, b):
    return lax.dot_general(a, b, (((0,), (1,)), ((), ())), preferred_element_type=F32)


def iota(shape, axis):
    return lax.broadcasted_iota(jnp.int32, shape, axis)


def kernel(n, rows, rope, nope, x_hbm, pos_hbm, wdq_hbm, wuq_hbm, wqr_hbm, wdkv_hbm, wkr_hbm, wuk_hbm, wuv_hbm, wout_hbm,
           gq_hbm, gkv_hbm, y_ref, x, pos, wdq, wuq, wqr, wdkv, wkr, wukv, wout, gq, gkv,
           cq, lat, gath, bias, qbd, kn_s, vt_s, m_s, l_s, acc_s, o_own, o_out, o_in, y_acc, s_s, p_s,
           load_sem, send_sem, recv_sem, pair_send, pair_recv):
    me = lax.axis_index('ctx')
    core = lax.rem(me, 2)
    chip = me // 2
    partner = me + 1 - 2 * core
    half = rows // 2
    rank = wdkv.shape[1]
    pair = 2 * rows
    cols = wuq.shape[1]
    groups = cols // LANES
    tables = rope // 2

    barrier = pltpu.get_barrier_semaphore()
    for j in range(1, n):
        pl.semaphore_signal(barrier, inc=1, device_id={'ctx': lax.rem(me + j, n)}, device_id_type=MESH)

    loads = []

    def load(src, dst, sem=None):
        sem = len(loads) if sem is None else sem
        copy = pltpu.make_async_copy(src, dst, load_sem.at[sem])
        copy.start()
        loads.append(copy)
        return copy

    def wait_all(ref, sem):
        pltpu.make_async_copy(ref, ref, sem).wait()

    mine = pl.ds(pl.multiple_of(core * rows, rows), rows)
    head_cols = pl.ds(pl.multiple_of(core * cols, LANES), cols)
    rope_cols = pl.ds(pl.multiple_of(core * wqr.shape[1], LANES), wqr.shape[1])
    d_model = x.shape[1]
    cuts = [(0, 1024), (1024, 1024), (2048, d_model - 2048)]
    ld_pos = load(pos_hbm, pos.at[core])
    ld_x = load(x_hbm, x.at[pl.ds(0, rows), :])
    x[rows:, :] = jnp.zeros((rows, d_model), BF16)
    o_own[rows:, :] = jnp.zeros((rows, cols), BF16)
    o_in[rows:, :] = jnp.zeros((rows, cols), BF16)
    ld_kr = load(wkr_hbm, wkr)
    ld_gkv = load(gkv_hbm, gkv)
    ld_dkv = [load(wdkv_hbm.at[pl.ds(c, h), :], wdkv.at[pl.ds(c, h), :]) for c, h in cuts]
    ld_dq = load(wdq_hbm, wdq)
    ld_gq = load(gq_hbm, gq)
    ld_uq = load(wuq_hbm.at[:, head_cols], wuq)
    ld_qr = load(wqr_hbm.at[:, rope_cols], wqr)
    ukv = len(loads)
    load(wuk_hbm.at[:, head_cols], wukv.at[0], ukv)
    load(wuv_hbm.at[:, head_cols], wukv.at[1], ukv)
    row_a = pl.multiple_of(core * cols, LANES)
    row_b = pl.multiple_of((1 - core) * cols, LANES)
    ld_out = [load(wout_hbm.at[pl.ds(row, cols), :], wout.at[pl.ds(at, cols), :], ukv + 1 + i) for i, (row, at) in enumerate(((row_a, 0), (row_b, cols)))]

    def rope_tables(pos_row):
        width = pos_row.shape[1]
        freq = iota((tables, width), 0)
        inv_freq = jnp.zeros((tables, width), F32)
        for i in range(tables):
            inv_freq = jnp.where(freq == i, np.float32(10000.0 ** (-2.0 * i / rope)), inv_freq)
        angles = pos_row.astype(F32) * inv_freq

        def table(vals):
            tall = jnp.concatenate([vals] * (LANES // tables), axis=0)
            if width < LANES:
                tall = jnp.concatenate([tall] * (LANES // width), axis=1)
            return jnp.transpose(tall)[:width, :]

        lead = lax.rem(iota((width, LANES), 1), rope) < tables
        cos_t, sin_t = table(jnp.cos(angles)), table(jnp.sin(angles))
        return cos_t, jnp.where(lead, -sin_t, sin_t), lead

    def rotate(a, tabs):
        cos_t, sin_t, lead = tabs
        other = jnp.where(lead, pltpu.roll(a, LANES - tables, 1), pltpu.roll(a, tables, 1))
        return a * cos_t + other * sin_t

    ld_pos.wait()
    tabs = rope_tables(pos[core])
    ld_x.wait()
    ld_kr.wait()
    kr = dot_nt(x[0:rows, :], wkr[...])
    c_kv = None
    for c, (first, height) in zip(ld_dkv, cuts):
        c.wait()
        term = dot_nn(x[0:rows, first:first + height], wdkv[first:first + height, :])
        c_kv = term if c_kv is None else c_kv + term
    ld_gkv.wait()
    c_kv = rms_rows(c_kv, gkv[...].reshape(1, rank))
    kr = rotate(jnp.concatenate([kr] * (LANES // rope), axis=1), tabs)
    pack = kr[0:16, :]
    lane16 = iota((16, LANES), 1) // rope
    for b in range(1, rows // 16):
        pack = jnp.where(lane16 == b, kr[16 * b:16 * b + 16, :], pack)
    pack = pack.astype(BF16)
    lat[0:rows, :] = c_kv[:, :LANES]
    lat[rows:2 * rows, :] = c_kv[:, LANES:]
    lat[2 * rows:2 * rows + 16, :] = pack
    gath[me, 0:rows, :] = c_kv[:, :LANES]
    gath[me, rows:2 * rows, :] = c_kv[:, LANES:]
    gath[me, 2 * rows:2 * rows + 16, :] = pack

    def query_latents():
        ld_dq.wait()
        ld_gq.wait()
        both = dot_nn(x[...], wdq[...])
        cq[mine, :] = rms_rows(both[:rows, :] + both[rows:, :], gq[...].reshape(1, wdq.shape[1]))

    pl.when(chip == 0)(query_latents)
    pl.semaphore_wait(barrier, n - 1)
    bit0, bit1 = lax.rem(chip, 2), chip // 2
    for j in range(1, n):
        flip_chip, flip_core = j // 2, j % 2
        peer_chip = (bit0 + (flip_chip % 2) * (1 - 2 * bit0)) + 2 * (bit1 + (flip_chip // 2) * (1 - 2 * bit1))
        peer = 2 * peer_chip + core + flip_core * (1 - 2 * core)
        pltpu.make_async_remote_copy(
            src_ref=lat, dst_ref=gath.at[me], send_sem=send_sem.at[0], recv_sem=recv_sem.at[(flip_chip + 1) // 2],
            device_id={'ctx': peer}, device_id_type=MESH).start()

    def to_partner(src, dst, index):
        copy = pltpu.make_async_remote_copy(
            src_ref=src, dst_ref=dst, send_sem=pair_send.at[index], recv_sem=pair_recv.at[index],
            device_id={'ctx': partner}, device_id_type=MESH)
        copy.start()
        return copy

    pair_pos = to_partner(pos.at[core], pos.at[core], 0)

    pl.when(chip > 0)(query_latents)
    pair_cq = to_partner(cq.at[mine, :], cq.at[mine, :], 1)
    qbd[...] = jnp.zeros_like(qbd)
    pair_pos.wait()
    pos_row = jnp.concatenate([pos[0], pos[1]], axis=1)
    tabs = rope_tables(pos_row)

    q_in = lax.rem(iota((1, pair), 1), rows)
    q_dev = 2 * chip + iota((1, pair), 1) // rows
    q_tok = jnp.where(q_in < half, half * q_dev + q_in, half * (2 * n - 1 - q_dev) + q_in - half)
    q_first = q_tok - pos_row
    side0, side1 = 1 - 2 * bit0, 2 - 4 * bit1
    chips = (chip, chip + side0, chip + side1, chip + side0 + side1)
    chunks = (chips[:1], chips[1:3], chips[3:])
    for i, owner in enumerate(chips):
        r = iota((pair, pair), 0)
        k_in = lax.rem(r, rows)
        k_dev = 2 * owner + r // rows
        k_tok = jnp.where(k_in < half, half * k_dev + k_in, half * (2 * n - 1 - k_dev) + k_in - half)
        ok = (k_tok <= q_tok) & (k_tok >= q_first)
        bias[i * pair:(i + 1) * pair, :] = jnp.where(ok, jnp.inf, -jnp.inf)

    pair_cq.wait()
    c_q = cq[...]
    ld_uq.wait()
    ld_qr.wait()
    qr_all = dot_nn(c_q, wqr[...])
    q_cols = {c: dot_nn(c_q, wuq[:, c:c + 256]).astype(BF16) for c in range(0, cols, 256)}
    for t in range(groups // 2):
        qt = jnp.transpose(rotate(qr_all[:, LANES * t:LANES * t + LANES], tabs).astype(BF16))
        for k in range(4):
            lo = (k % 2) * pair
            qbd[2 * t + k // 2, LANES + rope * k:LANES + rope * k + rope, lo:lo + pair] = qt[rope * k:rope * k + rope, :]
    for g in range(groups):
        qt = jnp.transpose(q_cols[g // 2 * 256][:, g % 2 * LANES:g % 2 * LANES + LANES])
        qbd[g, 0:nope, 0:pair] = qt[0:nope, :]
        qbd[g, nope:2 * nope, pair:2 * pair] = qt[nope:2 * nope, :]

    spread_r = iota((LANES, 4 * LANES), 0)
    spread_c = iota((LANES, 4 * LANES), 1)
    spread = (spread_r == rope * (spread_c // LANES) + lax.rem(spread_c, rope)).astype(F32).astype(BF16)
    scale2 = (nope + rope) ** -0.5 * math.log2(math.e)
    wait_all(wukv, load_sem.at[ukv])

    def attend(index):
        owners = chunks[index]
        count = 2 * len(owners)
        keys = count * rows
        base = 2 * sum(len(c) for c in chunks[:index])

        def rows_of(first, size):
            parts = [gath[pl.ds(2 * owner, 2), first:first + size, :].reshape(2 * size, LANES) for owner in owners]
            return jnp.concatenate(parts, axis=0)

        c_all = jnp.concatenate([rows_of(0, rows), rows_of(rows, rows)], axis=1)
        wide = dot_nn(rows_of(2 * rows, 16), spread).astype(BF16)
        krep = jnp.concatenate([wide[16 * j:16 * j + 16, LANES * b:LANES * b + LANES] for j in range(count) for b in range(rows // 16)], axis=0)

        def project(c):
            kn_s[0:keys, c:c + 256] = dot_nn(c_all, wukv[0, :, c:c + 256]).astype(BF16)
            vt_s[c:c + 256, 0:keys] = dot_tt(wukv[1, :, c:c + 256], c_all).astype(BF16)

        def score(g):
            s = dot_nn(jnp.concatenate([kn_s[0:keys, g * LANES:(g + 1) * LANES], krep], axis=1), qbd[g])
            tall = None
            for r in range(0, keys, STRIP):
                limit = bias[base * rows + r:base * rows + r + STRIP, :]
                strip = jnp.minimum(s[r:r + STRIP, :], jnp.concatenate([limit, limit], axis=1))
                s_s[g % SLOTS, r:r + STRIP, :] = strip
                for k in range(0, STRIP, 8):
                    tall = strip[k:k + 8, :] if tall is None else jnp.maximum(tall, strip[k:k + 8, :])
            m = jnp.max(tall, axis=0, keepdims=True)
            tops[g] = m if index == 0 else jnp.maximum(m, m_s[g])

        def weigh(g):
            total = None
            for r in range(0, keys, STRIP):
                p = jnp.exp2((s_s[g % SLOTS, r:r + STRIP, :] - tops[g]) * scale2)
                p_s[g % SLOTS, r:r + STRIP, :] = p.astype(BF16)
                for k in range(0, STRIP, 8):
                    total = p[k:k + 8, :] if total is None else total + p[k:k + 8, :]
            sums[g] = jnp.sum(total, axis=0, keepdims=True)

        def mix(g):
            o = dot_nn(vt_s[g * LANES:(g + 1) * LANES, 0:keys], p_s[g % SLOTS, 0:keys, :])
            outs[g] = [o[:nope, :pair], o[nope:, pair:]]

        def finish(g):
            lanes = slice(g * LANES, (g + 1) * LANES)
            m, l, o = tops[g], sums[g], outs[g]
            if index > 0:
                alpha = jnp.exp2((m_s[g] - m) * scale2)
                l = l_s[g] * alpha + l
                o = [acc_s[g, h * nope:(h + 1) * nope, :] * alpha[:, h * pair:(h + 1) * pair] + o[h] for h in range(2)]
            if index < len(chunks) - 1:
                m_s[g] = m
                l_s[g] = l
                acc_s[g, :nope, :] = o[0]
                acc_s[g, nope:, :] = o[1]
            else:
                inv = 1.0 / l
                o = [o[h] * inv[:, h * pair:(h + 1) * pair] for h in range(2)]
                ot = jnp.transpose(jnp.concatenate(o, axis=0).astype(BF16))
                both = [ot[:rows, :], ot[rows:, :]]
                o_own[0:rows, lanes] = jnp.where(core == 0, both[0], both[1])
                o_out[:, lanes] = jnp.where(core == 0, both[1], both[0])

        tops, sums, outs = {}, {}, {}
        lags = STAGES[len(owners) - 1]
        project(0)
        for t in range(groups + lags[2]):
            if t % 2 == 0 and 0 < t + LEAD < groups:
                project((t + LEAD) * LANES)
            for stage, lag in ((score, 0), (weigh, lags[0]), (mix, lags[1]), (finish, lags[2])):
                if 0 <= t - lag < groups:
                    stage(t - lag)

    wait_all(gath.at[pl.ds(0, 1)], recv_sem.at[0])
    attend(0)
    wait_all(gath.at[pl.ds(0, 4)], recv_sem.at[1])
    attend(1)
    wait_all(gath.at[pl.ds(0, 2)], recv_sem.at[2])
    attend(2)

    pair_o = to_partner(o_out, o_in.at[pl.ds(0, rows), :], 2)
    wait_all(gath.at[pl.ds(0, n - 1)], send_sem.at[0])
    for c in ld_out:
        c.wait()
    ov = o_own[...]
    for c in range(0, d_model, OUT_COLS):
        y_acc[:, c:c + OUT_COLS] = dot_nn(ov, wout[:cols, c:c + OUT_COLS])
    pair_o.wait()
    ov = o_in[...]
    for c in range(0, d_model, OUT_COLS):
        out = y_acc[:, c:c + OUT_COLS] + dot_nn(ov, wout[cols:, c:c + OUT_COLS])
        y_ref[:, c:c + OUT_COLS] = (out[:rows, :] + out[rows:, :]).astype(BF16)


def solution(mesh):
    n = mesh.shape['ctx']
    row_spec = P(('dp', 'ctx'), None)
    id_spec = P(('dp', 'ctx'))

    def per_device(x_rows, pos_rows, seg_rows, w_dq, w_uq, w_qr, w_dkv, w_kr, w_uk, w_uv, w_out, gain_q, gain_kv):
        rows, d_model = x_rows.shape
        rope = w_kr.shape[1]
        nope = w_uq.shape[1] * rope // w_qr.shape[1]
        cols = w_uq.shape[1] // 2
        groups = cols // LANES
        keys = n // 2 * rows
        operands = (x_rows, pos_rows.reshape(1, rows), w_dq, w_uq, w_qr, w_dkv, w_kr.T, w_uk, w_uv, w_out, gain_q, gain_kv)
        operands = tuple(pltpu.with_memory_space_constraint(a, pltpu.HBM) for a in operands)
        vm = lambda a: pltpu.VMEM(a.shape, a.dtype)
        cut = lambda a: pltpu.VMEM((a.shape[0], a.shape[1] // 2), a.dtype)
        return pl.pallas_call(
            functools.partial(kernel, n, rows, rope, nope),
            out_shape=jax.ShapeDtypeStruct((rows, w_out.shape[1]), BF16),
            in_specs=[pl.BlockSpec(memory_space=pl.ANY)] * len(operands),
            out_specs=pl.BlockSpec(memory_space=pltpu.VMEM),
            scratch_shapes=[
                pltpu.VMEM((2 * rows, d_model), BF16),
                pltpu.VMEM((2, 1, rows), jnp.int32),
                vm(w_dq), cut(w_uq), cut(w_qr), vm(w_dkv), vm(w_kr.T),
                pltpu.VMEM((2, w_uk.shape[0], cols), BF16),
                vm(w_out), vm(gain_q), vm(gain_kv),
                pltpu.VMEM((2 * rows, w_dq.shape[1]), BF16),
                pltpu.VMEM((2 * rows + 16, LANES), BF16),
                pltpu.VMEM((n, 2 * rows + 16, LANES), BF16),
                pltpu.VMEM((n * rows, 2 * rows), F32),
                pltpu.VMEM((groups, 2 * LANES, 4 * rows), BF16),
                pltpu.VMEM((keys, cols), BF16),
                pltpu.VMEM((cols, keys), BF16),
                pltpu.VMEM((groups, 1, 4 * rows), F32),
                pltpu.VMEM((groups, 1, 4 * rows), F32),
                pltpu.VMEM((groups, 2 * nope, 2 * rows), F32),
                pltpu.VMEM((2 * rows, cols), BF16),
                pltpu.VMEM((rows, cols), BF16),
                pltpu.VMEM((2 * rows, cols), BF16),
                pltpu.VMEM((2 * rows, w_out.shape[1]), F32),
                pltpu.VMEM((SLOTS, keys, 4 * rows), F32),
                pltpu.VMEM((SLOTS, keys, 4 * rows), BF16),
                pltpu.SemaphoreType.DMA((14,)),
                pltpu.SemaphoreType.DMA((1,)),
                pltpu.SemaphoreType.DMA((3,)),
                pltpu.SemaphoreType.DMA((3,)),
                pltpu.SemaphoreType.DMA((3,)),
            ],
            compiler_params=pltpu.CompilerParams(collective_id=0, has_side_effects=True, vmem_limit_bytes=42 * 1024 * 1024),
        )(*operands)

    return jax.shard_map(per_device, mesh=mesh, in_specs=(row_spec, id_spec, id_spec) + (P(),) * 10, out_specs=row_spec, check_vma=False)
```

```python
import functools
import math

import numpy as np
import jax
import jax.numpy as jnp
from jax import lax
from jax.experimental import pallas as pl
from jax.experimental.pallas import tpu as pltpu
from jax.sharding import PartitionSpec as P

NORM_EPS = 1e-6
MESH = pl.DeviceIdType.MESH
F32 = jnp.float32
BF16 = jnp.bfloat16
LANES = 128
STAGES = ((4, 6, 8), (2, 4, 6))
LEAD = 2
SLOTS = 10
FIRST_SEND = 6
OUT_COLS = 512
STRIP = 32


def rms_rows(vals, gain):
    mean_sq = jnp.mean(vals * vals, axis=-1, keepdims=True)
    return (vals * lax.rsqrt(mean_sq + NORM_EPS) * gain.astype(F32)).astype(BF16)


def dot_nn(a, b):
    return lax.dot_general(a, b, (((1,), (0,)), ((), ())), preferred_element_type=F32)


def dot_nt(a, b):
    return lax.dot_general(a, b, (((1,), (1,)), ((), ())), preferred_element_type=F32)


def dot_tt(a, b):
    return lax.dot_general(a, b, (((0,), (1,)), ((), ())), preferred_element_type=F32)


def iota(shape, axis):
    return lax.broadcasted_iota(jnp.int32, shape, axis)


def kernel(n, rows, rope, nope, x_hbm, pos_hbm, wdq_hbm, wuq_hbm, wqr_hbm, wdkv_hbm, wkr_hbm, wuk_hbm, wuv_hbm, wout_hbm,
           gq_hbm, gkv_hbm, y_ref, x, pos, wdq, wuq, wqr, wdkv, wkr, wukv, wout, gq, gkv,
           cq, lat, gath, bias, qbd, kn_s, vt_s, m_s, l_s, acc_s, o_own, o_out, o_in, y_acc, s_s, p_s,
           load_sem, send_sem, recv_sem, pair_send, pair_recv):
    me = lax.axis_index('ctx')
    core = lax.rem(me, 2)
    chip = me // 2
    partner = me + 1 - 2 * core
    half = rows // 2
    rank = wdkv.shape[1]
    pair = 2 * rows
    cols = wuq.shape[1]
    groups = cols // LANES
    tables = rope // 2

    barrier = pltpu.get_barrier_semaphore()
    for j in range(1, n):
        pl.semaphore_signal(barrier, inc=1, device_id={'ctx': lax.rem(me + j, n)}, device_id_type=MESH)

    loads = []

    def load(src, dst, sem=None):
        sem = len(loads) if sem is None else sem
        copy = pltpu.make_async_copy(src, dst, load_sem.at[sem])
        copy.start()
        loads.append(copy)
        return copy

    def wait_all(ref, sem):
        pltpu.make_async_copy(ref, ref, sem).wait()

    mine = pl.ds(pl.multiple_of(core * rows, rows), rows)
    head_cols = pl.ds(pl.multiple_of(core * cols, LANES), cols)
    rope_cols = pl.ds(pl.multiple_of(core * wqr.shape[1], LANES), wqr.shape[1])
    d_model = x.shape[1]
    cuts = [(0, 1024), (1024, 1024), (2048, d_model - 2048)]
    ld_pos = load(pos_hbm, pos.at[core])
    ld_x = load(x_hbm, x.at[pl.ds(0, rows), :])
    x[rows:, :] = jnp.zeros((rows, d_model), BF16)
    o_own[rows:, :] = jnp.zeros((rows, cols), BF16)
    o_in[rows:, :] = jnp.zeros((rows, cols), BF16)
    ld_kr = load(wkr_hbm, wkr)
    ld_gkv = load(gkv_hbm, gkv)
    ld_dkv = [load(wdkv_hbm.at[pl.ds(c, h), :], wdkv.at[pl.ds(c, h), :]) for c, h in cuts]
    ld_dq = load(wdq_hbm, wdq)
    ld_gq = load(gq_hbm, gq)
    ld_uq = load(wuq_hbm.at[:, head_cols], wuq)
    ld_qr = load(wqr_hbm.at[:, rope_cols], wqr)
    ukv = len(loads)
    load(wuk_hbm.at[:, head_cols], wukv.at[0], ukv)
    load(wuv_hbm.at[:, head_cols], wukv.at[1], ukv)
    row_a = pl.multiple_of(core * cols, LANES)
    row_b = pl.multiple_of((1 - core) * cols, LANES)
    for row, at in ((row_a, 0), (row_b, cols)):
        load(wout_hbm.at[pl.ds(row, cols), :], wout.at[pl.ds(at, cols), :], ukv + 1)

    def rope_tables(pos_row):
        width = pos_row.shape[1]
        freq = iota((tables, width), 0)
        inv_freq = jnp.zeros((tables, width), F32)
        for i in range(tables):
            inv_freq = jnp.where(freq == i, np.float32(10000.0 ** (-2.0 * i / rope)), inv_freq)
        angles = pos_row.astype(F32) * inv_freq

        def table(vals):
            tall = jnp.concatenate([vals] * (LANES // tables), axis=0)
            if width < LANES:
                tall = jnp.concatenate([tall] * (LANES // width), axis=1)
            return jnp.transpose(tall)[:width, :]

        lead = lax.rem(iota((width, LANES), 1), rope) < tables
        cos_t, sin_t = table(jnp.cos(angles)), table(jnp.sin(angles))
        return cos_t, jnp.where(lead, -sin_t, sin_t), lead

    def rotate(a, tabs):
        cos_t, sin_t, lead = tabs
        other = jnp.where(lead, pltpu.roll(a, LANES - tables, 1), pltpu.roll(a, tables, 1))
        return a * cos_t + other * sin_t

    ld_pos.wait()
    tabs = rope_tables(pos[core])
    ld_x.wait()
    ld_kr.wait()
    kr = dot_nt(x[0:rows, :], wkr[...])
    c_kv = None
    for c, (first, height) in zip(ld_dkv, cuts):
        c.wait()
        term = dot_nn(x[0:rows, first:first + height], wdkv[first:first + height, :])
        c_kv = term if c_kv is None else c_kv + term
    ld_gkv.wait()
    c_kv = rms_rows(c_kv, gkv[...].reshape(1, rank))
    kr = rotate(jnp.concatenate([kr] * (LANES // rope), axis=1), tabs)
    pack = kr[0:16, :]
    lane16 = iota((16, LANES), 1) // rope
    for b in range(1, rows // 16):
        pack = jnp.where(lane16 == b, kr[16 * b:16 * b + 16, :], pack)
    pack = pack.astype(BF16)
    lat[0:rows, :] = c_kv[:, :LANES]
    lat[rows:2 * rows, :] = c_kv[:, LANES:]
    lat[2 * rows:2 * rows + 16, :] = pack
    gath[me, 0:rows, :] = c_kv[:, :LANES]
    gath[me, rows:2 * rows, :] = c_kv[:, LANES:]
    gath[me, 2 * rows:2 * rows + 16, :] = pack

    def query_latents():
        ld_dq.wait()
        ld_gq.wait()
        both = dot_nn(x[...], wdq[...])
        cq[mine, :] = rms_rows(both[:rows, :] + both[rows:, :], gq[...].reshape(1, wdq.shape[1]))

    pl.when(chip == 0)(query_latents)
    pl.semaphore_wait(barrier, n - 1)
    bit0, bit1 = lax.rem(chip, 2), chip // 2
    def send(flip_core, flip_chip, sem):
        flip0, flip1 = lax.rem(flip_chip, 2), flip_chip // 2
        peer_chip = (bit0 + flip0 * (1 - 2 * bit0)) + 2 * (bit1 + flip1 * (1 - 2 * bit1))
        peer = 2 * peer_chip + core + flip_core * (1 - 2 * core)
        pltpu.make_async_remote_copy(
            src_ref=lat, dst_ref=gath.at[me], send_sem=send_sem.at[0], recv_sem=recv_sem.at[sem],
            device_id={'ctx': peer}, device_id_type=MESH).start()

    send(1, 0, 0)
    for k in range(3):
        flip_chip = lax.rem(k + 2 * (chip // 3), 3) + 1
        for flip_core in range(2):
            send(flip_core, flip_chip, (flip_chip + 2) // 2)

    def to_partner(src, dst, index):
        copy = pltpu.make_async_remote_copy(
            src_ref=src, dst_ref=dst, send_sem=pair_send.at[index], recv_sem=pair_recv.at[index],
            device_id={'ctx': partner}, device_id_type=MESH)
        copy.start()
        return copy

    pair_pos = to_partner(pos.at[core], pos.at[core], 0)

    pl.when(chip > 0)(query_latents)
    pair_cq = to_partner(cq.at[mine, :], cq.at[mine, :], 1)
    qbd[...] = jnp.zeros_like(qbd)
    pair_pos.wait()
    pos_row = jnp.concatenate([pos[0], pos[1]], axis=1)
    tabs = rope_tables(pos_row)

    q_in = lax.rem(iota((1, pair), 1), rows)
    q_dev = 2 * chip + iota((1, pair), 1) // rows
    q_tok = jnp.where(q_in < half, half * q_dev + q_in, half * (2 * n - 1 - q_dev) + q_in - half)
    q_first = q_tok - pos_row
    side0, side1 = 1 - 2 * bit0, 2 - 4 * bit1
    chips = (chip, chip + side0, chip + side1, chip + side0 + side1)
    chunks = (chips[:1], chips[1:2], chips[2:])
    for i, owner in enumerate(chips):
        r = iota((pair, pair), 0)
        k_in = lax.rem(r, rows)
        k_dev = 2 * owner + r // rows
        k_tok = jnp.where(k_in < half, half * k_dev + k_in, half * (2 * n - 1 - k_dev) + k_in - half)
        ok = (k_tok <= q_tok) & (k_tok >= q_first)
        bias[i * pair:(i + 1) * pair, :] = jnp.where(ok, jnp.inf, -jnp.inf)

    pair_cq.wait()
    c_q = cq[...]
    ld_uq.wait()
    ld_qr.wait()
    qr_all = dot_nn(c_q, wqr[...])
    q_cols = {c: dot_nn(c_q, wuq[:, c:c + 256]).astype(BF16) for c in range(0, cols, 256)}
    for t in range(groups // 2):
        qt = jnp.transpose(rotate(qr_all[:, LANES * t:LANES * t + LANES], tabs).astype(BF16))
        for k in range(4):
            lo = (k % 2) * pair
            qbd[2 * t + k // 2, LANES + rope * k:LANES + rope * k + rope, lo:lo + pair] = qt[rope * k:rope * k + rope, :]
    for g in range(groups):
        qt = jnp.transpose(q_cols[g // 2 * 256][:, g % 2 * LANES:g % 2 * LANES + LANES])
        qbd[g, 0:nope, 0:pair] = qt[0:nope, :]
        qbd[g, nope:2 * nope, pair:2 * pair] = qt[nope:2 * nope, :]

    spread_r = iota((LANES, 4 * LANES), 0)
    spread_c = iota((LANES, 4 * LANES), 1)
    spread = (spread_r == rope * (spread_c // LANES) + lax.rem(spread_c, rope)).astype(F32).astype(BF16)
    scale2 = (nope + rope) ** -0.5 * math.log2(math.e)
    wait_all(wukv, load_sem.at[ukv])

    pair_o = []

    def send_heads(first, last, index):
        part = pl.ds(first * LANES, (last - first) * LANES)
        return to_partner(o_out.at[:, part], o_in.at[pl.ds(0, rows), part], index)

    def attend(index):
        owners = chunks[index]
        count = 2 * len(owners)
        keys = count * rows
        base = 2 * sum(len(c) for c in chunks[:index])

        def rows_of(first, size):
            parts = [gath[pl.ds(2 * owner, 2), first:first + size, :].reshape(2 * size, LANES) for owner in owners]
            return jnp.concatenate(parts, axis=0)

        c_all = jnp.concatenate([rows_of(0, rows), rows_of(rows, rows)], axis=1)
        wide = dot_nn(rows_of(2 * rows, 16), spread).astype(BF16)
        krep = jnp.concatenate([wide[16 * j:16 * j + 16, LANES * b:LANES * b + LANES] for j in range(count) for b in range(rows // 16)], axis=0)

        def project(c):
            kn_s[0:keys, c:c + 256] = dot_nn(c_all, wukv[0, :, c:c + 256]).astype(BF16)
            vt_s[c:c + 256, 0:keys] = dot_tt(wukv[1, :, c:c + 256], c_all).astype(BF16)

        def score(g):
            s = dot_nn(jnp.concatenate([kn_s[0:keys, g * LANES:(g + 1) * LANES], krep], axis=1), qbd[g])
            tall = None
            for r in range(0, keys, STRIP):
                limit = bias[base * rows + r:base * rows + r + STRIP, :]
                strip = jnp.minimum(s[r:r + STRIP, :], jnp.concatenate([limit, limit], axis=1))
                s_s[g % SLOTS, r:r + STRIP, :] = strip
                for k in range(0, STRIP, 8):
                    tall = strip[k:k + 8, :] if tall is None else jnp.maximum(tall, strip[k:k + 8, :])
            m = jnp.max(tall, axis=0, keepdims=True)
            tops[g] = m if index == 0 else jnp.maximum(m, m_s[g])

        def weigh(g):
            total = None
            for r in range(0, keys, STRIP):
                p = jnp.exp2((s_s[g % SLOTS, r:r + STRIP, :] - tops[g]) * scale2)
                p_s[g % SLOTS, r:r + STRIP, :] = p.astype(BF16)
                for k in range(0, STRIP, 8):
                    total = p[k:k + 8, :] if total is None else total + p[k:k + 8, :]
            sums[g] = jnp.sum(total, axis=0, keepdims=True)

        def mix(g):
            o = dot_nn(vt_s[g * LANES:(g + 1) * LANES, 0:keys], p_s[g % SLOTS, 0:keys, :])
            outs[g] = [o[:nope, :pair], o[nope:, pair:]]

        def finish(g):
            lanes = slice(g * LANES, (g + 1) * LANES)
            m, l, o = tops[g], sums[g], outs[g]
            if index > 0:
                alpha = jnp.exp2((m_s[g] - m) * scale2)
                l = l_s[g] * alpha + l
                o = [acc_s[g, h * nope:(h + 1) * nope, :] * alpha[:, h * pair:(h + 1) * pair] + o[h] for h in range(2)]
            if index < len(chunks) - 1:
                m_s[g] = m
                l_s[g] = l
                acc_s[g, :nope, :] = o[0]
                acc_s[g, nope:, :] = o[1]
            else:
                inv = 1.0 / l
                o = [o[h] * inv[:, h * pair:(h + 1) * pair] for h in range(2)]
                ot = jnp.transpose(jnp.concatenate(o, axis=0).astype(BF16))
                both = [ot[:rows, :], ot[rows:, :]]
                o_own[0:rows, lanes] = jnp.where(core == 0, both[0], both[1])
                o_out[:, lanes] = jnp.where(core == 0, both[1], both[0])
                if g == FIRST_SEND - 1:
                    pair_o.append(send_heads(0, FIRST_SEND, 2))

        tops, sums, outs = {}, {}, {}
        lags = STAGES[len(owners) - 1]
        project(0)
        for t in range(groups + lags[2]):
            if t % 2 == 0 and 0 < t + LEAD < groups:
                project((t + LEAD) * LANES)
            for stage, lag in ((score, 0), (weigh, lags[0]), (mix, lags[1]), (finish, lags[2])):
                if 0 <= t - lag < groups:
                    stage(t - lag)

    wait_all(gath.at[pl.ds(0, 1)], recv_sem.at[0])
    attend(0)
    wait_all(gath.at[pl.ds(0, 2)], recv_sem.at[1])
    attend(1)
    wait_all(gath.at[pl.ds(0, 4)], recv_sem.at[2])
    attend(2)

    pair_o.append(send_heads(FIRST_SEND, groups, 3))
    wait_all(gath.at[pl.ds(0, n - 1)], send_sem.at[0])
    wait_all(wout, load_sem.at[ukv + 1])
    ov = o_own[...]
    for c in range(0, d_model, OUT_COLS):
        y_acc[:, c:c + OUT_COLS] = dot_nn(ov, wout[:cols, c:c + OUT_COLS])
    split = FIRST_SEND * LANES
    pair_o[0].wait()
    ov = o_in[:, :split]
    for c in range(0, d_model, OUT_COLS):
        y_acc[:, c:c + OUT_COLS] += dot_nn(ov, wout[cols:cols + split, c:c + OUT_COLS])
    pair_o[1].wait()
    ov = o_in[:, split:]
    for c in range(0, d_model, OUT_COLS):
        out = y_acc[:, c:c + OUT_COLS] + dot_nn(ov, wout[cols + split:, c:c + OUT_COLS])
        y_ref[:, c:c + OUT_COLS] = (out[:rows, :] + out[rows:, :]).astype(BF16)


def solution(mesh):
    n = mesh.shape['ctx']
    row_spec = P(('dp', 'ctx'), None)
    id_spec = P(('dp', 'ctx'))

    def per_device(x_rows, pos_rows, seg_rows, w_dq, w_uq, w_qr, w_dkv, w_kr, w_uk, w_uv, w_out, gain_q, gain_kv):
        rows, d_model = x_rows.shape
        rope = w_kr.shape[1]
        nope = w_uq.shape[1] * rope // w_qr.shape[1]
        cols = w_uq.shape[1] // 2
        groups = cols // LANES
        keys = n // 2 * rows
        operands = (x_rows, pos_rows.reshape(1, rows), w_dq, w_uq, w_qr, w_dkv, w_kr.T, w_uk, w_uv, w_out, gain_q, gain_kv)
        operands = tuple(pltpu.with_memory_space_constraint(a, pltpu.HBM) for a in operands)
        vm = lambda a: pltpu.VMEM(a.shape, a.dtype)
        cut = lambda a: pltpu.VMEM((a.shape[0], a.shape[1] // 2), a.dtype)
        return pl.pallas_call(
            functools.partial(kernel, n, rows, rope, nope),
            out_shape=jax.ShapeDtypeStruct((rows, w_out.shape[1]), BF16),
            in_specs=[pl.BlockSpec(memory_space=pl.ANY)] * len(operands),
            out_specs=pl.BlockSpec(memory_space=pltpu.VMEM),
            scratch_shapes=[
                pltpu.VMEM((2 * rows, d_model), BF16),
                pltpu.VMEM((2, 1, rows), jnp.int32),
                vm(w_dq), cut(w_uq), cut(w_qr), vm(w_dkv), vm(w_kr.T),
                pltpu.VMEM((2, w_uk.shape[0], cols), BF16),
                vm(w_out), vm(gain_q), vm(gain_kv),
                pltpu.VMEM((2 * rows, w_dq.shape[1]), BF16),
                pltpu.VMEM((2 * rows + 16, LANES), BF16),
                pltpu.VMEM((n, 2 * rows + 16, LANES), BF16),
                pltpu.VMEM((n * rows, 2 * rows), F32),
                pltpu.VMEM((groups, 2 * LANES, 4 * rows), BF16),
                pltpu.VMEM((keys, cols), BF16),
                pltpu.VMEM((cols, keys), BF16),
                pltpu.VMEM((groups, 1, 4 * rows), F32),
                pltpu.VMEM((groups, 1, 4 * rows), F32),
                pltpu.VMEM((groups, 2 * nope, 2 * rows), F32),
                pltpu.VMEM((2 * rows, cols), BF16),
                pltpu.VMEM((rows, cols), BF16),
                pltpu.VMEM((2 * rows, cols), BF16),
                pltpu.VMEM((2 * rows, w_out.shape[1]), F32),
                pltpu.VMEM((SLOTS, keys, 4 * rows), F32),
                pltpu.VMEM((SLOTS, keys, 4 * rows), BF16),
                pltpu.SemaphoreType.DMA((13,)),
                pltpu.SemaphoreType.DMA((1,)),
                pltpu.SemaphoreType.DMA((3,)),
                pltpu.SemaphoreType.DMA((4,)),
                pltpu.SemaphoreType.DMA((4,)),
            ],
            compiler_params=pltpu.CompilerParams(collective_id=0, has_side_effects=True, vmem_limit_bytes=42 * 1024 * 1024),
        )(*operands)

    return jax.shard_map(per_device, mesh=mesh, in_specs=(row_spec, id_spec, id_spec) + (P(),) * 10, out_specs=row_spec, check_vma=False)
```

```python
import functools
import math

import numpy as np
import jax
import jax.numpy as jnp
from jax import lax
from jax.experimental import pallas as pl
from jax.experimental.pallas import tpu as pltpu
from jax.sharding import PartitionSpec as P

NORM_EPS = 1e-6
MESH = pl.DeviceIdType.MESH
F32 = jnp.float32
BF16 = jnp.bfloat16
LANES = 128
STAGES = ((4, 6, 8), (2, 4, 6))
LEAD = 2
SLOTS = 10
SENDS = (0, 4, 10)
OUT_COLS = 512
STRIP = 32


def rms_rows(vals, gain):
    mean_sq = jnp.mean(vals * vals, axis=-1, keepdims=True)
    return (vals * lax.rsqrt(mean_sq + NORM_EPS) * gain.astype(F32)).astype(BF16)


def dot_nn(a, b):
    return lax.dot_general(a, b, (((1,), (0,)), ((), ())), preferred_element_type=F32)


def dot_nt(a, b):
    return lax.dot_general(a, b, (((1,), (1,)), ((), ())), preferred_element_type=F32)


def dot_tt(a, b):
    return lax.dot_general(a, b, (((0,), (1,)), ((), ())), preferred_element_type=F32)


def iota(shape, axis):
    return lax.broadcasted_iota(jnp.int32, shape, axis)


def kernel(n, rows, rope, nope, x_hbm, pos_hbm, wdq_hbm, wuq_hbm, wqr_hbm, wdkv_hbm, wkr_hbm, wuk_hbm, wuv_hbm, wout_hbm,
           gq_hbm, gkv_hbm, y_ref, x, pos, wdq, wuq, wqr, wdkv, wkr, wukv, wout, gq, gkv,
           cq, lat, gath, bias, qbd, kn_s, vt_s, m_s, l_s, acc_s, o_own, o_out, o_in, y_acc, s_s, p_s,
           load_sem, send_sem, recv_sem, pair_send, pair_recv):
    me = lax.axis_index('ctx')
    core = lax.rem(me, 2)
    chip = me // 2
    partner = me + 1 - 2 * core
    half = rows // 2
    rank = wdkv.shape[1]
    pair = 2 * rows
    cols = wuq.shape[1]
    groups = cols // LANES
    tables = rope // 2

    barrier = pltpu.get_barrier_semaphore()
    for j in range(1, n):
        pl.semaphore_signal(barrier, inc=1, device_id={'ctx': lax.rem(me + j, n)}, device_id_type=MESH)

    loads = []

    def load(src, dst, sem=None):
        sem = len(loads) if sem is None else sem
        copy = pltpu.make_async_copy(src, dst, load_sem.at[sem])
        copy.start()
        loads.append(copy)
        return copy

    def wait_all(ref, sem):
        pltpu.make_async_copy(ref, ref, sem).wait()

    mine = pl.ds(pl.multiple_of(core * rows, rows), rows)
    head_cols = pl.ds(pl.multiple_of(core * cols, LANES), cols)
    rope_cols = pl.ds(pl.multiple_of(core * wqr.shape[1], LANES), wqr.shape[1])
    d_model = x.shape[1]
    cuts = [(0, 1024), (1024, 1024), (2048, d_model - 2048)]
    ld_pos = load(pos_hbm, pos.at[core])
    ld_x = load(x_hbm, x.at[pl.ds(0, rows), :])
    x[rows:, :] = jnp.zeros((rows, d_model), BF16)
    o_own[rows:, :] = jnp.zeros((rows, cols), BF16)
    o_in[rows:, :] = jnp.zeros((rows, cols), BF16)
    ld_kr = load(wkr_hbm, wkr)
    ld_gkv = load(gkv_hbm, gkv)
    ld_dkv = [load(wdkv_hbm.at[pl.ds(c, h), :], wdkv.at[pl.ds(c, h), :]) for c, h in cuts]
    ld_dq = load(wdq_hbm, wdq)
    ld_gq = load(gq_hbm, gq)
    ld_uq = load(wuq_hbm.at[:, head_cols], wuq)
    ld_qr = load(wqr_hbm.at[:, rope_cols], wqr)
    ukv = len(loads)
    load(wuk_hbm.at[:, head_cols], wukv.at[0], ukv)
    load(wuv_hbm.at[:, head_cols], wukv.at[1], ukv)
    row_a = pl.multiple_of(core * cols, LANES)
    row_b = pl.multiple_of((1 - core) * cols, LANES)
    for row, at in ((row_a, 0), (row_b, cols)):
        load(wout_hbm.at[pl.ds(row, cols), :], wout.at[pl.ds(at, cols), :], ukv + 1)

    def rope_tables(pos_row):
        width = pos_row.shape[1]
        freq = iota((tables, width), 0)
        inv_freq = jnp.zeros((tables, width), F32)
        for i in range(tables):
            inv_freq = jnp.where(freq == i, np.float32(10000.0 ** (-2.0 * i / rope)), inv_freq)
        angles = pos_row.astype(F32) * inv_freq

        def table(vals):
            tall = jnp.concatenate([vals] * (LANES // tables), axis=0)
            if width < LANES:
                tall = jnp.concatenate([tall] * (LANES // width), axis=1)
            return jnp.transpose(tall)[:width, :]

        lead = lax.rem(iota((width, LANES), 1), rope) < tables
        cos_t, sin_t = table(jnp.cos(angles)), table(jnp.sin(angles))
        return cos_t, jnp.where(lead, -sin_t, sin_t), lead

    def rotate(a, tabs):
        cos_t, sin_t, lead = tabs
        other = jnp.where(lead, pltpu.roll(a, LANES - tables, 1), pltpu.roll(a, tables, 1))
        return a * cos_t + other * sin_t

    ld_pos.wait()
    tabs = rope_tables(pos[core])
    ld_x.wait()
    ld_kr.wait()
    kr = dot_nt(x[0:rows, :], wkr[...])
    c_kv = None
    for c, (first, height) in zip(ld_dkv, cuts):
        c.wait()
        term = dot_nn(x[0:rows, first:first + height], wdkv[first:first + height, :])
        c_kv = term if c_kv is None else c_kv + term
    ld_gkv.wait()
    c_kv = rms_rows(c_kv, gkv[...].reshape(1, rank))
    kr = rotate(jnp.concatenate([kr] * (LANES // rope), axis=1), tabs)
    pack = kr[0:16, :]
    lane16 = iota((16, LANES), 1) // rope
    for b in range(1, rows // 16):
        pack = jnp.where(lane16 == b, kr[16 * b:16 * b + 16, :], pack)
    pack = pack.astype(BF16)
    lat[0:rows, :] = c_kv[:, :LANES]
    lat[rows:2 * rows, :] = c_kv[:, LANES:]
    lat[2 * rows:2 * rows + 16, :] = pack
    gath[me, 0:rows, :] = c_kv[:, :LANES]
    gath[me, rows:2 * rows, :] = c_kv[:, LANES:]
    gath[me, 2 * rows:2 * rows + 16, :] = pack

    def query_latents():
        ld_dq.wait()
        ld_gq.wait()
        both = dot_nn(x[...], wdq[...])
        cq[mine, :] = rms_rows(both[:rows, :] + both[rows:, :], gq[...].reshape(1, wdq.shape[1]))

    pl.when(chip == 0)(query_latents)
    pl.semaphore_wait(barrier, n - 1)
    bit0, bit1 = lax.rem(chip, 2), chip // 2
    def send(flip_core, flip_chip, sem):
        flip0, flip1 = lax.rem(flip_chip, 2), flip_chip // 2
        peer_chip = (bit0 + flip0 * (1 - 2 * bit0)) + 2 * (bit1 + flip1 * (1 - 2 * bit1))
        peer = 2 * peer_chip + core + flip_core * (1 - 2 * core)
        pltpu.make_async_remote_copy(
            src_ref=lat, dst_ref=gath.at[me], send_sem=send_sem.at[0], recv_sem=recv_sem.at[sem],
            device_id={'ctx': peer}, device_id_type=MESH).start()

    send(1, 0, 0)
    for k in range(3):
        flip_chip = lax.rem(k + 2 * (chip // 3), 3) + 1
        for flip_core in range(2):
            send(flip_core, flip_chip, (flip_chip + 2) // 2)

    def to_partner(src, dst, index):
        copy = pltpu.make_async_remote_copy(
            src_ref=src, dst_ref=dst, send_sem=pair_send.at[index], recv_sem=pair_recv.at[index],
            device_id={'ctx': partner}, device_id_type=MESH)
        copy.start()
        return copy

    pair_pos = to_partner(pos.at[core], pos.at[core], 0)

    pl.when(chip > 0)(query_latents)
    pair_cq = to_partner(cq.at[mine, :], cq.at[mine, :], 1)
    qbd[...] = jnp.zeros_like(qbd)
    pair_pos.wait()
    pos_row = jnp.concatenate([pos[0], pos[1]], axis=1)
    tabs = rope_tables(pos_row)

    q_in = lax.rem(iota((1, pair), 1), rows)
    q_dev = 2 * chip + iota((1, pair), 1) // rows
    q_tok = jnp.where(q_in < half, half * q_dev + q_in, half * (2 * n - 1 - q_dev) + q_in - half)
    q_first = q_tok - pos_row
    side0, side1 = 1 - 2 * bit0, 2 - 4 * bit1
    chips = (chip, chip + side0, chip + side1, chip + side0 + side1)
    chunks = (chips[:1], chips[1:2], chips[2:])
    for i, owner in enumerate(chips):
        r = iota((pair, pair), 0)
        k_in = lax.rem(r, rows)
        k_dev = 2 * owner + r // rows
        k_tok = jnp.where(k_in < half, half * k_dev + k_in, half * (2 * n - 1 - k_dev) + k_in - half)
        ok = (k_tok <= q_tok) & (k_tok >= q_first)
        bias[i * pair:(i + 1) * pair, :] = jnp.where(ok, jnp.inf, -jnp.inf)

    pair_cq.wait()
    c_q = cq[...]
    ld_uq.wait()
    ld_qr.wait()
    qr_all = dot_nn(c_q, wqr[...])
    q_cols = {c: dot_nn(c_q, wuq[:, c:c + 256]).astype(BF16) for c in range(0, cols, 256)}
    for t in range(groups // 2):
        qt = jnp.transpose(rotate(qr_all[:, LANES * t:LANES * t + LANES], tabs).astype(BF16))
        for k in range(4):
            lo = (k % 2) * pair
            qbd[2 * t + k // 2, LANES + rope * k:LANES + rope * k + rope, lo:lo + pair] = qt[rope * k:rope * k + rope, :]
    for g in range(groups):
        qt = jnp.transpose(q_cols[g // 2 * 256][:, g % 2 * LANES:g % 2 * LANES + LANES])
        qbd[g, 0:nope, 0:pair] = qt[0:nope, :]
        qbd[g, nope:2 * nope, pair:2 * pair] = qt[nope:2 * nope, :]

    spread_r = iota((LANES, 4 * LANES), 0)
    spread_c = iota((LANES, 4 * LANES), 1)
    spread = (spread_r == rope * (spread_c // LANES) + lax.rem(spread_c, rope)).astype(F32).astype(BF16)
    scale2 = (nope + rope) ** -0.5 * math.log2(math.e)
    wait_all(wukv, load_sem.at[ukv])

    pair_o = []

    def send_heads(first, last, index):
        part = pl.ds(first * LANES, (last - first) * LANES)
        return to_partner(o_out.at[:, part], o_in.at[pl.ds(0, rows), part], index)

    def attend(index):
        owners = chunks[index]
        count = 2 * len(owners)
        keys = count * rows
        base = 2 * sum(len(c) for c in chunks[:index])

        def rows_of(first, size):
            parts = [gath[pl.ds(2 * owner, 2), first:first + size, :].reshape(2 * size, LANES) for owner in owners]
            return jnp.concatenate(parts, axis=0)

        c_all = jnp.concatenate([rows_of(0, rows), rows_of(rows, rows)], axis=1)
        wide = dot_nn(rows_of(2 * rows, 16), spread).astype(BF16)
        krep = jnp.concatenate([wide[16 * j:16 * j + 16, LANES * b:LANES * b + LANES] for j in range(count) for b in range(rows // 16)], axis=0)

        def project(c):
            kn_s[0:keys, c:c + 256] = dot_nn(c_all, wukv[0, :, c:c + 256]).astype(BF16)
            vt_s[c:c + 256, 0:keys] = dot_tt(wukv[1, :, c:c + 256], c_all).astype(BF16)

        def score(g):
            s = dot_nn(jnp.concatenate([kn_s[0:keys, g * LANES:(g + 1) * LANES], krep], axis=1), qbd[g])
            tall = None
            for r in range(0, keys, STRIP):
                limit = bias[base * rows + r:base * rows + r + STRIP, :]
                strip = jnp.minimum(s[r:r + STRIP, :], jnp.concatenate([limit, limit], axis=1))
                s_s[g % SLOTS, r:r + STRIP, :] = strip
                for k in range(0, STRIP, 8):
                    tall = strip[k:k + 8, :] if tall is None else jnp.maximum(tall, strip[k:k + 8, :])
            m = jnp.max(tall, axis=0, keepdims=True)
            tops[g] = m if index == 0 else jnp.maximum(m, m_s[g])

        def weigh(g):
            total = None
            for r in range(0, keys, STRIP):
                p = jnp.exp2((s_s[g % SLOTS, r:r + STRIP, :] - tops[g]) * scale2)
                p_s[g % SLOTS, r:r + STRIP, :] = p.astype(BF16)
                for k in range(0, STRIP, 8):
                    total = p[k:k + 8, :] if total is None else total + p[k:k + 8, :]
            sums[g] = jnp.sum(total, axis=0, keepdims=True)

        def mix(g):
            o = dot_nn(vt_s[g * LANES:(g + 1) * LANES, 0:keys], p_s[g % SLOTS, 0:keys, :])
            outs[g] = [o[:nope, :pair], o[nope:, pair:]]

        def finish(g):
            lanes = slice(g * LANES, (g + 1) * LANES)
            m, l, o = tops[g], sums[g], outs[g]
            if index > 0:
                alpha = jnp.exp2((m_s[g] - m) * scale2)
                l = l_s[g] * alpha + l
                o = [acc_s[g, h * nope:(h + 1) * nope, :] * alpha[:, h * pair:(h + 1) * pair] + o[h] for h in range(2)]
            if index < len(chunks) - 1:
                m_s[g] = m
                l_s[g] = l
                acc_s[g, :nope, :] = o[0]
                acc_s[g, nope:, :] = o[1]
            else:
                inv = 1.0 / l
                o = [o[h] * inv[:, h * pair:(h + 1) * pair] for h in range(2)]
                ot = jnp.transpose(jnp.concatenate(o, axis=0).astype(BF16))
                both = [ot[:rows, :], ot[rows:, :]]
                o_own[0:rows, lanes] = jnp.where(core == 0, both[0], both[1])
                o_out[:, lanes] = jnp.where(core == 0, both[1], both[0])
                if g + 1 in SENDS:
                    last = SENDS.index(g + 1)
                    pair_o.append(send_heads(SENDS[last - 1], g + 1, 1 + last))

        tops, sums, outs = {}, {}, {}
        lags = STAGES[len(owners) - 1]
        project(0)
        for t in range(groups + lags[2]):
            if t % 2 == 0 and 0 < t + LEAD < groups:
                project((t + LEAD) * LANES)
            for stage, lag in ((score, 0), (weigh, lags[0]), (mix, lags[1]), (finish, lags[2])):
                if 0 <= t - lag < groups:
                    stage(t - lag)

    wait_all(gath.at[pl.ds(0, 1)], recv_sem.at[0])
    attend(0)
    wait_all(gath.at[pl.ds(0, 2)], recv_sem.at[1])
    attend(1)
    wait_all(gath.at[pl.ds(0, 4)], recv_sem.at[2])
    attend(2)

    wait_all(gath.at[pl.ds(0, n - 1)], send_sem.at[0])
    wait_all(wout, load_sem.at[ukv + 1])
    ov = o_own[...]
    for c in range(0, d_model, OUT_COLS):
        y_acc[:, c:c + OUT_COLS] = dot_nn(ov, wout[:cols, c:c + OUT_COLS])
    for i, copy in enumerate(pair_o):
        copy.wait()
        first, last = SENDS[i] * LANES, SENDS[i + 1] * LANES
        ov = o_in[:, first:last]
        for c in range(0, d_model, OUT_COLS):
            out = y_acc[:, c:c + OUT_COLS] + dot_nn(ov, wout[cols + first:cols + last, c:c + OUT_COLS])
            if last < cols:
                y_acc[:, c:c + OUT_COLS] = out
            else:
                y_ref[:, c:c + OUT_COLS] = (out[:rows, :] + out[rows:, :]).astype(BF16)


def solution(mesh):
    n = mesh.shape['ctx']
    row_spec = P(('dp', 'ctx'), None)
    id_spec = P(('dp', 'ctx'))

    def per_device(x_rows, pos_rows, seg_rows, w_dq, w_uq, w_qr, w_dkv, w_kr, w_uk, w_uv, w_out, gain_q, gain_kv):
        rows, d_model = x_rows.shape
        rope = w_kr.shape[1]
        nope = w_uq.shape[1] * rope // w_qr.shape[1]
        cols = w_uq.shape[1] // 2
        groups = cols // LANES
        keys = n // 2 * rows
        operands = (x_rows, pos_rows.reshape(1, rows), w_dq, w_uq, w_qr, w_dkv, w_kr.T, w_uk, w_uv, w_out, gain_q, gain_kv)
        operands = tuple(pltpu.with_memory_space_constraint(a, pltpu.HBM) for a in operands)
        vm = lambda a: pltpu.VMEM(a.shape, a.dtype)
        cut = lambda a: pltpu.VMEM((a.shape[0], a.shape[1] // 2), a.dtype)
        return pl.pallas_call(
            functools.partial(kernel, n, rows, rope, nope),
            out_shape=jax.ShapeDtypeStruct((rows, w_out.shape[1]), BF16),
            in_specs=[pl.BlockSpec(memory_space=pl.ANY)] * len(operands),
            out_specs=pl.BlockSpec(memory_space=pltpu.VMEM),
            scratch_shapes=[
                pltpu.VMEM((2 * rows, d_model), BF16),
                pltpu.VMEM((2, 1, rows), jnp.int32),
                vm(w_dq), cut(w_uq), cut(w_qr), vm(w_dkv), vm(w_kr.T),
                pltpu.VMEM((2, w_uk.shape[0], cols), BF16),
                vm(w_out), vm(gain_q), vm(gain_kv),
                pltpu.VMEM((2 * rows, w_dq.shape[1]), BF16),
                pltpu.VMEM((2 * rows + 16, LANES), BF16),
                pltpu.VMEM((n, 2 * rows + 16, LANES), BF16),
                pltpu.VMEM((n * rows, 2 * rows), F32),
                pltpu.VMEM((groups, 2 * LANES, 4 * rows), BF16),
                pltpu.VMEM((keys, cols), BF16),
                pltpu.VMEM((cols, keys), BF16),
                pltpu.VMEM((groups, 1, 4 * rows), F32),
                pltpu.VMEM((groups, 1, 4 * rows), F32),
                pltpu.VMEM((groups, 2 * nope, 2 * rows), F32),
                pltpu.VMEM((2 * rows, cols), BF16),
                pltpu.VMEM((rows, cols), BF16),
                pltpu.VMEM((2 * rows, cols), BF16),
                pltpu.VMEM((2 * rows, w_out.shape[1]), F32),
                pltpu.VMEM((SLOTS, keys, 4 * rows), F32),
                pltpu.VMEM((SLOTS, keys, 4 * rows), BF16),
                pltpu.SemaphoreType.DMA((13,)),
                pltpu.SemaphoreType.DMA((1,)),
                pltpu.SemaphoreType.DMA((3,)),
                pltpu.SemaphoreType.DMA((1 + len(SENDS),)),
                pltpu.SemaphoreType.DMA((1 + len(SENDS),)),
            ],
            compiler_params=pltpu.CompilerParams(collective_id=0, has_side_effects=True, vmem_limit_bytes=42 * 1024 * 1024),
        )(*operands)

    return jax.shard_map(per_device, mesh=mesh, in_specs=(row_spec, id_spec, id_spec) + (P(),) * 10, out_specs=row_spec, check_vma=False)
```

```python
import functools
import math

import numpy as np
import jax
import jax.numpy as jnp
from jax import lax
from jax.experimental import pallas as pl
from jax.experimental.pallas import tpu as pltpu
from jax.sharding import PartitionSpec as P

NORM_EPS = 1e-6
MESH = pl.DeviceIdType.MESH
F32 = jnp.float32
BF16 = jnp.bfloat16
LANES = 128
STAGES = ((4, 6, 8), (2, 4, 6))
LEAD = 2
SLOTS = 10
SENDS = (0, 4, 10)
OUT_COLS = 512
STRIP = 32


def rms_rows(vals, gain):
    mean_sq = jnp.mean(vals * vals, axis=-1, keepdims=True)
    return (vals * lax.rsqrt(mean_sq + NORM_EPS) * gain.astype(F32)).astype(BF16)


def dot_nn(a, b):
    return lax.dot_general(a, b, (((1,), (0,)), ((), ())), preferred_element_type=F32)


def dot_nt(a, b):
    return lax.dot_general(a, b, (((1,), (1,)), ((), ())), preferred_element_type=F32)


def dot_tt(a, b):
    return lax.dot_general(a, b, (((0,), (1,)), ((), ())), preferred_element_type=F32)


def iota(shape, axis):
    return lax.broadcasted_iota(jnp.int32, shape, axis)


def kernel(n, rows, rope, nope, x_hbm, pos_hbm, wdq_hbm, wuq_hbm, wqr_hbm, wdkv_hbm, wkr_hbm, wuk_hbm, wuv_hbm, wout_hbm,
           gq_hbm, gkv_hbm, y_ref, x, pos, wdq, wuq, wqr, wdkv, wkr, wukv, wout, gq, gkv,
           cq, lat, gath, bias, qbd, kn_s, vt_s, m_s, l_s, acc_s, o_own, o_out, o_in, y_acc, s_s, p_s,
           load_sem, send_sem, recv_sem, pair_send, pair_recv):
    me = lax.axis_index('ctx')
    core = lax.rem(me, 2)
    chip = me // 2
    partner = me + 1 - 2 * core
    half = rows // 2
    rank = wdkv.shape[1]
    pair = 2 * rows
    cols = wuq.shape[1]
    groups = cols // LANES
    tables = rope // 2

    barrier = pltpu.get_barrier_semaphore()
    for j in range(1, n):
        pl.semaphore_signal(barrier, inc=1, device_id={'ctx': lax.rem(me + j, n)}, device_id_type=MESH)

    loads = []

    def load(src, dst, sem=None):
        sem = len(loads) if sem is None else sem
        copy = pltpu.make_async_copy(src, dst, load_sem.at[sem])
        copy.start()
        loads.append(copy)
        return copy

    def wait_all(ref, sem):
        pltpu.make_async_copy(ref, ref, sem).wait()

    mine = pl.ds(pl.multiple_of(core * rows, rows), rows)
    head_cols = pl.ds(pl.multiple_of(core * cols, LANES), cols)
    rope_cols = pl.ds(pl.multiple_of(core * wqr.shape[1], LANES), wqr.shape[1])
    d_model = x.shape[1]
    cuts = [(0, 1024), (1024, 1024), (2048, d_model - 2048)]
    ld_pos = load(pos_hbm, pos.at[core])
    ld_x = load(x_hbm, x.at[pl.ds(0, rows), :])
    x[rows:, :] = jnp.zeros((rows, d_model), BF16)
    o_own[rows:, :] = jnp.zeros((rows, cols), BF16)
    o_in[rows:, :] = jnp.zeros((rows, cols), BF16)
    ld_kr = load(wkr_hbm, wkr)
    ld_gkv = load(gkv_hbm, gkv)
    ld_dkv = [load(wdkv_hbm.at[pl.ds(c, h), :], wdkv.at[pl.ds(c, h), :]) for c, h in cuts]
    ld_dq = load(wdq_hbm, wdq)
    ld_gq = load(gq_hbm, gq)
    ld_uq = load(wuq_hbm.at[:, head_cols], wuq)
    ld_qr = load(wqr_hbm.at[:, rope_cols], wqr)
    ukv = len(loads)
    load(wuk_hbm.at[:, head_cols], wukv.at[0], ukv)
    load(wuv_hbm.at[:, head_cols], wukv.at[1], ukv)
    row_a = pl.multiple_of(core * cols, LANES)
    row_b = pl.multiple_of((1 - core) * cols, LANES)
    for row, at in ((row_a, 0), (row_b, cols)):
        load(wout_hbm.at[pl.ds(row, cols), :], wout.at[pl.ds(at, cols), :], ukv + 1)

    def rope_tables(pos_row):
        width = pos_row.shape[1]
        freq = iota((tables, width), 0)
        inv_freq = jnp.zeros((tables, width), F32)
        for i in range(tables):
            inv_freq = jnp.where(freq == i, np.float32(10000.0 ** (-2.0 * i / rope)), inv_freq)
        angles = pos_row.astype(F32) * inv_freq

        def table(vals):
            tall = jnp.concatenate([vals] * (LANES // tables), axis=0)
            if width < LANES:
                tall = jnp.concatenate([tall] * (LANES // width), axis=1)
            return jnp.transpose(tall)[:width, :]

        lead = lax.rem(iota((width, LANES), 1), rope) < tables
        cos_t, sin_t = table(jnp.cos(angles)), table(jnp.sin(angles))
        return cos_t, jnp.where(lead, -sin_t, sin_t), lead

    def rotate(a, tabs):
        cos_t, sin_t, lead = tabs
        other = jnp.where(lead, pltpu.roll(a, LANES - tables, 1), pltpu.roll(a, tables, 1))
        return a * cos_t + other * sin_t

    ld_pos.wait()
    tabs = rope_tables(pos[core])
    ld_x.wait()
    ld_kr.wait()
    kr = dot_nt(x[0:rows, :], wkr[...])
    c_kv = None
    for c, (first, height) in zip(ld_dkv, cuts):
        c.wait()
        term = dot_nn(x[0:rows, first:first + height], wdkv[first:first + height, :])
        c_kv = term if c_kv is None else c_kv + term
    ld_gkv.wait()
    c_kv = rms_rows(c_kv, gkv[...].reshape(1, rank))
    kr = rotate(jnp.concatenate([kr] * (LANES // rope), axis=1), tabs)
    pack = kr[0:16, :]
    lane16 = iota((16, LANES), 1) // rope
    for b in range(1, rows // 16):
        pack = jnp.where(lane16 == b, kr[16 * b:16 * b + 16, :], pack)
    pack = pack.astype(BF16)
    lat[0:rows, :] = c_kv[:, :LANES]
    lat[rows:2 * rows, :] = c_kv[:, LANES:]
    lat[2 * rows:2 * rows + 16, :] = pack
    gath[me, 0:rows, :] = c_kv[:, :LANES]
    gath[me, rows:2 * rows, :] = c_kv[:, LANES:]
    gath[me, 2 * rows:2 * rows + 16, :] = pack

    def query_latents():
        ld_dq.wait()
        ld_gq.wait()
        both = dot_nn(x[...], wdq[...])
        cq[mine, :] = rms_rows(both[:rows, :] + both[rows:, :], gq[...].reshape(1, wdq.shape[1]))

    pl.when(chip == 0)(query_latents)
    pl.semaphore_wait(barrier, n - 1)
    bit0, bit1 = lax.rem(chip, 2), chip // 2
    def send(flip_core, flip_chip, sem):
        flip0, flip1 = lax.rem(flip_chip, 2), flip_chip // 2
        peer_chip = (bit0 + flip0 * (1 - 2 * bit0)) + 2 * (bit1 + flip1 * (1 - 2 * bit1))
        peer = 2 * peer_chip + core + flip_core * (1 - 2 * core)
        pltpu.make_async_remote_copy(
            src_ref=lat, dst_ref=gath.at[me], send_sem=send_sem.at[0], recv_sem=recv_sem.at[sem],
            device_id={'ctx': peer}, device_id_type=MESH).start()

    send(1, 0, 0)
    for k in range(3):
        flip_chip = lax.rem(k + 2 * bit1, 3) + 1
        for flip_core in range(2):
            send(flip_core, flip_chip, (flip_chip + 2) // 2)

    def to_partner(src, dst, index):
        copy = pltpu.make_async_remote_copy(
            src_ref=src, dst_ref=dst, send_sem=pair_send.at[index], recv_sem=pair_recv.at[index],
            device_id={'ctx': partner}, device_id_type=MESH)
        copy.start()
        return copy

    pair_pos = to_partner(pos.at[core], pos.at[core], 0)

    pl.when(chip > 0)(query_latents)
    pair_cq = to_partner(cq.at[mine, :], cq.at[mine, :], 1)
    qbd[...] = jnp.zeros_like(qbd)
    pair_pos.wait()
    pos_row = jnp.concatenate([pos[0], pos[1]], axis=1)
    tabs = rope_tables(pos_row)

    q_in = lax.rem(iota((1, pair), 1), rows)
    q_dev = 2 * chip + iota((1, pair), 1) // rows
    q_tok = jnp.where(q_in < half, half * q_dev + q_in, half * (2 * n - 1 - q_dev) + q_in - half)
    q_first = q_tok - pos_row
    side0, side1 = 1 - 2 * bit0, 2 - 4 * bit1
    chips = (chip, chip + side0, chip + side1, chip + side0 + side1)
    chunks = (chips[:1], chips[1:2], chips[2:])
    for i, owner in enumerate(chips):
        r = iota((pair, pair), 0)
        k_in = lax.rem(r, rows)
        k_dev = 2 * owner + r // rows
        k_tok = jnp.where(k_in < half, half * k_dev + k_in, half * (2 * n - 1 - k_dev) + k_in - half)
        ok = (k_tok <= q_tok) & (k_tok >= q_first)
        bias[i * pair:(i + 1) * pair, :] = jnp.where(ok, jnp.inf, -jnp.inf)

    pair_cq.wait()
    c_q = cq[...]
    ld_uq.wait()
    ld_qr.wait()
    qr_all = dot_nn(c_q, wqr[...])
    q_cols = {c: dot_nn(c_q, wuq[:, c:c + 256]).astype(BF16) for c in range(0, cols, 256)}
    for t in range(groups // 2):
        qt = jnp.transpose(rotate(qr_all[:, LANES * t:LANES * t + LANES], tabs).astype(BF16))
        for k in range(4):
            lo = (k % 2) * pair
            qbd[2 * t + k // 2, LANES + rope * k:LANES + rope * k + rope, lo:lo + pair] = qt[rope * k:rope * k + rope, :]
    for g in range(groups):
        qt = jnp.transpose(q_cols[g // 2 * 256][:, g % 2 * LANES:g % 2 * LANES + LANES])
        qbd[g, 0:nope, 0:pair] = qt[0:nope, :]
        qbd[g, nope:2 * nope, pair:2 * pair] = qt[nope:2 * nope, :]

    spread_r = iota((LANES, 4 * LANES), 0)
    spread_c = iota((LANES, 4 * LANES), 1)
    spread = (spread_r == rope * (spread_c // LANES) + lax.rem(spread_c, rope)).astype(F32).astype(BF16)
    scale2 = (nope + rope) ** -0.5 * math.log2(math.e)
    wait_all(wukv, load_sem.at[ukv])

    pair_o = []

    def send_heads(first, last, index):
        part = pl.ds(first * LANES, (last - first) * LANES)
        return to_partner(o_out.at[:, part], o_in.at[pl.ds(0, rows), part], index)

    def attend(index):
        owners = chunks[index]
        count = 2 * len(owners)
        keys = count * rows
        base = 2 * sum(len(c) for c in chunks[:index])

        def rows_of(first, size):
            parts = [gath[pl.ds(2 * owner, 2), first:first + size, :].reshape(2 * size, LANES) for owner in owners]
            return jnp.concatenate(parts, axis=0)

        c_all = jnp.concatenate([rows_of(0, rows), rows_of(rows, rows)], axis=1)
        wide = dot_nn(rows_of(2 * rows, 16), spread).astype(BF16)
        krep = jnp.concatenate([wide[16 * j:16 * j + 16, LANES * b:LANES * b + LANES] for j in range(count) for b in range(rows // 16)], axis=0)

        def project(c):
            kn_s[0:keys, c:c + 256] = dot_nn(c_all, wukv[0, :, c:c + 256]).astype(BF16)
            if keys > LANES:
                vt_s[c:c + 256, 0:keys] = dot_tt(wukv[1, :, c:c + 256], c_all).astype(BF16)
            else:
                vals = dot_nn(c_all, wukv[1, :, c:c + 256]).astype(BF16)
                for t in range(0, 256, LANES):
                    vt_s[c + t:c + t + LANES, 0:keys] = jnp.transpose(vals[:, t:t + LANES])

        def score(g):
            s = dot_nn(jnp.concatenate([kn_s[0:keys, g * LANES:(g + 1) * LANES], krep], axis=1), qbd[g])
            tall = None
            for r in range(0, keys, STRIP):
                limit = bias[base * rows + r:base * rows + r + STRIP, :]
                strip = jnp.minimum(s[r:r + STRIP, :], jnp.concatenate([limit, limit], axis=1))
                s_s[g % SLOTS, r:r + STRIP, :] = strip
                for k in range(0, STRIP, 8):
                    tall = strip[k:k + 8, :] if tall is None else jnp.maximum(tall, strip[k:k + 8, :])
            m = jnp.max(tall, axis=0, keepdims=True)
            tops[g] = m if index == 0 else jnp.maximum(m, m_s[g])

        def weigh(g):
            total = None
            for r in range(0, keys, STRIP):
                p = jnp.exp2((s_s[g % SLOTS, r:r + STRIP, :] - tops[g]) * scale2)
                p_s[g % SLOTS, r:r + STRIP, :] = p.astype(BF16)
                for k in range(0, STRIP, 8):
                    total = p[k:k + 8, :] if total is None else total + p[k:k + 8, :]
            sums[g] = jnp.sum(total, axis=0, keepdims=True)

        def mix(g):
            o = dot_nn(vt_s[g * LANES:(g + 1) * LANES, 0:keys], p_s[g % SLOTS, 0:keys, :])
            outs[g] = [o[:nope, :pair], o[nope:, pair:]]

        def finish(g):
            lanes = slice(g * LANES, (g + 1) * LANES)
            m, l, o = tops[g], sums[g], outs[g]
            if index > 0:
                alpha = jnp.exp2((m_s[g] - m) * scale2)
                l = l_s[g] * alpha + l
                o = [acc_s[g, h * nope:(h + 1) * nope, :] * alpha[:, h * pair:(h + 1) * pair] + o[h] for h in range(2)]
            if index < len(chunks) - 1:
                m_s[g] = m
                l_s[g] = l
                acc_s[g, :nope, :] = o[0]
                acc_s[g, nope:, :] = o[1]
            else:
                inv = 1.0 / l
                o = [o[h] * inv[:, h * pair:(h + 1) * pair] for h in range(2)]
                ot = jnp.transpose(jnp.concatenate(o, axis=0).astype(BF16))
                both = [ot[:rows, :], ot[rows:, :]]
                o_own[0:rows, lanes] = jnp.where(core == 0, both[0], both[1])
                o_out[:, lanes] = jnp.where(core == 0, both[1], both[0])
                if g + 1 in SENDS:
                    last = SENDS.index(g + 1)
                    pair_o.append(send_heads(SENDS[last - 1], g + 1, 1 + last))

        tops, sums, outs = {}, {}, {}
        lags = STAGES[len(owners) - 1]
        project(0)
        for t in range(groups + lags[2]):
            if t % 2 == 0 and 0 < t + LEAD < groups:
                project((t + LEAD) * LANES)
            for stage, lag in ((score, 0), (weigh, lags[0]), (mix, lags[1]), (finish, lags[2])):
                if 0 <= t - lag < groups:
                    stage(t - lag)

    wait_all(gath.at[pl.ds(0, 1)], recv_sem.at[0])
    attend(0)
    wait_all(gath.at[pl.ds(0, 2)], recv_sem.at[1])
    attend(1)
    wait_all(gath.at[pl.ds(0, 4)], recv_sem.at[2])
    attend(2)

    wait_all(gath.at[pl.ds(0, n - 1)], send_sem.at[0])
    wait_all(wout, load_sem.at[ukv + 1])
    ov = o_own[...]
    for c in range(0, d_model, OUT_COLS):
        y_acc[:, c:c + OUT_COLS] = dot_nn(ov, wout[:cols, c:c + OUT_COLS])
    for i, copy in enumerate(pair_o):
        copy.wait()
        first, last = SENDS[i] * LANES, SENDS[i + 1] * LANES
        ov = o_in[:, first:last]
        for c in range(0, d_model, OUT_COLS):
            out = y_acc[:, c:c + OUT_COLS] + dot_nn(ov, wout[cols + first:cols + last, c:c + OUT_COLS])
            if last < cols:
                y_acc[:, c:c + OUT_COLS] = out
            else:
                y_ref[:, c:c + OUT_COLS] = (out[:rows, :] + out[rows:, :]).astype(BF16)


def solution(mesh):
    n = mesh.shape['ctx']
    row_spec = P(('dp', 'ctx'), None)
    id_spec = P(('dp', 'ctx'))

    def per_device(x_rows, pos_rows, seg_rows, w_dq, w_uq, w_qr, w_dkv, w_kr, w_uk, w_uv, w_out, gain_q, gain_kv):
        rows, d_model = x_rows.shape
        rope = w_kr.shape[1]
        nope = w_uq.shape[1] * rope // w_qr.shape[1]
        cols = w_uq.shape[1] // 2
        groups = cols // LANES
        keys = n // 2 * rows
        operands = (x_rows, pos_rows.reshape(1, rows), w_dq, w_uq, w_qr, w_dkv, w_kr.T, w_uk, w_uv, w_out, gain_q, gain_kv)
        operands = tuple(pltpu.with_memory_space_constraint(a, pltpu.HBM) for a in operands)
        vm = lambda a: pltpu.VMEM(a.shape, a.dtype)
        cut = lambda a: pltpu.VMEM((a.shape[0], a.shape[1] // 2), a.dtype)
        return pl.pallas_call(
            functools.partial(kernel, n, rows, rope, nope),
            out_shape=jax.ShapeDtypeStruct((rows, w_out.shape[1]), BF16),
            in_specs=[pl.BlockSpec(memory_space=pl.ANY)] * len(operands),
            out_specs=pl.BlockSpec(memory_space=pltpu.VMEM),
            scratch_shapes=[
                pltpu.VMEM((2 * rows, d_model), BF16),
                pltpu.VMEM((2, 1, rows), jnp.int32),
                vm(w_dq), cut(w_uq), cut(w_qr), vm(w_dkv), vm(w_kr.T),
                pltpu.VMEM((2, w_uk.shape[0], cols), BF16),
                vm(w_out), vm(gain_q), vm(gain_kv),
                pltpu.VMEM((2 * rows, w_dq.shape[1]), BF16),
                pltpu.VMEM((2 * rows + 16, LANES), BF16),
                pltpu.VMEM((n, 2 * rows + 16, LANES), BF16),
                pltpu.VMEM((n * rows, 2 * rows), F32),
                pltpu.VMEM((groups, 2 * LANES, 4 * rows), BF16),
                pltpu.VMEM((keys, cols), BF16),
                pltpu.VMEM((cols, keys), BF16),
                pltpu.VMEM((groups, 1, 4 * rows), F32),
                pltpu.VMEM((groups, 1, 4 * rows), F32),
                pltpu.VMEM((groups, 2 * nope, 2 * rows), F32),
                pltpu.VMEM((2 * rows, cols), BF16),
                pltpu.VMEM((rows, cols), BF16),
                pltpu.VMEM((2 * rows, cols), BF16),
                pltpu.VMEM((2 * rows, w_out.shape[1]), F32),
                pltpu.VMEM((SLOTS, keys, 4 * rows), F32),
                pltpu.VMEM((SLOTS, keys, 4 * rows), BF16),
                pltpu.SemaphoreType.DMA((13,)),
                pltpu.SemaphoreType.DMA((1,)),
                pltpu.SemaphoreType.DMA((3,)),
                pltpu.SemaphoreType.DMA((1 + len(SENDS),)),
                pltpu.SemaphoreType.DMA((1 + len(SENDS),)),
            ],
            compiler_params=pltpu.CompilerParams(collective_id=0, has_side_effects=True, vmem_limit_bytes=42 * 1024 * 1024),
        )(*operands)

    return jax.shard_map(per_device, mesh=mesh, in_specs=(row_spec, id_spec, id_spec) + (P(),) * 10, out_specs=row_spec, check_vma=False)
```

```python
import functools
import math

import numpy as np
import jax
import jax.numpy as jnp
from jax import lax
from jax.experimental import pallas as pl
from jax.experimental.pallas import tpu as pltpu
from jax.sharding import PartitionSpec as P

NORM_EPS = 1e-6
MESH = pl.DeviceIdType.MESH
F32 = jnp.float32
BF16 = jnp.bfloat16
LANES = 128
STAGES = ((4, 6, 8), (2, 4, 6))
LEAD = 2
SLOTS = 10
SENDS = (0, 4, 10)
OUT_COLS = 512
STRIP = 32


def rms_rows(vals, gain):
    mean_sq = jnp.mean(vals * vals, axis=-1, keepdims=True)
    return (vals * lax.rsqrt(mean_sq + NORM_EPS) * gain.astype(F32)).astype(BF16)


def dot_nn(a, b):
    return lax.dot_general(a, b, (((1,), (0,)), ((), ())), preferred_element_type=F32)


def dot_nt(a, b):
    return lax.dot_general(a, b, (((1,), (1,)), ((), ())), preferred_element_type=F32)


def dot_tt(a, b):
    return lax.dot_general(a, b, (((0,), (1,)), ((), ())), preferred_element_type=F32)


def iota(shape, axis):
    return lax.broadcasted_iota(jnp.int32, shape, axis)


def kernel(n, rows, rope, nope, x_hbm, pos_hbm, wdq_hbm, wuq_hbm, wqr_hbm, wdkv_hbm, wkr_hbm, wuk_hbm, wuv_hbm, wout_hbm,
           gq_hbm, gkv_hbm, y_ref, x, pos, wdq, wuq, wqr, wdkv, wkr, wukv, wout, gq, gkv,
           cq, lat, gath, bias, qbd, kn_s, vt_s, m_s, l_s, acc_s, o_own, o_out, o_in, y_acc, s_s, p_s,
           load_sem, send_sem, recv_sem, pair_send, pair_recv):
    me = lax.axis_index('ctx')
    core = lax.rem(me, 2)
    chip = me // 2
    partner = me + 1 - 2 * core
    half = rows // 2
    rank = wdkv.shape[1]
    pair = 2 * rows
    cols = wuq.shape[1]
    groups = cols // LANES
    tables = rope // 2

    barrier = pltpu.get_barrier_semaphore()
    for j in range(1, n):
        pl.semaphore_signal(barrier, inc=1, device_id={'ctx': lax.rem(me + j, n)}, device_id_type=MESH)

    loads = []

    def load(src, dst, sem=None):
        sem = len(loads) if sem is None else sem
        copy = pltpu.make_async_copy(src, dst, load_sem.at[sem])
        copy.start()
        loads.append(copy)
        return copy

    def wait_all(ref, sem):
        pltpu.make_async_copy(ref, ref, sem).wait()

    mine = pl.ds(pl.multiple_of(core * rows, rows), rows)
    head_cols = pl.ds(pl.multiple_of(core * cols, LANES), cols)
    rope_cols = pl.ds(pl.multiple_of(core * wqr.shape[1], LANES), wqr.shape[1])
    d_model = x.shape[1]
    cuts = [(0, 1280), (1280, 768), (2048, d_model - 2048)]
    ld_pos = load(pos_hbm, pos.at[core])
    ld_x = load(x_hbm, x.at[pl.ds(0, rows), :])
    x[rows:, :] = jnp.zeros((rows, d_model), BF16)
    o_own[rows:, :] = jnp.zeros((rows, cols), BF16)
    o_in[rows:, :] = jnp.zeros((rows, cols), BF16)
    ld_kr = load(wkr_hbm, wkr)
    ld_gkv = load(gkv_hbm, gkv)
    ld_dkv = [load(wdkv_hbm.at[pl.ds(c, h), :], wdkv.at[pl.ds(c, h), :]) for c, h in cuts]
    ld_dq = load(wdq_hbm, wdq)
    ld_gq = load(gq_hbm, gq)
    ld_uq = load(wuq_hbm.at[:, head_cols], wuq)
    ld_qr = load(wqr_hbm.at[:, rope_cols], wqr)
    ukv = len(loads)
    load(wuk_hbm.at[:, head_cols], wukv.at[0], ukv)
    load(wuv_hbm.at[:, head_cols], wukv.at[1], ukv)
    row_a = pl.multiple_of(core * cols, LANES)
    row_b = pl.multiple_of((1 - core) * cols, LANES)
    for row, at in ((row_a, 0), (row_b, cols)):
        load(wout_hbm.at[pl.ds(row, cols), :], wout.at[pl.ds(at, cols), :], ukv + 1)

    def rope_tables(pos_row):
        width = pos_row.shape[1]
        freq = iota((tables, width), 0)
        inv_freq = jnp.zeros((tables, width), F32)
        for i in range(tables):
            inv_freq = jnp.where(freq == i, np.float32(10000.0 ** (-2.0 * i / rope)), inv_freq)
        angles = pos_row.astype(F32) * inv_freq

        def table(vals):
            tall = jnp.concatenate([vals] * (LANES // tables), axis=0)
            if width < LANES:
                tall = jnp.concatenate([tall] * (LANES // width), axis=1)
            return jnp.transpose(tall)[:width, :]

        lead = lax.rem(iota((width, LANES), 1), rope) < tables
        cos_t, sin_t = table(jnp.cos(angles)), table(jnp.sin(angles))
        return cos_t, jnp.where(lead, -sin_t, sin_t), lead

    def rotate(a, tabs):
        cos_t, sin_t, lead = tabs
        other = jnp.where(lead, pltpu.roll(a, LANES - tables, 1), pltpu.roll(a, tables, 1))
        return a * cos_t + other * sin_t

    ld_pos.wait()
    tabs = rope_tables(pos[core])
    ld_x.wait()
    ld_kr.wait()
    kr = dot_nt(x[0:rows, :], wkr[...])
    c_kv = None
    for c, (first, height) in zip(ld_dkv, cuts):
        c.wait()
        term = dot_nn(x[0:rows, first:first + height], wdkv[first:first + height, :])
        c_kv = term if c_kv is None else c_kv + term
    ld_gkv.wait()
    c_kv = rms_rows(c_kv, gkv[...].reshape(1, rank))
    kr = rotate(jnp.concatenate([kr] * (LANES // rope), axis=1), tabs)
    pack = kr[0:16, :]
    lane16 = iota((16, LANES), 1) // rope
    for b in range(1, rows // 16):
        pack = jnp.where(lane16 == b, kr[16 * b:16 * b + 16, :], pack)
    pack = pack.astype(BF16)
    lat[0:rows, :] = c_kv[:, :LANES]
    lat[rows:2 * rows, :] = c_kv[:, LANES:]
    lat[2 * rows:2 * rows + 16, :] = pack
    gath[me, 0:rows, :] = c_kv[:, :LANES]
    gath[me, rows:2 * rows, :] = c_kv[:, LANES:]
    gath[me, 2 * rows:2 * rows + 16, :] = pack

    def query_latents():
        ld_dq.wait()
        ld_gq.wait()
        both = dot_nn(x[...], wdq[...])
        cq[mine, :] = rms_rows(both[:rows, :] + both[rows:, :], gq[...].reshape(1, wdq.shape[1]))

    pl.when(chip == 0)(query_latents)
    pl.semaphore_wait(barrier, n - 1)
    bit0, bit1 = lax.rem(chip, 2), chip // 2
    def send(flip_core, flip_chip, sem):
        flip0, flip1 = lax.rem(flip_chip, 2), flip_chip // 2
        peer_chip = (bit0 + flip0 * (1 - 2 * bit0)) + 2 * (bit1 + flip1 * (1 - 2 * bit1))
        peer = 2 * peer_chip + core + flip_core * (1 - 2 * core)
        pltpu.make_async_remote_copy(
            src_ref=lat, dst_ref=gath.at[me], send_sem=send_sem.at[0], recv_sem=recv_sem.at[sem],
            device_id={'ctx': peer}, device_id_type=MESH).start()

    send(1, 0, 0)
    for k in range(3):
        flip_chip = lax.rem(k + 2 * bit1, 3) + 1
        for flip_core in range(2):
            send(flip_core, flip_chip, (flip_chip + 2) // 2)

    def to_partner(src, dst, index):
        copy = pltpu.make_async_remote_copy(
            src_ref=src, dst_ref=dst, send_sem=pair_send.at[index], recv_sem=pair_recv.at[index],
            device_id={'ctx': partner}, device_id_type=MESH)
        copy.start()
        return copy

    pair_pos = to_partner(pos.at[core], pos.at[core], 0)

    pl.when(chip > 0)(query_latents)
    pair_cq = to_partner(cq.at[mine, :], cq.at[mine, :], 1)
    qbd[...] = jnp.zeros_like(qbd)
    pair_pos.wait()
    pos_row = jnp.concatenate([pos[0], pos[1]], axis=1)
    tabs = rope_tables(pos_row)

    q_in = lax.rem(iota((1, pair), 1), rows)
    q_dev = 2 * chip + iota((1, pair), 1) // rows
    q_tok = jnp.where(q_in < half, half * q_dev + q_in, half * (2 * n - 1 - q_dev) + q_in - half)
    q_first = q_tok - pos_row
    side0, side1 = 1 - 2 * bit0, 2 - 4 * bit1
    chips = (chip, chip + side0, chip + side1, chip + side0 + side1)
    chunks = (chips[:1], chips[1:2], chips[2:])
    for i, owner in enumerate(chips):
        r = iota((pair, pair), 0)
        k_in = lax.rem(r, rows)
        k_dev = 2 * owner + r // rows
        k_tok = jnp.where(k_in < half, half * k_dev + k_in, half * (2 * n - 1 - k_dev) + k_in - half)
        ok = (k_tok <= q_tok) & (k_tok >= q_first)
        bias[i * pair:(i + 1) * pair, :] = jnp.where(ok, jnp.inf, -jnp.inf)

    pair_cq.wait()
    c_q = cq[...]
    ld_uq.wait()
    ld_qr.wait()
    qr_all = dot_nn(c_q, wqr[...])
    q_cols = {c: dot_nn(c_q, wuq[:, c:c + 256]).astype(BF16) for c in range(0, cols, 256)}
    for t in range(groups // 2):
        qt = jnp.transpose(rotate(qr_all[:, LANES * t:LANES * t + LANES], tabs).astype(BF16))
        for k in range(4):
            lo = (k % 2) * pair
            qbd[2 * t + k // 2, LANES + rope * k:LANES + rope * k + rope, lo:lo + pair] = qt[rope * k:rope * k + rope, :]
    for g in range(groups):
        qt = jnp.transpose(q_cols[g // 2 * 256][:, g % 2 * LANES:g % 2 * LANES + LANES])
        qbd[g, 0:nope, 0:pair] = qt[0:nope, :]
        qbd[g, nope:2 * nope, pair:2 * pair] = qt[nope:2 * nope, :]

    spread_r = iota((LANES, 4 * LANES), 0)
    spread_c = iota((LANES, 4 * LANES), 1)
    spread = (spread_r == rope * (spread_c // LANES) + lax.rem(spread_c, rope)).astype(F32).astype(BF16)
    scale2 = (nope + rope) ** -0.5 * math.log2(math.e)
    wait_all(wukv, load_sem.at[ukv])

    pair_o = []

    def send_heads(first, last, index):
        part = pl.ds(first * LANES, (last - first) * LANES)
        return to_partner(o_out.at[:, part], o_in.at[pl.ds(0, rows), part], index)

    def attend(index):
        owners = chunks[index]
        count = 2 * len(owners)
        keys = count * rows
        base = 2 * sum(len(c) for c in chunks[:index])

        def rows_of(first, size):
            parts = [gath[pl.ds(2 * owner, 2), first:first + size, :].reshape(2 * size, LANES) for owner in owners]
            return jnp.concatenate(parts, axis=0)

        c_all = jnp.concatenate([rows_of(0, rows), rows_of(rows, rows)], axis=1)
        wide = dot_nn(rows_of(2 * rows, 16), spread).astype(BF16)
        krep = jnp.concatenate([wide[16 * j:16 * j + 16, LANES * b:LANES * b + LANES] for j in range(count) for b in range(rows // 16)], axis=0)

        def project(c):
            kn_s[0:keys, c:c + 256] = dot_nn(c_all, wukv[0, :, c:c + 256]).astype(BF16)
            if keys > LANES:
                vt_s[c:c + 256, 0:keys] = dot_tt(wukv[1, :, c:c + 256], c_all).astype(BF16)
            else:
                vals = dot_nn(c_all, wukv[1, :, c:c + 256]).astype(BF16)
                for t in range(0, 256, LANES):
                    vt_s[c + t:c + t + LANES, 0:keys] = jnp.transpose(vals[:, t:t + LANES])

        def score(g):
            s = dot_nn(jnp.concatenate([kn_s[0:keys, g * LANES:(g + 1) * LANES], krep], axis=1), qbd[g])
            tall = None
            for r in range(0, keys, STRIP):
                limit = bias[base * rows + r:base * rows + r + STRIP, :]
                strip = jnp.minimum(s[r:r + STRIP, :], jnp.concatenate([limit, limit], axis=1))
                s_s[g % SLOTS, r:r + STRIP, :] = strip
                for k in range(0, STRIP, 8):
                    tall = strip[k:k + 8, :] if tall is None else jnp.maximum(tall, strip[k:k + 8, :])
            m = jnp.max(tall, axis=0, keepdims=True)
            tops[g] = m if index == 0 else jnp.maximum(m, m_s[g])

        def weigh(g):
            total = None
            for r in range(0, keys, STRIP):
                p = jnp.exp2((s_s[g % SLOTS, r:r + STRIP, :] - tops[g]) * scale2)
                p_s[g % SLOTS, r:r + STRIP, :] = p.astype(BF16)
                for k in range(0, STRIP, 8):
                    total = p[k:k + 8, :] if total is None else total + p[k:k + 8, :]
            sums[g] = jnp.sum(total, axis=0, keepdims=True)

        def mix(g):
            o = dot_nn(vt_s[g * LANES:(g + 1) * LANES, 0:keys], p_s[g % SLOTS, 0:keys, :])
            outs[g] = [o[:nope, :pair], o[nope:, pair:]]

        def finish(g):
            lanes = slice(g * LANES, (g + 1) * LANES)
            m, l, o = tops[g], sums[g], outs[g]
            if index > 0:
                alpha = jnp.exp2((m_s[g] - m) * scale2)
                l = l_s[g] * alpha + l
                o = [acc_s[g, h * nope:(h + 1) * nope, :] * alpha[:, h * pair:(h + 1) * pair] + o[h] for h in range(2)]
            if index < len(chunks) - 1:
                m_s[g] = m
                l_s[g] = l
                acc_s[g, :nope, :] = o[0]
                acc_s[g, nope:, :] = o[1]
            else:
                inv = 1.0 / l
                o = [o[h] * inv[:, h * pair:(h + 1) * pair] for h in range(2)]
                ot = jnp.transpose(jnp.concatenate(o, axis=0).astype(BF16))
                both = [ot[:rows, :], ot[rows:, :]]
                o_own[0:rows, lanes] = jnp.where(core == 0, both[0], both[1])
                o_out[:, lanes] = jnp.where(core == 0, both[1], both[0])
                if g + 1 in SENDS:
                    last = SENDS.index(g + 1)
                    pair_o.append(send_heads(SENDS[last - 1], g + 1, 1 + last))

        tops, sums, outs = {}, {}, {}
        lags = STAGES[len(owners) - 1]
        project(0)
        for t in range(groups + lags[2]):
            if t % 2 == 0 and 0 < t + LEAD < groups:
                project((t + LEAD) * LANES)
            for stage, lag in ((score, 0), (weigh, lags[0]), (mix, lags[1]), (finish, lags[2])):
                if 0 <= t - lag < groups:
                    stage(t - lag)

    wait_all(gath.at[pl.ds(0, 1)], recv_sem.at[0])
    attend(0)
    wait_all(gath.at[pl.ds(0, 2)], recv_sem.at[1])
    attend(1)
    wait_all(gath.at[pl.ds(0, 4)], recv_sem.at[2])
    attend(2)

    wait_all(gath.at[pl.ds(0, n - 1)], send_sem.at[0])
    wait_all(wout, load_sem.at[ukv + 1])
    ov = o_own[...]
    for c in range(0, d_model, OUT_COLS):
        y_acc[:, c:c + OUT_COLS] = dot_nn(ov, wout[:cols, c:c + OUT_COLS])
    for i, copy in enumerate(pair_o):
        copy.wait()
        first, last = SENDS[i] * LANES, SENDS[i + 1] * LANES
        ov = o_in[:, first:last]
        for c in range(0, d_model, OUT_COLS):
            out = y_acc[:, c:c + OUT_COLS] + dot_nn(ov, wout[cols + first:cols + last, c:c + OUT_COLS])
            if last < cols:
                y_acc[:, c:c + OUT_COLS] = out
            else:
                y_ref[:, c:c + OUT_COLS] = (out[:rows, :] + out[rows:, :]).astype(BF16)


def solution(mesh):
    n = mesh.shape['ctx']
    row_spec = P(('dp', 'ctx'), None)
    id_spec = P(('dp', 'ctx'))

    def per_device(x_rows, pos_rows, seg_rows, w_dq, w_uq, w_qr, w_dkv, w_kr, w_uk, w_uv, w_out, gain_q, gain_kv):
        rows, d_model = x_rows.shape
        rope = w_kr.shape[1]
        nope = w_uq.shape[1] * rope // w_qr.shape[1]
        cols = w_uq.shape[1] // 2
        groups = cols // LANES
        keys = n // 2 * rows
        operands = (x_rows, pos_rows.reshape(1, rows), w_dq, w_uq, w_qr, w_dkv, w_kr.T, w_uk, w_uv, w_out, gain_q, gain_kv)
        operands = tuple(pltpu.with_memory_space_constraint(a, pltpu.HBM) for a in operands)
        vm = lambda a: pltpu.VMEM(a.shape, a.dtype)
        cut = lambda a: pltpu.VMEM((a.shape[0], a.shape[1] // 2), a.dtype)
        return pl.pallas_call(
            functools.partial(kernel, n, rows, rope, nope),
            out_shape=jax.ShapeDtypeStruct((rows, w_out.shape[1]), BF16),
            in_specs=[pl.BlockSpec(memory_space=pl.ANY)] * len(operands),
            out_specs=pl.BlockSpec(memory_space=pltpu.VMEM),
            scratch_shapes=[
                pltpu.VMEM((2 * rows, d_model), BF16),
                pltpu.VMEM((2, 1, rows), jnp.int32),
                vm(w_dq), cut(w_uq), cut(w_qr), vm(w_dkv), vm(w_kr.T),
                pltpu.VMEM((2, w_uk.shape[0], cols), BF16),
                vm(w_out), vm(gain_q), vm(gain_kv),
                pltpu.VMEM((2 * rows, w_dq.shape[1]), BF16),
                pltpu.VMEM((2 * rows + 16, LANES), BF16),
                pltpu.VMEM((n, 2 * rows + 16, LANES), BF16),
                pltpu.VMEM((n * rows, 2 * rows), F32),
                pltpu.VMEM((groups, 2 * LANES, 4 * rows), BF16),
                pltpu.VMEM((keys, cols), BF16),
                pltpu.VMEM((cols, keys), BF16),
                pltpu.VMEM((groups, 1, 4 * rows), F32),
                pltpu.VMEM((groups, 1, 4 * rows), F32),
                pltpu.VMEM((groups, 2 * nope, 2 * rows), F32),
                pltpu.VMEM((2 * rows, cols), BF16),
                pltpu.VMEM((rows, cols), BF16),
                pltpu.VMEM((2 * rows, cols), BF16),
                pltpu.VMEM((2 * rows, w_out.shape[1]), F32),
                pltpu.VMEM((SLOTS, keys, 4 * rows), F32),
                pltpu.VMEM((SLOTS, keys, 4 * rows), BF16),
                pltpu.SemaphoreType.DMA((13,)),
                pltpu.SemaphoreType.DMA((1,)),
                pltpu.SemaphoreType.DMA((3,)),
                pltpu.SemaphoreType.DMA((1 + len(SENDS),)),
                pltpu.SemaphoreType.DMA((1 + len(SENDS),)),
            ],
            compiler_params=pltpu.CompilerParams(collective_id=0, has_side_effects=True, vmem_limit_bytes=42 * 1024 * 1024),
        )(*operands)

    return jax.shard_map(per_device, mesh=mesh, in_specs=(row_spec, id_spec, id_spec) + (P(),) * 10, out_specs=row_spec, check_vma=False)
```

```python
import functools
import math

import numpy as np
import jax
import jax.numpy as jnp
from jax import lax
from jax.experimental import pallas as pl
from jax.experimental.pallas import tpu as pltpu
from jax.sharding import PartitionSpec as P

NORM_EPS = 1e-6
MESH = pl.DeviceIdType.MESH
F32 = jnp.float32
BF16 = jnp.bfloat16
LANES = 128
STAGES = ((5, 7, 9), (2, 4, 6))
LEAD = 2
SLOTS = 10
SENDS = (0, 4, 10)
OUT_COLS = 512
STRIP = 32


def rms_rows(vals, gain):
    mean_sq = jnp.mean(vals * vals, axis=-1, keepdims=True)
    return (vals * lax.rsqrt(mean_sq + NORM_EPS) * gain.astype(F32)).astype(BF16)


def dot_nn(a, b):
    return lax.dot_general(a, b, (((1,), (0,)), ((), ())), preferred_element_type=F32)


def dot_nt(a, b):
    return lax.dot_general(a, b, (((1,), (1,)), ((), ())), preferred_element_type=F32)


def dot_tt(a, b):
    return lax.dot_general(a, b, (((0,), (1,)), ((), ())), preferred_element_type=F32)


def iota(shape, axis):
    return lax.broadcasted_iota(jnp.int32, shape, axis)


def kernel(n, rows, rope, nope, x_hbm, pos_hbm, wdq_hbm, wuq_hbm, wqr_hbm, wdkv_hbm, wkr_hbm, wuk_hbm, wuv_hbm, wout_hbm,
           gq_hbm, gkv_hbm, y_ref, x, pos, wdq, wuq, wqr, wdkv, wkr, wukv, wout, gq, gkv,
           cq, lat, gath, bias, qbd, kn_s, vt_s, m_s, l_s, acc_s, o_own, o_out, o_in, y_acc, s_s, p_s,
           load_sem, send_sem, recv_sem, pair_send, pair_recv):
    me = lax.axis_index('ctx')
    core = lax.rem(me, 2)
    chip = me // 2
    partner = me + 1 - 2 * core
    half = rows // 2
    rank = wdkv.shape[1]
    pair = 2 * rows
    cols = wuq.shape[1]
    groups = cols // LANES
    tables = rope // 2

    barrier = pltpu.get_barrier_semaphore()
    for j in range(1, n):
        pl.semaphore_signal(barrier, inc=1, device_id={'ctx': lax.rem(me + j, n)}, device_id_type=MESH)

    loads = []

    def load(src, dst, sem=None):
        sem = len(loads) if sem is None else sem
        copy = pltpu.make_async_copy(src, dst, load_sem.at[sem])
        copy.start()
        loads.append(copy)
        return copy

    def wait_all(ref, sem):
        pltpu.make_async_copy(ref, ref, sem).wait()

    mine = pl.ds(pl.multiple_of(core * rows, rows), rows)
    head_cols = pl.ds(pl.multiple_of(core * cols, LANES), cols)
    rope_cols = pl.ds(pl.multiple_of(core * wqr.shape[1], LANES), wqr.shape[1])
    d_model = x.shape[1]
    cuts = [(0, 1024), (1024, 1024), (2048, d_model - 2048)]
    ld_pos = load(pos_hbm, pos.at[core])
    ld_x = load(x_hbm, x.at[pl.ds(0, rows), :])
    x[rows:, :] = jnp.zeros((rows, d_model), BF16)
    o_own[rows:, :] = jnp.zeros((rows, cols), BF16)
    o_in[rows:, :] = jnp.zeros((rows, cols), BF16)
    ld_kr = load(wkr_hbm, wkr)
    ld_gkv = load(gkv_hbm, gkv)
    ld_dkv = [load(wdkv_hbm.at[pl.ds(c, h), :], wdkv.at[pl.ds(c, h), :]) for c, h in cuts]
    ld_dq = load(wdq_hbm, wdq)
    ld_gq = load(gq_hbm, gq)
    ld_uq = load(wuq_hbm.at[:, head_cols], wuq)
    ld_qr = load(wqr_hbm.at[:, rope_cols], wqr)
    ukv = len(loads)
    load(wuk_hbm.at[:, head_cols], wukv.at[0], ukv)
    load(wuv_hbm.at[:, head_cols], wukv.at[1], ukv)
    row_a = pl.multiple_of(core * cols, LANES)
    row_b = pl.multiple_of((1 - core) * cols, LANES)
    for row, at in ((row_a, 0), (row_b, cols)):
        load(wout_hbm.at[pl.ds(row, cols), :], wout.at[pl.ds(at, cols), :], ukv + 1)

    def rope_tables(pos_row):
        width = pos_row.shape[1]
        freq = iota((tables, width), 0)
        inv_freq = jnp.zeros((tables, width), F32)
        for i in range(tables):
            inv_freq = jnp.where(freq == i, np.float32(10000.0 ** (-2.0 * i / rope)), inv_freq)
        angles = pos_row.astype(F32) * inv_freq

        def table(vals):
            tall = jnp.concatenate([vals] * (LANES // tables), axis=0)
            if width < LANES:
                tall = jnp.concatenate([tall] * (LANES // width), axis=1)
            return jnp.transpose(tall)[:width, :]

        lead = lax.rem(iota((width, LANES), 1), rope) < tables
        cos_t, sin_t = table(jnp.cos(angles)), table(jnp.sin(angles))
        return cos_t, jnp.where(lead, -sin_t, sin_t), lead

    def rotate(a, tabs):
        cos_t, sin_t, lead = tabs
        other = jnp.where(lead, pltpu.roll(a, LANES - tables, 1), pltpu.roll(a, tables, 1))
        return a * cos_t + other * sin_t

    ld_pos.wait()
    tabs = rope_tables(pos[core])
    ld_x.wait()
    ld_kr.wait()
    kr = dot_nt(x[0:rows, :], wkr[...])
    c_kv = None
    for c, (first, height) in zip(ld_dkv, cuts):
        c.wait()
        term = dot_nn(x[0:rows, first:first + height], wdkv[first:first + height, :])
        c_kv = term if c_kv is None else c_kv + term
    ld_gkv.wait()
    c_kv = rms_rows(c_kv, gkv[...].reshape(1, rank))
    kr = rotate(jnp.concatenate([kr] * (LANES // rope), axis=1), tabs)
    pack = kr[0:16, :]
    lane16 = iota((16, LANES), 1) // rope
    for b in range(1, rows // 16):
        pack = jnp.where(lane16 == b, kr[16 * b:16 * b + 16, :], pack)
    pack = pack.astype(BF16)
    lat[0:rows, :] = c_kv[:, :LANES]
    lat[rows:2 * rows, :] = c_kv[:, LANES:]
    lat[2 * rows:2 * rows + 16, :] = pack
    gath[me, 0:rows, :] = c_kv[:, :LANES]
    gath[me, rows:2 * rows, :] = c_kv[:, LANES:]
    gath[me, 2 * rows:2 * rows + 16, :] = pack

    def query_latents():
        ld_dq.wait()
        ld_gq.wait()
        both = dot_nn(x[...], wdq[...])
        cq[mine, :] = rms_rows(both[:rows, :] + both[rows:, :], gq[...].reshape(1, wdq.shape[1]))

    pl.when(chip == 0)(query_latents)
    pl.semaphore_wait(barrier, n - 1)
    bit0, bit1 = lax.rem(chip, 2), chip // 2
    def send(flip_core, flip_chip, sem):
        flip0, flip1 = lax.rem(flip_chip, 2), flip_chip // 2
        peer_chip = (bit0 + flip0 * (1 - 2 * bit0)) + 2 * (bit1 + flip1 * (1 - 2 * bit1))
        peer = 2 * peer_chip + core + flip_core * (1 - 2 * core)
        pltpu.make_async_remote_copy(
            src_ref=lat, dst_ref=gath.at[me], send_sem=send_sem.at[0], recv_sem=recv_sem.at[sem],
            device_id={'ctx': peer}, device_id_type=MESH).start()

    send(1, 0, 0)
    for k in range(3):
        flip_chip = lax.rem(k + 2 * bit1, 3) + 1
        for flip_core in range(2):
            send(flip_core, flip_chip, (flip_chip + 2) // 2)

    def to_partner(src, dst, index):
        copy = pltpu.make_async_remote_copy(
            src_ref=src, dst_ref=dst, send_sem=pair_send.at[index], recv_sem=pair_recv.at[index],
            device_id={'ctx': partner}, device_id_type=MESH)
        copy.start()
        return copy

    pair_pos = to_partner(pos.at[core], pos.at[core], 0)

    pl.when(chip > 0)(query_latents)
    pair_cq = to_partner(cq.at[mine, :], cq.at[mine, :], 1)
    qbd[...] = jnp.zeros_like(qbd)
    pair_pos.wait()
    pos_row = jnp.concatenate([pos[0], pos[1]], axis=1)
    tabs = rope_tables(pos_row)

    q_in = lax.rem(iota((1, pair), 1), rows)
    q_dev = 2 * chip + iota((1, pair), 1) // rows
    q_tok = jnp.where(q_in < half, half * q_dev + q_in, half * (2 * n - 1 - q_dev) + q_in - half)
    q_first = q_tok - pos_row
    side0, side1 = 1 - 2 * bit0, 2 - 4 * bit1
    chips = (chip, chip + side0, chip + side1, chip + side0 + side1)
    chunks = (chips[:1], chips[1:2], chips[2:])
    for i, owner in enumerate(chips):
        r = iota((pair, pair), 0)
        k_in = lax.rem(r, rows)
        k_dev = 2 * owner + r // rows
        k_tok = jnp.where(k_in < half, half * k_dev + k_in, half * (2 * n - 1 - k_dev) + k_in - half)
        ok = (k_tok <= q_tok) & (k_tok >= q_first)
        bias[i * pair:(i + 1) * pair, :] = jnp.where(ok, jnp.inf, -jnp.inf)

    pair_cq.wait()
    c_q = cq[...]
    ld_uq.wait()
    ld_qr.wait()
    qr_all = dot_nn(c_q, wqr[...])
    q_cols = {c: dot_nn(c_q, wuq[:, c:c + 256]).astype(BF16) for c in range(0, cols, 256)}
    for t in range(groups // 2):
        qt = jnp.transpose(rotate(qr_all[:, LANES * t:LANES * t + LANES], tabs).astype(BF16))
        for k in range(4):
            lo = (k % 2) * pair
            qbd[2 * t + k // 2, LANES + rope * k:LANES + rope * k + rope, lo:lo + pair] = qt[rope * k:rope * k + rope, :]
    for g in range(groups):
        qt = jnp.transpose(q_cols[g // 2 * 256][:, g % 2 * LANES:g % 2 * LANES + LANES])
        qbd[g, 0:nope, 0:pair] = qt[0:nope, :]
        qbd[g, nope:2 * nope, pair:2 * pair] = qt[nope:2 * nope, :]

    spread_r = iota((LANES, 4 * LANES), 0)
    spread_c = iota((LANES, 4 * LANES), 1)
    spread = (spread_r == rope * (spread_c // LANES) + lax.rem(spread_c, rope)).astype(F32).astype(BF16)
    scale2 = (nope + rope) ** -0.5 * math.log2(math.e)
    wait_all(wukv, load_sem.at[ukv])

    pair_o = []

    def send_heads(first, last, index):
        part = pl.ds(first * LANES, (last - first) * LANES)
        return to_partner(o_out.at[:, part], o_in.at[pl.ds(0, rows), part], index)

    def attend(index):
        owners = chunks[index]
        count = 2 * len(owners)
        keys = count * rows
        base = 2 * sum(len(c) for c in chunks[:index])

        def rows_of(first, size):
            parts = [gath[pl.ds(2 * owner, 2), first:first + size, :].reshape(2 * size, LANES) for owner in owners]
            return jnp.concatenate(parts, axis=0)

        c_all = jnp.concatenate([rows_of(0, rows), rows_of(rows, rows)], axis=1)
        wide = dot_nn(rows_of(2 * rows, 16), spread).astype(BF16)
        krep = jnp.concatenate([wide[16 * j:16 * j + 16, LANES * b:LANES * b + LANES] for j in range(count) for b in range(rows // 16)], axis=0)

        def project(c):
            kn_s[0:keys, c:c + 256] = dot_nn(c_all, wukv[0, :, c:c + 256]).astype(BF16)
            if keys > LANES:
                vt_s[c:c + 256, 0:keys] = dot_tt(wukv[1, :, c:c + 256], c_all).astype(BF16)
            else:
                vals = dot_nn(c_all, wukv[1, :, c:c + 256]).astype(BF16)
                for t in range(0, 256, LANES):
                    vt_s[c + t:c + t + LANES, 0:keys] = jnp.transpose(vals[:, t:t + LANES])

        def score(g):
            s = dot_nn(jnp.concatenate([kn_s[0:keys, g * LANES:(g + 1) * LANES], krep], axis=1), qbd[g])
            tall = None
            for r in range(0, keys, STRIP):
                limit = bias[base * rows + r:base * rows + r + STRIP, :]
                strip = jnp.minimum(s[r:r + STRIP, :], jnp.concatenate([limit, limit], axis=1))
                s_s[g % SLOTS, r:r + STRIP, :] = strip
                for k in range(0, STRIP, 8):
                    tall = strip[k:k + 8, :] if tall is None else jnp.maximum(tall, strip[k:k + 8, :])
            m = jnp.max(tall, axis=0, keepdims=True)
            tops[g] = m if index == 0 else jnp.maximum(m, m_s[g])

        def weigh(g):
            total = None
            for r in range(0, keys, STRIP):
                p = jnp.exp2((s_s[g % SLOTS, r:r + STRIP, :] - tops[g]) * scale2)
                p_s[g % SLOTS, r:r + STRIP, :] = p.astype(BF16)
                for k in range(0, STRIP, 8):
                    total = p[k:k + 8, :] if total is None else total + p[k:k + 8, :]
            sums[g] = jnp.sum(total, axis=0, keepdims=True)

        def mix(g):
            o = dot_nn(vt_s[g * LANES:(g + 1) * LANES, 0:keys], p_s[g % SLOTS, 0:keys, :])
            outs[g] = [o[:nope, :pair], o[nope:, pair:]]

        def finish(g):
            lanes = slice(g * LANES, (g + 1) * LANES)
            m, l, o = tops[g], sums[g], outs[g]
            if index > 0:
                alpha = jnp.exp2((m_s[g] - m) * scale2)
                l = l_s[g] * alpha + l
                o = [acc_s[g, h * nope:(h + 1) * nope, :] * alpha[:, h * pair:(h + 1) * pair] + o[h] for h in range(2)]
            if index < len(chunks) - 1:
                m_s[g] = m
                l_s[g] = l
                acc_s[g, :nope, :] = o[0]
                acc_s[g, nope:, :] = o[1]
            else:
                inv = 1.0 / l
                o = [o[h] * inv[:, h * pair:(h + 1) * pair] for h in range(2)]
                ot = jnp.transpose(jnp.concatenate(o, axis=0).astype(BF16))
                both = [ot[:rows, :], ot[rows:, :]]
                o_own[0:rows, lanes] = jnp.where(core == 0, both[0], both[1])
                o_out[:, lanes] = jnp.where(core == 0, both[1], both[0])
                if g + 1 in SENDS:
                    last = SENDS.index(g + 1)
                    pair_o.append(send_heads(SENDS[last - 1], g + 1, 1 + last))

        tops, sums, outs = {}, {}, {}
        lags = STAGES[len(owners) - 1]
        project(0)
        for t in range(groups + lags[2]):
            if t % 2 == 0 and 0 < t + LEAD < groups:
                project((t + LEAD) * LANES)
            for stage, lag in ((score, 0), (weigh, lags[0]), (mix, lags[1]), (finish, lags[2])):
                if 0 <= t - lag < groups:
                    stage(t - lag)

    wait_all(gath.at[pl.ds(0, 1)], recv_sem.at[0])
    attend(0)
    wait_all(gath.at[pl.ds(0, 2)], recv_sem.at[1])
    attend(1)
    wait_all(gath.at[pl.ds(0, 4)], recv_sem.at[2])
    attend(2)

    wait_all(gath.at[pl.ds(0, n - 1)], send_sem.at[0])
    wait_all(wout, load_sem.at[ukv + 1])
    ov = o_own[...]
    for c in range(0, d_model, OUT_COLS):
        y_acc[:, c:c + OUT_COLS] = dot_nn(ov, wout[:cols, c:c + OUT_COLS])
    for i, copy in enumerate(pair_o):
        copy.wait()
        first, last = SENDS[i] * LANES, SENDS[i + 1] * LANES
        ov = o_in[:, first:last]
        for c in range(0, d_model, OUT_COLS):
            out = y_acc[:, c:c + OUT_COLS] + dot_nn(ov, wout[cols + first:cols + last, c:c + OUT_COLS])
            if last < cols:
                y_acc[:, c:c + OUT_COLS] = out
            else:
                y_ref[:, c:c + OUT_COLS] = (out[:rows, :] + out[rows:, :]).astype(BF16)


def solution(mesh):
    n = mesh.shape['ctx']
    row_spec = P(('dp', 'ctx'), None)
    id_spec = P(('dp', 'ctx'))

    def per_device(x_rows, pos_rows, seg_rows, w_dq, w_uq, w_qr, w_dkv, w_kr, w_uk, w_uv, w_out, gain_q, gain_kv):
        rows, d_model = x_rows.shape
        rope = w_kr.shape[1]
        nope = w_uq.shape[1] * rope // w_qr.shape[1]
        cols = w_uq.shape[1] // 2
        groups = cols // LANES
        keys = n // 2 * rows
        operands = (x_rows, pos_rows.reshape(1, rows), w_dq, w_uq, w_qr, w_dkv, w_kr.T, w_uk, w_uv, w_out, gain_q, gain_kv)
        operands = tuple(pltpu.with_memory_space_constraint(a, pltpu.HBM) for a in operands)
        vm = lambda a: pltpu.VMEM(a.shape, a.dtype)
        cut = lambda a: pltpu.VMEM((a.shape[0], a.shape[1] // 2), a.dtype)
        return pl.pallas_call(
            functools.partial(kernel, n, rows, rope, nope),
            out_shape=jax.ShapeDtypeStruct((rows, w_out.shape[1]), BF16),
            in_specs=[pl.BlockSpec(memory_space=pl.ANY)] * len(operands),
            out_specs=pl.BlockSpec(memory_space=pltpu.VMEM),
            scratch_shapes=[
                pltpu.VMEM((2 * rows, d_model), BF16),
                pltpu.VMEM((2, 1, rows), jnp.int32),
                vm(w_dq), cut(w_uq), cut(w_qr), vm(w_dkv), vm(w_kr.T),
                pltpu.VMEM((2, w_uk.shape[0], cols), BF16),
                vm(w_out), vm(gain_q), vm(gain_kv),
                pltpu.VMEM((2 * rows, w_dq.shape[1]), BF16),
                pltpu.VMEM((2 * rows + 16, LANES), BF16),
                pltpu.VMEM((n, 2 * rows + 16, LANES), BF16),
                pltpu.VMEM((n * rows, 2 * rows), F32),
                pltpu.VMEM((groups, 2 * LANES, 4 * rows), BF16),
                pltpu.VMEM((keys, cols), BF16),
                pltpu.VMEM((cols, keys), BF16),
                pltpu.VMEM((groups, 1, 4 * rows), F32),
                pltpu.VMEM((groups, 1, 4 * rows), F32),
                pltpu.VMEM((groups, 2 * nope, 2 * rows), F32),
                pltpu.VMEM((2 * rows, cols), BF16),
                pltpu.VMEM((rows, cols), BF16),
                pltpu.VMEM((2 * rows, cols), BF16),
                pltpu.VMEM((2 * rows, w_out.shape[1]), F32),
                pltpu.VMEM((SLOTS, keys, 4 * rows), F32),
                pltpu.VMEM((SLOTS, keys, 4 * rows), BF16),
                pltpu.SemaphoreType.DMA((13,)),
                pltpu.SemaphoreType.DMA((1,)),
                pltpu.SemaphoreType.DMA((3,)),
                pltpu.SemaphoreType.DMA((1 + len(SENDS),)),
                pltpu.SemaphoreType.DMA((1 + len(SENDS),)),
            ],
            compiler_params=pltpu.CompilerParams(collective_id=0, has_side_effects=True, vmem_limit_bytes=42 * 1024 * 1024),
        )(*operands)

    return jax.shard_map(per_device, mesh=mesh, in_specs=(row_spec, id_spec, id_spec) + (P(),) * 10, out_specs=row_spec, check_vma=False)
```
